8 devices in a mesh: dp: 1 (over z), tp: 8 (over y, x, core).
Axes of the slice: x: 2, y: 2, z: 1, core: 2. Of those that a mesh axis runs over, the one named last changes fastest.
Arguments:
- enc_out: bfloat16 [128, 192, 512], P('dp')
- w_proj: bfloat16 [512, 1024], P(None, 'tp')
- labels: int32 [128, 48], P('dp')
- in_len: int32 [128], P('dp')
- lab_len: int32 [128], P('dp')
Outputs:
- output 1: float32 [128], P('dp')
- output 2: float32 [512, 1024], P('dp', 'tp')
- output 3: float32 [128, 192, 512], P('dp')
All inputs are finite; a program needn't handle non-finite values.
Results may differ from the reference program's by a relative error of at most 0.001.
Values are sent between devices in bfloat16 or wider.
A program may use at most 1 GiB of HBM per device.

```python
import math
import jax
import jax.numpy as jnp
from jax import lax

HIDDEN = 512
VOCAB = 1024
FRAMES = 192
MAX_LABELS = 48
BATCH = 128
LAB_MIN = max(1, MAX_LABELS // 5)
NEG_FILL = -1.0e30


def draw_targets(int_key):
    key_lab, key_len, key_in, key_pos = jax.random.split(int_key, 4)
    seq_ids = jnp.arange(BATCH)
    full_pos = jax.random.randint(key_pos, (), 0, BATCH)
    tight_pos = (full_pos + BATCH // 2) % BATCH
    lab_len = jax.random.randint(key_len, (BATCH,), LAB_MIN, MAX_LABELS + 1)
    lab_len = jnp.where(seq_ids == full_pos, MAX_LABELS, jnp.where(seq_ids == tight_pos, LAB_MIN, lab_len))
    in_low = jnp.maximum(2 * lab_len + 1, FRAMES // 5)
    in_len = jax.random.randint(key_in, (BATCH,), in_low, FRAMES + 1)
    in_len = jnp.where(seq_ids == full_pos, FRAMES, jnp.where(seq_ids == tight_pos, 2 * LAB_MIN + 1, in_len))
    lab_ids = jnp.arange(MAX_LABELS)
    labels = jax.random.randint(key_lab, (BATCH, MAX_LABELS), 1, VOCAB)
    at_full = (seq_ids == full_pos)[:, None]
    labels = jnp.where(at_full & (lab_ids == 0)[None, :], 1, jnp.where(at_full & (lab_ids == MAX_LABELS - 1)[None, :], VOCAB - 1, labels))
    return labels.astype(jnp.int32), in_len.astype(jnp.int32), lab_len.astype(jnp.int32)


def setup_inputs(seed: int = 0, part: int = 0) -> dict:
    base_key = jax.random.key(seed)
    part_key = jax.random.fold_in(base_key, part)
    key_hs, key_int = jax.random.split(part_key, 2)
    key_w = jax.random.key(seed + 1)
    enc_out = jax.random.normal(key_hs, (BATCH, FRAMES, HIDDEN), jnp.float32).astype(jnp.bfloat16)
    w_proj = (jax.random.normal(key_w, (HIDDEN, VOCAB), jnp.float32) * (2.0 / math.sqrt(HIDDEN))).astype(jnp.bfloat16)
    labels, in_len, lab_len = draw_targets(key_int)
    return {"enc_out": enc_out, "w_proj": w_proj, "labels": labels, "in_len": in_len, "lab_len": lab_len}


def lattice_loss(label_lp, labels, in_len, lab_len):
    n_seq, n_frames, n_cols = label_lp.shape
    n_lab = n_cols - 1
    n_states = 2 * n_lab + 1
    blank_lp = label_lp[:, :, :1]
    interleaved = jnp.stack([jnp.broadcast_to(blank_lp, (n_seq, n_frames, n_lab)), label_lp[:, :, 1:]], axis=-1)
    emit_all = jnp.concatenate([interleaved.reshape(n_seq, n_frames, 2 * n_lab), blank_lp], axis=-1)
    emit_tm = jnp.swapaxes(emit_all, 0, 1)
    skip_lab = jnp.pad(labels[:, 1:] != labels[:, :-1], ((0, 0), (1, 0)))
    skip_ok = jnp.pad(jnp.stack([jnp.zeros_like(skip_lab), skip_lab], axis=-1).reshape(n_seq, 2 * n_lab), ((0, 0), (0, 1)))
    state_ids = jnp.arange(n_states)
    neg_one = jnp.full((n_seq, 1), NEG_FILL, label_lp.dtype)
    neg_two = jnp.full((n_seq, 2), NEG_FILL, label_lp.dtype)
    alpha_init = jnp.where(state_ids[None, :] == 0, 0.0, neg_one)

    def lattice_step(alpha_prev, step_in):
        emit_t, frame_idx = step_in
        prev_one = jnp.concatenate([neg_one, alpha_prev[:, :-1]], axis=1)
        prev_two = jnp.where(skip_ok, jnp.concatenate([neg_two, alpha_prev[:, :-2]], axis=1), NEG_FILL)
        top_val = lax.stop_gradient(jnp.maximum(jnp.maximum(alpha_prev, prev_one), prev_two))
        merged = top_val + jnp.log(jnp.exp(alpha_prev - top_val) + jnp.exp(prev_one - top_val) + jnp.exp(prev_two - top_val))
        live_seq = (frame_idx < in_len)[:, None]
        return jnp.where(live_seq, merged + emit_t, alpha_prev), None

    alpha_end, _ = lax.scan(lattice_step, alpha_init, (emit_tm, jnp.arange(n_frames)))
    end_sel = (state_ids[None, :] == 2 * lab_len[:, None]) | (state_ids[None, :] == 2 * lab_len[:, None] - 1)
    return -jax.nn.logsumexp(jnp.where(end_sel, alpha_end, NEG_FILL), axis=1)


def label_logprobs(logits, ext_seq):
    log_norm = jax.nn.logsumexp(logits, axis=-1)
    return jnp.take(logits, ext_seq, axis=1) - log_norm[:, None]


def reference(enc_out, w_proj, labels, in_len, lab_len):
    ext_all = jnp.concatenate([jnp.zeros((BATCH, 1), jnp.int32), labels], axis=1)

    def forward_seq(seq_in):
        enc_seq, ext_seq = seq_in
        logits = jnp.dot(enc_seq, w_proj, preferred_element_type=jnp.float32)
        return label_logprobs(logits, ext_seq)

    label_lp = lax.map(forward_seq, (enc_out, ext_all))
    loss, lattice_vjp = jax.vjp(lambda lp_in: lattice_loss(lp_in, labels, in_len, lab_len), label_lp)
    (lp_grad,) = lattice_vjp(jnp.ones_like(loss))

    def backward_seq(grad_acc, seq_in):
        enc_seq, ext_seq, cot_seq = seq_in
        logits = jnp.dot(enc_seq, w_proj, preferred_element_type=jnp.float32)
        _, lp_vjp = jax.vjp(lambda z_in: label_logprobs(z_in, ext_seq), logits)
        (grad_z,) = lp_vjp(cot_seq)
        grad_bf = grad_z.astype(jnp.bfloat16)
        grad_acc = grad_acc + jnp.dot(enc_seq.T, grad_bf, preferred_element_type=jnp.float32)
        grad_hs = jnp.dot(grad_bf, w_proj.T, preferred_element_type=jnp.float32)
        return grad_acc, grad_hs

    grad_w, grad_hs = lax.scan(backward_seq, jnp.zeros((HIDDEN, VOCAB), jnp.float32), (enc_out, ext_all, lp_grad))
    return loss, grad_w, grad_hs
```

```python
import functools

import jax
import jax.numpy as jnp
from jax import lax
from jax.experimental import pallas as pl
from jax.experimental.pallas import tpu as pltpu
from jax.sharding import PartitionSpec as P

NEG_FILL = -1.0e30
CH = 32
NCH = 8
PITCH = 104
DUMMY = 55
UNR = 4
MESH = pl.DeviceIdType.MESH
F32 = jnp.float32
BF16 = jnp.bfloat16


def gather_kernel(n, w_ref, out_ref, send_sem, recv_sem):
    me = lax.axis_index("tp")
    barrier = pltpu.get_barrier_semaphore()
    for i in range(1, n):
        peer = lax.rem(me + i, n)
        pl.semaphore_signal(barrier, inc=1, device_id={"tp": peer}, device_id_type=MESH)
    pl.semaphore_wait(barrier, n - 1)
    copies = []
    for i in range(1, n):
        peer = lax.rem(me + i, n)
        copy = pltpu.make_async_remote_copy(
            src_ref=w_ref,
            dst_ref=out_ref.at[me],
            send_sem=send_sem.at[i],
            recv_sem=recv_sem.at[i],
            device_id={"tp": peer},
            device_id_type=MESH,
        )
        copy.start()
        copies.append(copy)
    out_ref[me] = w_ref[...]
    for copy in copies:
        copy.wait()


def take_lanes(x, idx):
    return jnp.take_along_axis(x, idx, axis=1, mode="promise_in_bounds")


def lse2(a, b):
    top = jnp.maximum(a, b)
    return top + jnp.log(1.0 + jnp.exp(jnp.minimum(a, b) - top))


def ctc_kernel(
    n_seq, n_frames, n_lab,
    in_len, labt_ref, inrow_ref, lenrow_ref, enc_hbm, wg_hbm,
    loss_ref, gw_ref, ghs_hbm,
    enc_v, w_v, wt_v, oh_v, gl_v, eo_v, et_v, ab_v, inv_v, nxt_v, z0_v, z1_v, g0_v, g1_v, h0_v, h1_v, top_v, sum_v, lse_v, gwt_v, lacc_v, zero_v, flag_v,
    tabb, tabt, flag_s, enc_sem, w_sem, gh_sem, zero_sem, flag_sem,
):
    me = lax.axis_index("tp")
    n_vocab = w_v.shape[1]
    n_blk = n_vocab // 128
    n_grp = n_seq // 4
    mid = n_frames // 2
    n_per = n_frames // CH
    per_mid = mid // CH

    def enc_copy(g):
        rows = pl.ds(pl.multiple_of(4 * g * n_frames, 4 * n_frames), 4 * n_frames)
        return pltpu.make_async_copy(enc_hbm.at[rows], enc_v.at[rows], enc_sem.at[g])

    w_copies = [pltpu.make_async_copy(wg_hbm.at[k], w_v.at[:, pl.ds(k * 128, 128)], w_sem.at[k]) for k in range(n_blk)]
    for copy in w_copies:
        copy.start()

    @pl.loop(0, n_grp)
    def _(g):
        enc_copy(g).start()

    for ref in (zero_v, lacc_v, gwt_v, z0_v, z1_v, g0_v, g1_v):
        ref[...] = jnp.zeros_like(ref)
    for j in range(4 * NCH):
        tabb[j] = 0
        tabt[j] = 0

    def zero_copy(b, j):
        return pltpu.make_async_copy(zero_v, ghs_hbm.at[pl.ds(pl.multiple_of(b * n_frames + j * CH, CH), CH)], zero_sem)

    sub48 = lax.broadcasted_iota(jnp.int32, (48, 128), 0)
    in_row = inrow_ref[...]
    len_row = lenrow_ref[...]
    lab48 = jnp.where(sub48 < len_row, labt_ref[...], -1 - sub48)
    skip = lab48 != pltpu.roll(lab48, 1, 0)

    nxt = jnp.full((48, 128), DUMMY, jnp.int32)
    later = jnp.zeros((48, 128), jnp.int32)
    for d in range(n_lab - 1, 0, -1):
        same = (pltpu.roll(lab48, 48 - d, 0) == lab48) & (sub48 < 48 - d)
        nxt = jnp.where(same, sub48 + d, nxt)
        later = later + jnp.where(same, 1, 0)
    nxt_f = jnp.concatenate([nxt.astype(F32), jnp.full((16, 128), float(DUMMY), F32)], axis=0)
    nxt_v[...] = jnp.concatenate([nxt_f, nxt_f + 64.0], axis=0).T.astype(jnp.int32)
    flag_v[...] = jnp.broadcast_to(jnp.max(later.astype(F32), axis=0, keepdims=True), (8, 128)).astype(jnp.int32)
    flag_copy = pltpu.make_async_copy(flag_v, flag_s, flag_sem)
    flag_copy.start()

    for copy in w_copies:
        copy.wait()
    wt_v[...] = w_v[...].T
    row16 = lax.broadcasted_iota(jnp.int32, (16, wt_v.shape[1]), 0)
    tail = jnp.where(row16 == 0, wt_v[0:16, :].astype(F32), 0.0).astype(BF16)
    for k in range(8):
        gl_v[k * 64 + 48:(k + 1) * 64, :] = tail

    lane48 = lax.broadcasted_iota(jnp.int32, (48, 128), 1)
    sub48f = sub48.astype(F32)
    lane1 = lax.broadcasted_iota(jnp.int32, (1, 128), 1)
    lane_mid = lax.broadcasted_iota(jnp.int32, (mid, 128), 1)

    def emit_group(g, n):
        for k in range(4):
            b = 4 * g + k
            cnt = (in_len[b] + CH - 1) // CH
            for j in range(n_per):
                tabb[4 * NCH + n + j] = b
                tabt[4 * NCH + n + j] = j * CH

                @pl.when(j >= cnt)
                def _():
                    zero_copy(b, j).start()
            n = n + cnt
            col = take_lanes(lab48, jnp.full((48, 128), b, jnp.int32))
            firsts = []
            for j in range(n_blk):
                hit = col == lane48 + 128 * j
                oh_v[k * 48:(k + 1) * 48, j * 128:(j + 1) * 128] = jnp.where(hit, 1.0, 0.0).astype(BF16)
                start = jnp.where(lane1 == 0, 48.0, float(DUMMY)) if j == 0 else float(DUMMY)
                firsts.append(jnp.minimum(jnp.min(jnp.where(hit, sub48f, float(DUMMY)), axis=0, keepdims=True), start))
            inv_v[pl.ds(pl.multiple_of(b * 8, 8), 8), :] = jnp.concatenate(firsts, axis=0).astype(jnp.int32)
        picked = jnp.dot(oh_v[...], wt_v[...], preferred_element_type=F32).astype(BF16)
        enc_copy(g).wait()
        for k in range(4):
            for h in range(2):
                gl_v[k * 128 + h * 64:k * 128 + h * 64 + 48, :] = picked[k * 48:(k + 1) * 48]
        for k in range(4):
            b = 4 * g + k
            x = enc_v[pl.ds(pl.multiple_of(b * n_frames, n_frames), n_frames), :]
            e = lax.dot_general(x, gl_v[k * 128:(k + 1) * 128, :], (((1,), (1,)), ((), ())), preferred_element_type=F32)
            eo_v[pl.ds(pl.multiple_of(b * PITCH, 8), mid), :] = jnp.where(lane_mid < 64, e[0:mid], e[mid:n_frames])
        return n

    n_live = lax.fori_loop(0, n_grp, emit_group, 0)
    for j in range(4 * NCH):
        tabb[4 * NCH + n_live + j] = 0
        tabt[4 * NCH + n_live + j] = 0
    n_iter = (n_live + NCH - 1) // NCH

    def turn_emissions(jj, acc):
        for u in range(UNR):
            j = jj * UNR + u
            turned = eo_v[pl.ds(j, n_seq, stride=PITCH), :].T
            low = turned[48:49]
            high = turned[112:113]
            et_v[pl.ds(pl.multiple_of(j * 48, 8), 48), :] = turned[0:48] - low
            et_v[pl.ds(pl.multiple_of((j + mid) * 48, 8), 48), :] = turned[64:112] - high
            acc = acc + jnp.where(j < in_row, low, 0.0) + jnp.where(j + mid < in_row, high, 0.0)
        return acc

    blank_sum = lax.fori_loop(0, mid // UNR, turn_emissions, jnp.zeros((1, 128), F32))

    neg8 = jnp.full((8, 128), NEG_FILL, F32)
    sub56 = lax.broadcasted_iota(jnp.int32, (56, 128), 0)
    skip56 = jnp.concatenate([jnp.where(skip, 1.0, 0.0), jnp.zeros((8, 128), F32)], axis=0) > 0.5

    def emit_at(t):
        return et_v[pl.ds(pl.multiple_of(t * 48, 8), 48), :]

    def alpha_step(t, blk, lab):
        shifted = pltpu.roll(jnp.concatenate([lab, neg8], axis=0), 1, 0)
        blk_new = lse2(blk, shifted)
        via = jnp.where(skip, blk_new[0:48], blk[0:48])
        lab_new = lse2(lab, via) + emit_at(t)
        live = t < in_row
        return jnp.where(live, blk_new, blk), jnp.where(live, lab_new, lab)

    def beta_step(t, blk, lab):
        emitted = lab + emit_at(t + 1)
        blk_new = lse2(blk, jnp.concatenate([emitted, neg8], axis=0))
        via = jnp.where(skip56, blk_new, blk)
        lab_new = lse2(emitted, pltpu.roll(via, 55, 0)[0:48])
        live = t + 1 < in_row
        return jnp.where(live, blk_new, blk), jnp.where(live, lab_new, lab)

    def keep(t, blk, lab):
        row = pl.multiple_of(t * 104, 8)
        ab_v[pl.ds(row, 56), :] = blk
        ab_v[pl.ds(row + 56, 48), :] = lab

    a_blk = jnp.where(sub56 == 0, 0.0, NEG_FILL).astype(F32) + jnp.zeros((56, 128), F32)
    a_lab = jnp.full((48, 128), NEG_FILL, F32)
    b_blk = jnp.where(sub56 == len_row, 0.0, NEG_FILL).astype(F32)
    b_lab = jnp.where(sub48 == len_row - 1, 0.0, NEG_FILL).astype(F32)

    a_blk, a_lab = alpha_step(0, a_blk, a_lab)
    keep(0, a_blk, a_lab)
    keep(n_frames - 1, b_blk, b_lab)

    def first_half(k, state):
        a_blk, a_lab, b_blk, b_lab = state
        a_blk, a_lab = alpha_step(k, a_blk, a_lab)
        keep(k, a_blk, a_lab)
        t = n_frames - 1 - k
        b_blk, b_lab = beta_step(t, b_blk, b_lab)
        keep(t, b_blk, b_lab)
        return a_blk, a_lab, b_blk, b_lab

    a_blk, a_lab, b_blk, b_lab = lax.fori_loop(1, mid, first_half, (a_blk, a_lab, b_blk, b_lab))

    m_blk, m_lab = beta_step(mid - 1, b_blk, b_lab)
    s_blk = a_blk + m_blk
    s_lab = a_lab + m_lab
    top = jnp.maximum(jnp.max(s_blk, axis=0, keepdims=True), jnp.max(s_lab, axis=0, keepdims=True))
    total = jnp.sum(jnp.exp(s_blk - top), axis=0, keepdims=True) + jnp.sum(jnp.exp(s_lab - top), axis=0, keepdims=True)
    log_z = top + jnp.log(total)
    sub8 = lax.broadcasted_iota(jnp.int32, (8, 128), 0)

    def put_occ(t, blk, lab):
        row = pl.multiple_of(t * 104, 8)
        occ_blk = jnp.sum(jnp.exp(ab_v[pl.ds(row, 56), :] + (blk - log_z)), axis=0, keepdims=True)
        occ_lab = jnp.exp(ab_v[pl.ds(row + 56, 48), :] + (lab - log_z))
        ab_v[pl.ds(row, 48), :] = occ_lab
        ab_v[pl.ds(row + 48, 8), :] = jnp.where(sub8 == 0, occ_blk, 0.0)

    def second_half(k, state):
        a_blk, a_lab, b_blk, b_lab = state
        a_blk, a_lab = alpha_step(k, a_blk, a_lab)
        t = n_frames - 1 - k
        b_blk, b_lab = beta_step(t, b_blk, b_lab)
        put_occ(k, a_blk, a_lab)
        put_occ(t, b_blk, b_lab)
        return a_blk, a_lab, b_blk, b_lab

    lax.fori_loop(mid, n_frames, second_half, (a_blk, a_lab, b_blk, b_lab))

    zero8 = jnp.zeros((8, 128), F32)

    @pl.loop(0, mid // UNR)
    def _(jj):
        for u in range(UNR):
            j = jj * UNR + u
            low = ab_v[pl.ds(pl.multiple_of(j * 104, 8), 56), :]
            high = ab_v[pl.ds(pl.multiple_of((j + mid) * 104, 8), 56), :]
            turned = jnp.concatenate([low, zero8, high, zero8], axis=0).T
            eo_v[pl.ds(j, n_seq, stride=PITCH), :] = turned + take_lanes(turned, nxt_v[...])

    flag_copy.wait()

    @pl.loop(0, n_seq)
    def _(b):
        @pl.when(flag_s[0, b] > 1)
        def _():
            rows = pl.ds(pl.multiple_of(b * PITCH, 8), mid)
            count = flag_s[0, b]
            rounds = sum((count >= 2 ** r).astype(jnp.int32) for r in range(1, 6))

            def more(_, link):
                link = take_lanes(link, link)
                occ = eo_v[rows, :]
                eo_v[rows, :] = occ + take_lanes(occ, jnp.broadcast_to(link[0:1], (mid, 128)))
                return link

            lax.fori_loop(0, rounds, more, jnp.broadcast_to(nxt_v[pl.ds(b, 1), :], (8, 128)))

    row_ids = lax.broadcasted_iota(jnp.int32, (CH, 128), 0)
    own = pl.ds(pl.multiple_of(me * 128, 128), 128)

    def chunk(i, c):
        idx = i * NCH + c
        return tabb[idx + 4 * NCH], tabt[idx + 4 * NCH], (idx >= 0) & (idx < n_live)

    def enc_rows(i):
        parts = []
        for c in range(NCH):
            b, t0, _ = chunk(i, c)
            parts.append(enc_v[pl.ds(pl.multiple_of(b * n_frames + t0, CH), CH), :])
        return jnp.concatenate(parts, axis=0)

    def gh_copy(i, c, h_v, par):
        b, t0, _ = chunk(i, c)
        row = pl.multiple_of(b * n_frames + t0, CH)
        return pltpu.make_async_copy(h_v.at[pl.ds(c * CH, CH)], ghs_hbm.at[pl.ds(row, CH)], gh_sem.at[par, c])

    def gh_wait(i, h_v, par):
        for c in range(NCH):
            @pl.when(chunk(i, c)[2])
            def _():
                gh_copy(i, c, h_v, par).wait()

    def stage(i, zw, zr, gwr, gr, h_v, par):
        gh_wait(i - 4, h_v, par)
        zw[...] = jnp.dot(enc_rows(i), w_v[...], preferred_element_type=F32)
        for r in range(NCH * CH // 8):
            rows = slice(r * 8, (r + 1) * 8)
            z = zr[rows, :]
            parts = [z[:, j * 128:(j + 1) * 128] for j in range(n_blk)]
            top = functools.reduce(jnp.maximum, parts)
            top_v[rows, :] = top
            sum_v[rows, :] = functools.reduce(jnp.add, [jnp.exp(part - top) for part in parts])
        tops = top_v[...]
        top = jnp.max(tops, axis=1, keepdims=True)
        lse_v[...] = jnp.broadcast_to(top + jnp.log(jnp.sum(sum_v[...] * jnp.exp(tops - top), axis=1, keepdims=True)), (NCH * CH, 128))
        for c in range(NCH):
            b, t0, ok = chunk(i - 1, c)
            rows = slice(c * CH, (c + 1) * CH)
            live = row_ids < jnp.where(ok, in_len[b], 0) - t0
            lse = lse_v[rows, :]
            lacc_v[pl.ds(b, 1), :] += jnp.sum(jnp.where(live, lse, 0.0), axis=0, keepdims=True)
            lse = jnp.where(live, lse, 3.0e38)
            upper = (t0 >= mid).astype(jnp.int32)
            occ = jnp.where(live, eo_v[pl.ds(pl.multiple_of(b * PITCH + t0 - upper * mid, 8), CH), :], 0.0)
            inv = inv_v[pl.ds(pl.multiple_of(b * 8, 8), 8), :] + upper * 64
            for j in range(n_blk):
                cols = slice(j * 128, (j + 1) * 128)
                col_occ = take_lanes(occ, jnp.broadcast_to(inv[j:j + 1], (CH, 128)))
                gwr[rows, cols] = (jnp.exp(zr[rows, cols] - lse) - col_occ).astype(BF16)
        h_v[...] = jnp.dot(gr[...], wt_v[...], preferred_element_type=F32)
        gwt_v[...] += lax.dot_general(gr[:, own], enc_rows(i - 2), (((0,), (0,)), ((), ())), preferred_element_type=F32)
        for c in range(NCH):
            @pl.when(chunk(i - 2, c)[2])
            def _():
                gh_copy(i - 2, c, h_v, par).start()

    trips = (n_iter + 3) // 2

    @pl.loop(0, trips)
    def _(ii):
        stage(2 * ii, z0_v, z1_v, g1_v, g0_v, h0_v, 0)
        stage(2 * ii + 1, z1_v, z0_v, g0_v, g1_v, h1_v, 1)

    gh_wait(2 * trips - 4, h0_v, 0)
    gh_wait(2 * trips - 3, h1_v, 1)
    gw_ref[...] = gwt_v[...].T
    loss_ref[...] = lacc_v[...].T[0:1, :] - blank_sum - log_z

    @pl.loop(0, n_seq)
    def _(b):
        cnt = (in_len[b] + CH - 1) // CH
        for j in range(n_per):
            @pl.when(j >= cnt)
            def _():
                zero_copy(b, j).wait()


def solution(mesh):
    n_dev = mesh.shape["tp"]

    def device_fn(enc_out, w_loc, labels, in_len, lab_len):
        n_seq, n_frames, hidden = enc_out.shape
        n_lab = labels.shape[1]
        n_cols = w_loc.shape[1]
        n_vocab = n_cols * n_dev
        vmem = pl.BlockSpec(memory_space=pltpu.VMEM)
        smem = pl.BlockSpec(memory_space=pltpu.SMEM)
        anyspace = pl.BlockSpec(memory_space=pl.ANY)
        w_all = pl.pallas_call(
            functools.partial(gather_kernel, n_dev),
            out_shape=jax.ShapeDtypeStruct((n_dev, hidden, n_cols), BF16),
            in_specs=[vmem],
            out_specs=vmem,
            scratch_shapes=[pltpu.SemaphoreType.DMA((n_dev,)), pltpu.SemaphoreType.DMA((n_dev,))],
            compiler_params=pltpu.CompilerParams(collective_id=0, has_side_effects=True),
            name="gather_w",
        )(w_loc)
        n_per = n_frames // CH
        n_grp = n_seq // 4
        loss, grad_w, grad_hs = pl.pallas_call(
            functools.partial(ctc_kernel, n_seq, n_frames, n_lab),
            out_shape=(
                jax.ShapeDtypeStruct((1, n_seq), F32),
                jax.ShapeDtypeStruct((hidden, n_cols), F32),
                jax.ShapeDtypeStruct((n_seq * n_frames, hidden), F32),
            ),
            in_specs=[smem, vmem, vmem, vmem, anyspace, anyspace],
            out_specs=(vmem, vmem, anyspace),
            scratch_shapes=[
                pltpu.VMEM((n_seq * n_frames, hidden), BF16),
                pltpu.VMEM((hidden, n_vocab), BF16),
                pltpu.VMEM((n_vocab, hidden), BF16),
                pltpu.VMEM((192, n_vocab), BF16),
                pltpu.VMEM((512, hidden), BF16),
                pltpu.VMEM((n_seq * PITCH, 128), F32),
                pltpu.VMEM((n_frames * 48, 128), F32),
                pltpu.VMEM((n_frames * 104, 128), F32),
                pltpu.VMEM((n_seq * n_dev, 128), jnp.int32),
                pltpu.VMEM((n_seq, 128), jnp.int32),
                pltpu.VMEM((NCH * CH, n_vocab), F32),
                pltpu.VMEM((NCH * CH, n_vocab), F32),
                pltpu.VMEM((NCH * CH, n_vocab), BF16),
                pltpu.VMEM((NCH * CH, n_vocab), BF16),
                pltpu.VMEM((NCH * CH, hidden), F32),
                pltpu.VMEM((NCH * CH, hidden), F32),
                pltpu.VMEM((NCH * CH, 128), F32),
                pltpu.VMEM((NCH * CH, 128), F32),
                pltpu.VMEM((NCH * CH, 128), F32),
                pltpu.VMEM((n_cols, hidden), F32),
                pltpu.VMEM((n_seq, 128), F32),
                pltpu.VMEM((CH, hidden), F32),
                pltpu.VMEM((8, 128), jnp.int32),
                pltpu.SMEM((n_seq * n_per + 10 * NCH,), jnp.int32),
                pltpu.SMEM((n_seq * n_per + 10 * NCH,), jnp.int32),
                pltpu.SMEM((8, 128), jnp.int32),
                pltpu.SemaphoreType.DMA((n_grp,)),
                pltpu.SemaphoreType.DMA((n_dev,)),
                pltpu.SemaphoreType.DMA((2, NCH)),
                pltpu.SemaphoreType.DMA,
                pltpu.SemaphoreType.DMA,
            ],
            compiler_params=pltpu.CompilerParams(vmem_limit_bytes=63 * 1024 * 1024),
            name="ctc",
        )(in_len, labels.T, in_len.reshape(1, n_seq), lab_len.reshape(1, n_seq), enc_out.reshape(n_seq * n_frames, hidden), w_all)
        return loss.reshape(n_seq), grad_w, grad_hs.reshape(n_seq, n_frames, hidden)

    return jax.shard_map(device_fn, mesh=mesh, in_specs=(P("dp"), P(None, "tp"), P("dp"), P("dp"), P("dp")), out_specs=(P("dp"), P("dp", "tp"), P("dp")), check_vma=False)
```

```python
import functools

import jax
import jax.numpy as jnp
from jax import lax
from jax.experimental import pallas as pl
from jax.experimental.pallas import tpu as pltpu
from jax.sharding import PartitionSpec as P

NEG_FILL = -1.0e30
CH = 32
NCH = 8
PAD = 8 * NCH
PITCH = 104
DUMMY = 55
UNR = 4
AHEAD = 6
MESH = pl.DeviceIdType.MESH
F32 = jnp.float32
BF16 = jnp.bfloat16


def gather_kernel(w_ref, out_ref, send_sem, recv_sem):
    me = lax.axis_index("tp")
    core, col, row = lax.rem(me, 2), lax.rem(me // 2, 2), me // 4
    mate = me + 1 - 2 * core
    across = me + 2 * (1 - 2 * col)
    along = me + 4 * (1 - 2 * row)
    far = across + along - me
    barrier = pltpu.get_barrier_semaphore()
    for peer in (mate, across, along):
        pl.semaphore_signal(barrier, inc=1, device_id={"tp": peer}, device_id_type=MESH)
    pl.semaphore_wait(barrier, 3)
    rows = w_ref.shape[0]
    upper, lower = pl.ds(0, rows // 2), pl.ds(rows // 2, rows // 2)

    def push(k, src, dst, peer):
        copy = pltpu.make_async_remote_copy(
            src_ref=src, dst_ref=dst, send_sem=send_sem.at[k], recv_sem=recv_sem.at[k],
            device_id={"tp": peer}, device_id_type=MESH,
        )
        copy.start()
        return copy

    own = out_ref.at[me]
    copies = [push(1, w_ref, own, across), push(2, w_ref, own, along), push(0, w_ref, own, mate)]
    out_ref[me] = w_ref[...]
    copies[0].wait_recv()
    copies.append(push(4, out_ref.at[across, upper], out_ref.at[across, upper], along))
    copies.append(push(3, out_ref.at[across], out_ref.at[across], mate))
    copies[1].wait_recv()
    copies.append(push(6, out_ref.at[along, lower], out_ref.at[along, lower], across))
    copies.append(push(5, out_ref.at[along], out_ref.at[along], mate))
    copies[3].wait_recv()
    copies.append(push(7, out_ref.at[far, upper], out_ref.at[far, upper], mate))
    copies[5].wait_recv()
    copies.append(push(8, out_ref.at[far, lower], out_ref.at[far, lower], mate))
    for k in (2, 4, 6, 7, 8):
        copies[k].wait_recv()
    for copy in copies:
        copy.wait_send()


def take_lanes(x, idx):
    return jnp.take_along_axis(x, idx, axis=1, mode="promise_in_bounds")


def lse2(a, b):
    top = jnp.maximum(a, b)
    return top + jnp.log(1.0 + jnp.exp(jnp.minimum(a, b) - top))


def ctc_kernel(
    n_seq, n_frames, n_lab,
    in_len, labt_ref, inrow_ref, lenrow_ref, enc_hbm, wg_hbm,
    loss_ref, gw_ref, ghs_hbm,
    enc_v, w_v, wt_v, oh0_v, oh1_v, gl0_v, gl1_v, eo_v, et_v, ab_v, inv_v, nxt_v, z0_v, z1_v, g0_v, g1_v, h0_v, h1_v, top_v, sum_v, lse_v, gwt_v, lacc_v, zero_v, flag_v,
    tabb, tabt, flag_s, enc_sem, w_sem, gh_sem, zero_sem, flag_sem,
):
    me = lax.axis_index("tp")
    n_vocab = w_v.shape[1]
    n_blk = n_vocab // 128
    n_grp = n_seq // 4
    mid = n_frames // 2
    n_per = n_frames // CH
    per_mid = mid // CH

    def enc_copy(g):
        rows = pl.ds(pl.multiple_of(4 * g * n_frames, 4 * n_frames), 4 * n_frames)
        return pltpu.make_async_copy(enc_hbm.at[rows], enc_v.at[rows], enc_sem.at[g])

    w_copies = [pltpu.make_async_copy(wg_hbm.at[k], w_v.at[:, pl.ds(k * 128, 128)], w_sem.at[k]) for k in range(n_blk)]
    for copy in w_copies:
        copy.start()

    for g in range(AHEAD):
        enc_copy(g).start()

    for ref in (zero_v, lacc_v, gwt_v, z0_v, z1_v, g0_v, g1_v):
        ref[...] = jnp.zeros_like(ref)
    for j in range(PAD):
        tabb[j] = 0
        tabt[j] = 0

    def zero_copy(b, j):
        return pltpu.make_async_copy(zero_v, ghs_hbm.at[pl.ds(pl.multiple_of(b * n_frames + j * CH, CH), CH)], zero_sem)

    sub48 = lax.broadcasted_iota(jnp.int32, (48, 128), 0)
    in_row = inrow_ref[...]
    len_row = lenrow_ref[...]
    lab48 = jnp.where(sub48 < len_row, labt_ref[...], -1 - sub48)
    skip = lab48 != pltpu.roll(lab48, 1, 0)

    nxt = jnp.full((48, 128), DUMMY, jnp.int32)
    later = jnp.zeros((48, 128), jnp.int32)
    for d in range(n_lab - 1, 0, -1):
        same = (pltpu.roll(lab48, 48 - d, 0) == lab48) & (sub48 < 48 - d)
        nxt = jnp.where(same, sub48 + d, nxt)
        later = later + jnp.where(same, 1, 0)
    nxt_f = jnp.concatenate([nxt.astype(F32), jnp.full((16, 128), float(DUMMY), F32)], axis=0)
    nxt_v[...] = jnp.concatenate([nxt_f, nxt_f + 64.0], axis=0).T.astype(jnp.int32)
    flag_v[...] = jnp.broadcast_to(jnp.max(later.astype(F32), axis=0, keepdims=True), (8, 128)).astype(jnp.int32)
    flag_copy = pltpu.make_async_copy(flag_v, flag_s, flag_sem)
    flag_copy.start()

    for copy in w_copies:
        copy.wait()
    wt_v[...] = w_v[...].T
    row16 = lax.broadcasted_iota(jnp.int32, (16, wt_v.shape[1]), 0)
    tail = jnp.where(row16 == 0, wt_v[0:16, :].astype(F32), 0.0).astype(BF16)
    for k in range(8):
        gl0_v[k * 64 + 48:(k + 1) * 64, :] = tail
        gl1_v[k * 64 + 48:(k + 1) * 64, :] = tail

    lane48 = lax.broadcasted_iota(jnp.int32, (48, 128), 1)
    sub48f = sub48.astype(F32)
    lane1 = lax.broadcasted_iota(jnp.int32, (1, 128), 1)
    lane_mid = lax.broadcasted_iota(jnp.int32, (mid, 128), 1)

    def list_group(g, n):
        for k in range(4):
            b = jnp.minimum(4 * g + k, n_seq - 1)
            cnt = jnp.where(g < n_grp, (in_len[b] + CH - 1) // CH, n_per)
            for j in range(n_per):
                tabb[PAD + n + j] = b
                tabt[PAD + n + j] = j * CH

                @pl.when(j >= cnt)
                def _():
                    zero_copy(b, j).start()
            n = n + jnp.where(g < n_grp, cnt, 0)
        return n

    def build_hot(g, oh_v):
        for k in range(4):
            b = 4 * g + k
            col = take_lanes(lab48, jnp.full((48, 128), b, jnp.int32))
            firsts = []
            for j in range(n_blk):
                hit = col == lane48 + 128 * j
                oh_v[k * 48:(k + 1) * 48, j * 128:(j + 1) * 128] = jnp.where(hit, 1.0, 0.0).astype(BF16)
                start = jnp.where(lane1 == 0, 48.0, float(DUMMY)) if j == 0 else float(DUMMY)
                firsts.append(jnp.minimum(jnp.min(jnp.where(hit, sub48f, float(DUMMY)), axis=0, keepdims=True), start))
            inv_v[pl.ds(pl.multiple_of(b * 8, 8), 8), :] = jnp.concatenate(firsts, axis=0).astype(jnp.int32)

    def pick_cols(oh_v, gl_v):
        picked = jnp.dot(oh_v[...], wt_v[...], preferred_element_type=F32).astype(BF16)
        for k in range(4):
            for h in range(2):
                gl_v[k * 128 + h * 64:k * 128 + h * 64 + 48, :] = picked[k * 48:(k + 1) * 48]

    def emit_group(g, gl_v):
        for k in range(4):
            b = 4 * g + k
            x = enc_v[pl.ds(pl.multiple_of(b * n_frames, n_frames), n_frames), :]
            e = lax.dot_general(x, gl_v[k * 128:(k + 1) * 128, :], (((1,), (1,)), ((), ())), preferred_element_type=F32)
            eo_v[pl.ds(pl.multiple_of(b * PITCH, 8), mid), :] = jnp.where(lane_mid < 64, e[0:mid], e[mid:n_frames])

    build_hot(0, oh0_v)

    def emit_pair(ii, n):
        for s in range(2):
            g = 2 * ii + s

            @pl.when((g >= 1) & (g <= n_grp))
            def _():
                enc_copy(g - 1).wait()

            @pl.when(g + AHEAD < n_grp)
            def _():
                enc_copy(g + AHEAD).start()
        n = list_group(2 * ii + 1, list_group(2 * ii, n))
        for s in range(2):
            g = 2 * ii + s
            build_hot(jnp.minimum(g + 1, n_grp - 1), (oh1_v, oh0_v)[s])
            pick_cols((oh0_v, oh1_v)[s], (gl0_v, gl1_v)[s])
            emit_group(jnp.clip(g - 1, 0, n_grp - 1), (gl1_v, gl0_v)[s])
        return n

    n_live = lax.fori_loop(0, n_grp // 2 + 1, emit_pair, 0)
    for j in range(PAD):
        tabb[PAD + n_live + j] = 0
        tabt[PAD + n_live + j] = 0
    n_iter = (n_live + NCH - 1) // NCH

    def turn_emissions(jj, acc):
        for u in range(UNR):
            j = jj * UNR + u
            turned = eo_v[pl.ds(j, n_seq, stride=PITCH), :].T
            low = turned[48:49]
            high = turned[112:113]
            et_v[pl.ds(pl.multiple_of(j * 48, 8), 48), :] = turned[0:48] - low
            et_v[pl.ds(pl.multiple_of((j + mid) * 48, 8), 48), :] = turned[64:112] - high
            acc = acc + jnp.where(j < in_row, low, 0.0) + jnp.where(j + mid < in_row, high, 0.0)
        return acc

    blank_sum = lax.fori_loop(0, mid // UNR, turn_emissions, jnp.zeros((1, 128), F32))

    neg8 = jnp.full((8, 128), NEG_FILL, F32)
    sub56 = lax.broadcasted_iota(jnp.int32, (56, 128), 0)
    skip56 = jnp.concatenate([jnp.where(skip, 1.0, 0.0), jnp.zeros((8, 128), F32)], axis=0) > 0.5

    def emit_at(t):
        return et_v[pl.ds(pl.multiple_of(t * 48, 8), 48), :]

    def alpha_step(t, blk, lab):
        shifted = pltpu.roll(jnp.concatenate([lab, neg8], axis=0), 1, 0)
        blk_new = lse2(blk, shifted)
        via = jnp.where(skip, blk_new[0:48], blk[0:48])
        lab_new = lse2(lab, via) + emit_at(t)
        live = t < in_row
        return jnp.where(live, blk_new, blk), jnp.where(live, lab_new, lab)

    def beta_step(t, blk, lab):
        emitted = lab + emit_at(t + 1)
        blk_new = lse2(blk, jnp.concatenate([emitted, neg8], axis=0))
        via = jnp.where(skip56, blk_new, blk)
        lab_new = lse2(emitted, pltpu.roll(via, 55, 0)[0:48])
        live = t + 1 < in_row
        return jnp.where(live, blk_new, blk), jnp.where(live, lab_new, lab)

    def keep(t, blk, lab):
        row = pl.multiple_of(t * 104, 8)
        ab_v[pl.ds(row, 56), :] = blk
        ab_v[pl.ds(row + 56, 48), :] = lab

    a_blk = jnp.where(sub56 == 0, 0.0, NEG_FILL).astype(F32) + jnp.zeros((56, 128), F32)
    a_lab = jnp.full((48, 128), NEG_FILL, F32)
    b_blk = jnp.where(sub56 == len_row, 0.0, NEG_FILL).astype(F32)
    b_lab = jnp.where(sub48 == len_row - 1, 0.0, NEG_FILL).astype(F32)

    a_blk, a_lab = alpha_step(0, a_blk, a_lab)
    keep(0, a_blk, a_lab)
    keep(n_frames - 1, b_blk, b_lab)

    def first_half(k, state):
        a_blk, a_lab, b_blk, b_lab = state
        a_blk, a_lab = alpha_step(k, a_blk, a_lab)
        keep(k, a_blk, a_lab)
        t = n_frames - 1 - k
        b_blk, b_lab = beta_step(t, b_blk, b_lab)
        keep(t, b_blk, b_lab)
        return a_blk, a_lab, b_blk, b_lab

    a_blk, a_lab, b_blk, b_lab = lax.fori_loop(1, mid, first_half, (a_blk, a_lab, b_blk, b_lab))

    m_blk, m_lab = beta_step(mid - 1, b_blk, b_lab)
    s_blk = a_blk + m_blk
    s_lab = a_lab + m_lab
    top = jnp.maximum(jnp.max(s_blk, axis=0, keepdims=True), jnp.max(s_lab, axis=0, keepdims=True))
    total = jnp.sum(jnp.exp(s_blk - top), axis=0, keepdims=True) + jnp.sum(jnp.exp(s_lab - top), axis=0, keepdims=True)
    log_z = top + jnp.log(total)
    sub8 = lax.broadcasted_iota(jnp.int32, (8, 128), 0)

    def put_occ(t, blk, lab):
        row = pl.multiple_of(t * 104, 8)
        occ_blk = jnp.sum(jnp.exp(ab_v[pl.ds(row, 56), :] + (blk - log_z)), axis=0, keepdims=True)
        occ_lab = jnp.exp(ab_v[pl.ds(row + 56, 48), :] + (lab - log_z))
        ab_v[pl.ds(row, 48), :] = occ_lab
        ab_v[pl.ds(row + 48, 8), :] = jnp.where(sub8 == 0, occ_blk, 0.0)

    def second_half(k, state):
        a_blk, a_lab, b_blk, b_lab = state
        t = n_frames - 1 - k
        put_occ(k - 1, a_blk, a_lab)
        put_occ(t + 1, b_blk, b_lab)
        a_blk, a_lab = alpha_step(k, a_blk, a_lab)
        b_blk, b_lab = beta_step(t, b_blk, b_lab)
        return a_blk, a_lab, b_blk, b_lab

    a_blk, a_lab = alpha_step(mid, a_blk, a_lab)
    a_blk, a_lab, b_blk, b_lab = lax.fori_loop(mid + 1, n_frames, second_half, (a_blk, a_lab, m_blk, m_lab))
    put_occ(n_frames - 1, a_blk, a_lab)
    put_occ(0, b_blk, b_lab)

    zero8 = jnp.zeros((8, 128), F32)

    @pl.loop(0, mid // UNR)
    def _(jj):
        for u in range(UNR):
            j = jj * UNR + u
            low = ab_v[pl.ds(pl.multiple_of(j * 104, 8), 56), :]
            high = ab_v[pl.ds(pl.multiple_of((j + mid) * 104, 8), 56), :]
            turned = jnp.concatenate([low, zero8, high, zero8], axis=0).T
            eo_v[pl.ds(j, n_seq, stride=PITCH), :] = turned + take_lanes(turned, nxt_v[...])

    flag_copy.wait()

    def more_rounds(b):
        @pl.when(flag_s[0, b] > 1)
        def _():
            rows = pl.ds(pl.multiple_of(b * PITCH, 8), mid)
            count = flag_s[0, b]
            rounds = sum((count >= 2 ** r).astype(jnp.int32) for r in range(1, 6))

            def more(_, link):
                link = take_lanes(link, link)
                occ = eo_v[rows, :]
                eo_v[rows, :] = occ + take_lanes(occ, jnp.broadcast_to(link[0:1], (mid, 128)))
                return link

            lax.fori_loop(0, rounds, more, jnp.broadcast_to(nxt_v[pl.ds(b, 1), :], (8, 128)))

    @pl.loop(0, n_seq // 16)
    def _(bb):
        most = functools.reduce(jnp.maximum, [flag_s[0, bb * 16 + u] for u in range(16)])

        @pl.when(most > 1)
        def _():
            @pl.loop(0, 16)
            def _(u):
                more_rounds(bb * 16 + u)

    row_ids = lax.broadcasted_iota(jnp.int32, (CH, 128), 0)
    own = pl.ds(pl.multiple_of(me * 128, 128), 128)

    def chunk(i, c):
        idx = i * NCH + c
        return tabb[idx + PAD], tabt[idx + PAD], (idx >= 0) & (idx < n_live)

    def enc_rows(i):
        parts = []
        for c in range(NCH):
            b, t0, _ = chunk(i, c)
            parts.append(enc_v[pl.ds(pl.multiple_of(b * n_frames + t0, CH), CH), :])
        return jnp.concatenate(parts, axis=0)

    def gh_copy(i, c, h_v, par):
        b, t0, _ = chunk(i, c)
        row = pl.multiple_of(b * n_frames + t0, CH)
        return pltpu.make_async_copy(h_v.at[pl.ds(c * CH, CH)], ghs_hbm.at[pl.ds(row, CH)], gh_sem.at[par, c])

    def gh_wait(i, h_v, par):
        for c in range(NCH):
            @pl.when(chunk(i, c)[2])
            def _():
                gh_copy(i, c, h_v, par).wait()

    def gh_start(i, h_v, par):
        for c in range(NCH):
            @pl.when(chunk(i, c)[2])
            def _():
                gh_copy(i, c, h_v, par).start()

    def stage(i, zw, zr, gwr, gr, h_v):
        zw[...] = jnp.dot(enc_rows(i), w_v[...], preferred_element_type=F32)
        for r in range(NCH * CH // 8):
            rows = slice(r * 8, (r + 1) * 8)
            z = zr[rows, :]
            parts = [z[:, j * 128:(j + 1) * 128] for j in range(n_blk)]
            top = functools.reduce(jnp.maximum, parts)
            top_v[rows, :] = top
            sum_v[rows, :] = functools.reduce(jnp.add, [jnp.exp(part - top) for part in parts])
        tops = top_v[...]
        top = jnp.max(tops, axis=1, keepdims=True)
        lse_v[...] = jnp.broadcast_to(top + jnp.log(jnp.sum(sum_v[...] * jnp.exp(tops - top), axis=1, keepdims=True)), (NCH * CH, 128))
        for c in range(NCH):
            b, t0, ok = chunk(i - 1, c)
            rows = slice(c * CH, (c + 1) * CH)
            live = row_ids < jnp.where(ok, in_len[b], 0) - t0
            lse = lse_v[rows, :]
            lacc_v[pl.ds(b, 1), :] += jnp.sum(jnp.where(live, lse, 0.0), axis=0, keepdims=True)
            lse = jnp.where(live, lse, 3.0e38)
            upper = (t0 >= mid).astype(jnp.int32)
            occ = jnp.where(live, eo_v[pl.ds(pl.multiple_of(b * PITCH + t0 - upper * mid, 8), CH), :], 0.0)
            inv = inv_v[pl.ds(pl.multiple_of(b * 8, 8), 8), :] + upper * 64
            for j in range(n_blk):
                cols = slice(j * 128, (j + 1) * 128)
                col_occ = take_lanes(occ, jnp.broadcast_to(inv[j:j + 1], (CH, 128)))
                gwr[rows, cols] = (jnp.exp(zr[rows, cols] - lse) - col_occ).astype(BF16)
        h_v[...] = jnp.dot(gr[...], wt_v[...], preferred_element_type=F32)
        gwt_v[...] += lax.dot_general(gr[:, own], enc_rows(i - 2), (((0,), (0,)), ((), ())), preferred_element_type=F32)

    trips = (n_iter + 3) // 2

    @pl.loop(0, trips)
    def _(ii):
        i = 2 * ii
        slot = lax.rem(ii, 2)
        gh_wait(i - 6, h0_v.at[slot], 2 * slot)
        gh_wait(i - 5, h1_v.at[slot], 2 * slot + 1)
        stage(i, z0_v, z1_v, g1_v, g0_v, h0_v.at[slot])
        stage(i + 1, z1_v, z0_v, g0_v, g1_v, h1_v.at[slot])
        gh_start(i - 2, h0_v.at[slot], 2 * slot)
        gh_start(i - 1, h1_v.at[slot], 2 * slot + 1)

    for back in (2, 1):
        slot = lax.rem(trips - back + 2, 2)
        gh_wait(2 * (trips - back) - 2, h0_v.at[slot], 2 * slot)
        gh_wait(2 * (trips - back) - 1, h1_v.at[slot], 2 * slot + 1)
    gw_ref[...] = gwt_v[...].T
    loss_ref[...] = lacc_v[...].T[0:1, :] - blank_sum - log_z

    @pl.loop(0, n_seq * n_per - n_live)
    def _(_):
        zero_copy(0, 0).wait()


def solution(mesh):
    n_dev = mesh.shape["tp"]

    def device_fn(enc_out, w_loc, labels, in_len, lab_len):
        n_seq, n_frames, hidden = enc_out.shape
        n_lab = labels.shape[1]
        n_cols = w_loc.shape[1]
        n_vocab = n_cols * n_dev
        vmem = pl.BlockSpec(memory_space=pltpu.VMEM)
        smem = pl.BlockSpec(memory_space=pltpu.SMEM)
        anyspace = pl.BlockSpec(memory_space=pl.ANY)
        w_all = pl.pallas_call(
            gather_kernel,
            out_shape=jax.ShapeDtypeStruct((n_dev, hidden, n_cols), BF16),
            in_specs=[vmem],
            out_specs=vmem,
            scratch_shapes=[pltpu.SemaphoreType.DMA((9,)), pltpu.SemaphoreType.DMA((9,))],
            compiler_params=pltpu.CompilerParams(collective_id=0, has_side_effects=True),
            name="gather_w",
        )(w_loc)
        n_per = n_frames // CH
        n_grp = n_seq // 4
        loss, grad_w, grad_hs = pl.pallas_call(
            functools.partial(ctc_kernel, n_seq, n_frames, n_lab),
            out_shape=(
                jax.ShapeDtypeStruct((1, n_seq), F32),
                jax.ShapeDtypeStruct((hidden, n_cols), F32),
                jax.ShapeDtypeStruct((n_seq * n_frames, hidden), F32),
            ),
            in_specs=[smem, vmem, vmem, vmem, anyspace, anyspace],
            out_specs=(vmem, vmem, anyspace),
            scratch_shapes=[
                pltpu.VMEM((n_seq * n_frames, hidden), BF16),
                pltpu.VMEM((hidden, n_vocab), BF16),
                pltpu.VMEM((n_vocab, hidden), BF16),
                pltpu.VMEM((192, n_vocab), BF16),
                pltpu.VMEM((192, n_vocab), BF16),
                pltpu.VMEM((512, hidden), BF16),
                pltpu.VMEM((512, hidden), BF16),
                pltpu.VMEM((n_seq * PITCH, 128), F32),
                pltpu.VMEM((n_frames * 48, 128), F32),
                pltpu.VMEM((n_frames * 104, 128), F32),
                pltpu.VMEM((n_seq * n_dev, 128), jnp.int32),
                pltpu.VMEM((n_seq, 128), jnp.int32),
                pltpu.VMEM((NCH * CH, n_vocab), F32),
                pltpu.VMEM((NCH * CH, n_vocab), F32),
                pltpu.VMEM((NCH * CH, n_vocab), BF16),
                pltpu.VMEM((NCH * CH, n_vocab), BF16),
                pltpu.VMEM((2, NCH * CH, hidden), F32),
                pltpu.VMEM((2, NCH * CH, hidden), F32),
                pltpu.VMEM((NCH * CH, 128), F32),
                pltpu.VMEM((NCH * CH, 128), F32),
                pltpu.VMEM((NCH * CH, 128), F32),
                pltpu.VMEM((n_cols, hidden), F32),
                pltpu.VMEM((n_seq, 128), F32),
                pltpu.VMEM((CH, hidden), F32),
                pltpu.VMEM((8, 128), jnp.int32),
                pltpu.SMEM((n_seq * n_per + 3 * PAD,), jnp.int32),
                pltpu.SMEM((n_seq * n_per + 3 * PAD,), jnp.int32),
                pltpu.SMEM((8, 128), jnp.int32),
                pltpu.SemaphoreType.DMA((n_grp,)),
                pltpu.SemaphoreType.DMA((n_dev,)),
                pltpu.SemaphoreType.DMA((4, NCH)),
                pltpu.SemaphoreType.DMA,
                pltpu.SemaphoreType.DMA,
            ],
            compiler_params=pltpu.CompilerParams(vmem_limit_bytes=63 * 1024 * 1024),
            name="ctc",
        )(in_len, labels.T, in_len.reshape(1, n_seq), lab_len.reshape(1, n_seq), enc_out.reshape(n_seq * n_frames, hidden), w_all)
        return loss.reshape(n_seq), grad_w, grad_hs.reshape(n_seq, n_frames, hidden)

    return jax.shard_map(device_fn, mesh=mesh, in_specs=(P("dp"), P(None, "tp"), P("dp"), P("dp"), P("dp")), out_specs=(P("dp"), P("dp", "tp"), P("dp")), check_vma=False)
```

```python
import functools

import jax
import jax.numpy as jnp
from jax import lax
from jax.experimental import pallas as pl
from jax.experimental.pallas import tpu as pltpu
from jax.sharding import PartitionSpec as P

NEG_FILL = -1.0e30
CH = 32
NCH = 16
PAD = 6 * NCH
PITCH = 136
DUMMY = 55
UNR = 4
AHEAD = 6
MESH = pl.DeviceIdType.MESH
F32 = jnp.float32
BF16 = jnp.bfloat16


def gather_kernel(w_ref, out_ref, send_sem, recv_sem):
    me = lax.axis_index("tp")
    core, col, row = lax.rem(me, 2), lax.rem(me // 2, 2), me // 4
    mate = me + 1 - 2 * core
    across = me + 2 * (1 - 2 * col)
    along = me + 4 * (1 - 2 * row)
    far = across + along - me
    barrier = pltpu.get_barrier_semaphore()
    for peer in (mate, across, along):
        pl.semaphore_signal(barrier, inc=1, device_id={"tp": peer}, device_id_type=MESH)
    pl.semaphore_wait(barrier, 3)
    rows = w_ref.shape[0]
    upper, lower = pl.ds(0, rows // 2), pl.ds(rows // 2, rows // 2)

    def push(k, src, dst, peer):
        copy = pltpu.make_async_remote_copy(
            src_ref=src, dst_ref=dst, send_sem=send_sem.at[k], recv_sem=recv_sem.at[k],
            device_id={"tp": peer}, device_id_type=MESH,
        )
        copy.start()
        return copy

    own = out_ref.at[me]
    copies = [push(1, w_ref, own, across), push(2, w_ref, own, along), push(0, w_ref, own, mate)]
    out_ref[me] = w_ref[...]
    copies[0].wait_recv()
    copies.append(push(4, out_ref.at[across, upper], out_ref.at[across, upper], along))
    copies.append(push(3, out_ref.at[across], out_ref.at[across], mate))
    copies[1].wait_recv()
    copies.append(push(6, out_ref.at[along, lower], out_ref.at[along, lower], across))
    copies.append(push(5, out_ref.at[along], out_ref.at[along], mate))
    copies[3].wait_recv()
    copies.append(push(7, out_ref.at[far, upper], out_ref.at[far, upper], mate))
    copies[5].wait_recv()
    copies.append(push(8, out_ref.at[far, lower], out_ref.at[far, lower], mate))
    for k in (2, 4, 6, 7, 8):
        copies[k].wait_recv()
    for copy in copies:
        copy.wait_send()


def take_lanes(x, idx):
    return jnp.take_along_axis(x, idx, axis=1, mode="promise_in_bounds")


def lse2(a, b):
    top = jnp.maximum(a, b)
    return top + jnp.log(1.0 + jnp.exp(jnp.minimum(a, b) - top))


def ctc_kernel(
    n_seq, n_frames, n_lab,
    in_len, labt_ref, inrow_ref, lenrow_ref, enc_hbm, wg_hbm,
    loss_ref, gw_ref, ghs_hbm,
    enc_v, w_v, wt_v, oh0_v, oh1_v, gl0_v, gl1_v, eo_v, et_v, ab_v, inv_v, nxt_v, z0_v, z1_v, g0_v, g1_v, h0_v, h1_v, top0_v, top1_v, sum0_v, sum1_v, lse0_v, lse1_v, gwt_v, lacc_v, zero_v, flag_v,
    tabb, tabt, flag_s, enc_sem, w_sem, gh_sem, zero_sem, flag_sem,
):
    me = lax.axis_index("tp")
    n_vocab = w_v.shape[1]
    n_blk = n_vocab // 128
    n_grp = n_seq // 4
    mid = n_frames // 2
    n_per = n_frames // CH
    per_mid = mid // CH

    def enc_copy(g):
        rows = pl.ds(pl.multiple_of(4 * g * n_frames, 4 * n_frames), 4 * n_frames)
        return pltpu.make_async_copy(enc_hbm.at[rows], enc_v.at[rows], enc_sem.at[g])

    w_copies = [pltpu.make_async_copy(wg_hbm.at[k], w_v.at[:, pl.ds(k * 128, 128)], w_sem.at[k]) for k in range(n_blk)]
    for copy in w_copies:
        copy.start()

    for g in range(AHEAD):
        enc_copy(g).start()

    for ref in (zero_v, lacc_v, gwt_v, z1_v, lse1_v, g0_v, g1_v):
        ref[...] = jnp.zeros_like(ref)
    sub48 = lax.broadcasted_iota(jnp.int32, (48, 128), 0)
    in_row = inrow_ref[...]
    len_row = lenrow_ref[...]
    lab48 = jnp.where(sub48 < len_row, labt_ref[...], -1 - sub48)
    skip = lab48 != pltpu.roll(lab48, 1, 0)

    nxt = jnp.full((48, 128), DUMMY, jnp.int32)
    later = jnp.zeros((48, 128), jnp.int32)
    for d in range(n_lab - 1, 0, -1):
        same = (pltpu.roll(lab48, 48 - d, 0) == lab48) & (sub48 < 48 - d)
        nxt = jnp.where(same, sub48 + d, nxt)
        later = later + jnp.where(same, 1, 0)
    nxt_f = jnp.concatenate([nxt.astype(F32), jnp.full((16, 128), float(DUMMY), F32)], axis=0)
    nxt_v[...] = jnp.concatenate([nxt_f, nxt_f + 64.0], axis=0).T.astype(jnp.int32)
    flag_v[...] = jnp.broadcast_to(jnp.max(later.astype(F32), axis=0, keepdims=True), (8, 128)).astype(jnp.int32)
    flag_copy = pltpu.make_async_copy(flag_v, flag_s, flag_sem)
    flag_copy.start()

    for copy in w_copies:
        copy.wait()
    wt_v[...] = w_v[...].T
    row16 = lax.broadcasted_iota(jnp.int32, (16, wt_v.shape[1]), 0)
    tail = jnp.where(row16 == 0, wt_v[0:16, :].astype(F32), 0.0).astype(BF16)
    for k in range(8):
        gl0_v[k * 64 + 48:(k + 1) * 64, :] = tail
        gl1_v[k * 64 + 48:(k + 1) * 64, :] = tail

    lane48 = lax.broadcasted_iota(jnp.int32, (48, 128), 1)
    sub48f = sub48.astype(F32)
    lane1 = lax.broadcasted_iota(jnp.int32, (1, 128), 1)
    lane_mid = lax.broadcasted_iota(jnp.int32, (mid, 128), 1)

    def list_group(g, n):
        for k in range(4):
            b = 4 * g + k
            cnt = (in_len[jnp.minimum(b, n_seq - 1)] + CH - 1) // CH
            dead = n_seq * n_per - 1 - (b * n_per - n)
            for j in range(n_per):
                slot = jnp.where(g < n_grp, PAD + jnp.where(j < cnt, n + j, dead - (j - cnt)), j)
                tabb[slot] = b
                tabt[slot] = j * CH
            n = n + jnp.where(g < n_grp, cnt, 0)
        return n

    def build_hot(g, oh_v):
        for k in range(4):
            b = 4 * g + k
            col = take_lanes(lab48, jnp.full((48, 128), b, jnp.int32))
            firsts = []
            for j in range(n_blk):
                hit = col == lane48 + 128 * j
                oh_v[k * 48:(k + 1) * 48, j * 128:(j + 1) * 128] = jnp.where(hit, 1.0, 0.0).astype(BF16)
                start = jnp.where(lane1 == 0, 48.0, float(DUMMY)) if j == 0 else float(DUMMY)
                firsts.append(jnp.minimum(jnp.min(jnp.where(hit, sub48f, float(DUMMY)), axis=0, keepdims=True), start))
            inv_v[pl.ds(pl.multiple_of(b * 8, 8), 8), :] = jnp.concatenate(firsts, axis=0).astype(jnp.int32)

    def pick_cols(oh_v, gl_v):
        picked = jnp.dot(oh_v[...], wt_v[...], preferred_element_type=F32).astype(BF16)
        for k in range(4):
            for h in range(2):
                gl_v[k * 128 + h * 64:k * 128 + h * 64 + 48, :] = picked[k * 48:(k + 1) * 48]

    def emit_group(g, gl_v):
        for k in range(4):
            b = 4 * g + k
            x = enc_v[pl.ds(pl.multiple_of(b * n_frames, n_frames), n_frames), :]
            e = lax.dot_general(x, gl_v[k * 128:(k + 1) * 128, :], (((1,), (1,)), ((), ())), preferred_element_type=F32)
            eo_v[pl.ds(b, mid, stride=PITCH), :] = jnp.where(lane_mid < 64, e[0:mid], e[mid:n_frames])

    build_hot(0, oh0_v)

    def emit_pair(ii, n):
        for s in range(2):
            g = 2 * ii + s

            @pl.when((g >= 1) & (g <= n_grp))
            def _():
                enc_copy(g - 1).wait()

            @pl.when(g + AHEAD < n_grp)
            def _():
                enc_copy(g + AHEAD).start()
        n = list_group(2 * ii + 1, list_group(2 * ii, n))
        for s in range(2):
            g = 2 * ii + s
            build_hot(jnp.minimum(g + 1, n_grp - 1), (oh1_v, oh0_v)[s])
            pick_cols((oh0_v, oh1_v)[s], (gl0_v, gl1_v)[s])
            emit_group(jnp.clip(g - 1, 0, n_grp - 1), (gl1_v, gl0_v)[s])
        return n

    n_live = lax.fori_loop(0, n_grp // 2 + 1, emit_pair, 0)
    for j in range(PAD):
        for base in (0, PAD + n_seq * n_per):
            tabb[base + j] = 0
            tabt[base + j] = 0
    n_iter = (n_live + NCH - 1) // NCH

    def zero_copy(k):
        row = pl.multiple_of(tabb[PAD + k] * n_frames + tabt[PAD + k], CH)
        return pltpu.make_async_copy(zero_v, ghs_hbm.at[pl.ds(row, CH)], zero_sem)

    @pl.loop(n_iter * NCH, n_seq * n_per)
    def _(k):
        zero_copy(k).start()

    def turn_emissions(jj, acc):
        for u in range(UNR):
            j = jj * UNR + u
            turned = eo_v[pl.ds(pl.multiple_of(j * PITCH, 8), n_seq), :].T
            low = turned[48:49]
            high = turned[112:113]
            et_v[pl.ds(pl.multiple_of(j * 48, 8), 48), :] = turned[0:48] - low
            et_v[pl.ds(pl.multiple_of((j + mid) * 48, 8), 48), :] = turned[64:112] - high
            acc = acc + jnp.where(j < in_row, low, 0.0) + jnp.where(j + mid < in_row, high, 0.0)
        return acc

    blank_sum = lax.fori_loop(0, mid // UNR, turn_emissions, jnp.zeros((1, 128), F32))

    neg8 = jnp.full((8, 128), NEG_FILL, F32)
    sub56 = lax.broadcasted_iota(jnp.int32, (56, 128), 0)

    def emit_at(t):
        return et_v[pl.ds(pl.multiple_of(t * 48, 8), 48), :]

    def alpha_step(t, blk, lab):
        shifted = pltpu.roll(jnp.concatenate([lab, neg8], axis=0), 1, 0)
        blk_new = lse2(blk, shifted)
        via = jnp.where(skip, blk_new[0:48], blk[0:48])
        lab_new = lse2(lab, via) + emit_at(t)
        live = t < in_row
        return jnp.where(live, blk_new, blk), jnp.where(live, lab_new, lab)

    def beta_step(t, blk, lab):
        emitted = lab + emit_at(t + 1)
        blk_new = lse2(blk, jnp.concatenate([emitted, neg8], axis=0))
        via = jnp.concatenate([jnp.where(skip, blk_new[0:48], blk[0:48]), blk_new[48:56]], axis=0)
        lab_new = lse2(emitted, pltpu.roll(via, 55, 0)[0:48])
        live = t + 1 < in_row
        return jnp.where(live, blk_new, blk), jnp.where(live, lab_new, lab)

    def keep(t, blk, lab):
        row = pl.multiple_of(t * 104, 8)
        ab_v[pl.ds(row, 56), :] = blk
        ab_v[pl.ds(row + 56, 48), :] = lab

    a_blk = jnp.where(sub56 == 0, 0.0, NEG_FILL).astype(F32) + jnp.zeros((56, 128), F32)
    a_lab = jnp.full((48, 128), NEG_FILL, F32)
    b_blk = jnp.where(sub56 == len_row, 0.0, NEG_FILL).astype(F32)
    b_lab = jnp.where(sub48 == len_row - 1, 0.0, NEG_FILL).astype(F32)

    a_blk, a_lab = alpha_step(0, a_blk, a_lab)
    keep(0, a_blk, a_lab)
    keep(n_frames - 1, b_blk, b_lab)

    def first_half(k, state):
        a_blk, a_lab, b_blk, b_lab = state
        a_blk, a_lab = alpha_step(k, a_blk, a_lab)
        keep(k, a_blk, a_lab)
        t = n_frames - 1 - k
        b_blk, b_lab = beta_step(t, b_blk, b_lab)
        keep(t, b_blk, b_lab)
        return a_blk, a_lab, b_blk, b_lab

    a_blk, a_lab, b_blk, b_lab = lax.fori_loop(1, mid, first_half, (a_blk, a_lab, b_blk, b_lab))

    m_blk, m_lab = beta_step(mid - 1, b_blk, b_lab)
    s_blk = a_blk + m_blk
    s_lab = a_lab + m_lab
    top = jnp.maximum(jnp.max(s_blk, axis=0, keepdims=True), jnp.max(s_lab, axis=0, keepdims=True))
    total = jnp.sum(jnp.exp(s_blk - top), axis=0, keepdims=True) + jnp.sum(jnp.exp(s_lab - top), axis=0, keepdims=True)
    log_z = top + jnp.log(total)
    sub8 = lax.broadcasted_iota(jnp.int32, (8, 128), 0)

    def put_occ(t, blk, lab):
        row = pl.multiple_of(t * 104, 8)
        occ_blk = jnp.sum(jnp.exp(ab_v[pl.ds(row, 56), :] + (blk - log_z)), axis=0, keepdims=True)
        occ_lab = jnp.exp(ab_v[pl.ds(row + 56, 48), :] + (lab - log_z))
        ab_v[pl.ds(row, 48), :] = occ_lab
        ab_v[pl.ds(row + 48, 8), :] = jnp.where(sub8 == 0, occ_blk, 0.0)

    def second_half(k, state):
        a_blk, a_lab, b_blk, b_lab = state
        t = n_frames - 1 - k
        put_occ(k - 1, a_blk, a_lab)
        put_occ(t + 1, b_blk, b_lab)
        a_blk, a_lab = alpha_step(k, a_blk, a_lab)
        b_blk, b_lab = beta_step(t, b_blk, b_lab)
        return a_blk, a_lab, b_blk, b_lab

    a_blk, a_lab = alpha_step(mid, a_blk, a_lab)
    a_blk, a_lab, b_blk, b_lab = lax.fori_loop(mid + 1, n_frames, second_half, (a_blk, a_lab, m_blk, m_lab))
    put_occ(n_frames - 1, a_blk, a_lab)
    put_occ(0, b_blk, b_lab)

    zero8 = jnp.zeros((8, 128), F32)

    @pl.loop(0, mid // UNR)
    def _(jj):
        for u in range(UNR):
            j = jj * UNR + u
            low = ab_v[pl.ds(pl.multiple_of(j * 104, 8), 56), :]
            high = ab_v[pl.ds(pl.multiple_of((j + mid) * 104, 8), 56), :]
            turned = jnp.concatenate([low, zero8, high, zero8], axis=0).T
            eo_v[pl.ds(pl.multiple_of(j * PITCH, 8), n_seq), :] = turned + take_lanes(turned, nxt_v[...])

    flag_copy.wait()

    def more_rounds(b):
        @pl.when(flag_s[0, b] > 1)
        def _():
            rows = pl.ds(b, mid, stride=PITCH)
            count = flag_s[0, b]
            rounds = sum((count >= 2 ** r).astype(jnp.int32) for r in range(1, 6))

            def more(_, link):
                link = take_lanes(link, link)
                occ = eo_v[rows, :]
                eo_v[rows, :] = occ + take_lanes(occ, jnp.broadcast_to(link[0:1], (mid, 128)))
                return link

            lax.fori_loop(0, rounds, more, jnp.broadcast_to(nxt_v[pl.ds(b, 1), :], (8, 128)))

    @pl.loop(0, n_seq // 16)
    def _(bb):
        most = functools.reduce(jnp.maximum, [flag_s[0, bb * 16 + u] for u in range(16)])

        @pl.when(most > 1)
        def _():
            @pl.loop(0, 16)
            def _(u):
                more_rounds(bb * 16 + u)

    row_ids = lax.broadcasted_iota(jnp.int32, (CH, 128), 0)
    own = pl.ds(pl.multiple_of(me * 128, 128), 128)

    def chunk(i, c):
        idx = i * NCH + c
        return tabb[idx + PAD], tabt[idx + PAD], (i >= 0) & (i < n_iter)

    def enc_rows(i):
        parts = []
        for c in range(NCH):
            b, t0, _ = chunk(i, c)
            parts.append(enc_v[pl.ds(pl.multiple_of(b * n_frames + t0, CH), CH), :])
        return jnp.concatenate(parts, axis=0)

    def gh_wait(i, h_v, par):
        @pl.when((i >= 0) & (i < n_iter))
        def _():
            pltpu.make_async_copy(h_v, ghs_hbm.at[pl.ds(0, NCH * CH)], gh_sem.at[par]).wait()

    def gh_start(i, h_v, par):
        @pl.when((i >= 0) & (i < n_iter))
        def _():
            for c in range(NCH):
                b, t0, _ = chunk(i, c)
                row = pl.multiple_of(b * n_frames + t0, CH)
                pltpu.make_async_copy(h_v.at[pl.ds(c * CH, CH)], ghs_hbm.at[pl.ds(row, CH)], gh_sem.at[par]).start()

    def stage(i, zw, zr, lse_w, lse_r, top_v, sum_v, gwr, gr, h_v):
        zw[...] = jnp.dot(enc_rows(i), w_v[...], preferred_element_type=F32)
        h_v[...] = jnp.dot(gr[...], wt_v[...], preferred_element_type=F32)
        gwt_v[...] += lax.dot_general(gr[:, own], enc_rows(i - 2), (((0,), (0,)), ((), ())), preferred_element_type=F32)
        for c in range(NCH):
            b, t0, ok = chunk(i - 1, c)
            rows = slice(c * CH, (c + 1) * CH)
            live = row_ids < jnp.where(ok, in_len[b], 0) - t0
            lse = lse_r[rows, :]
            lacc_v[pl.ds(b, 1), :] += jnp.sum(jnp.where(live, lse, 0.0), axis=0, keepdims=True)
            lse = jnp.where(live, lse, 3.0e38)
            upper = (t0 >= mid).astype(jnp.int32)
            occ = jnp.where(live, eo_v[pl.ds(b + (t0 - upper * mid) * PITCH, CH, stride=PITCH), :], 0.0)
            inv = inv_v[pl.ds(pl.multiple_of(b * 8, 8), 8), :] + upper * 64
            for j in range(n_blk):
                cols = slice(j * 128, (j + 1) * 128)
                col_occ = take_lanes(occ, jnp.broadcast_to(inv[j:j + 1], (CH, 128)))
                gwr[rows, cols] = (jnp.exp(zr[rows, cols] - lse) - col_occ).astype(BF16)
        for r in range(NCH * CH // 8):
            rows = slice(r * 8, (r + 1) * 8)
            z = zw[rows, :]
            parts = [z[:, j * 128:(j + 1) * 128] for j in range(n_blk)]
            top = functools.reduce(jnp.maximum, parts)
            top_v[rows, :] = top
            sum_v[rows, :] = functools.reduce(jnp.add, [jnp.exp(part - top) for part in parts])
        tops = top_v[...]
        top = jnp.max(tops, axis=1, keepdims=True)
        lse_w[...] = jnp.broadcast_to(top + jnp.log(jnp.sum(sum_v[...] * jnp.exp(tops - top), axis=1, keepdims=True)), (NCH * CH, 128))

    trips = (n_iter + 3) // 2

    @pl.loop(0, trips)
    def _(ii):
        i = 2 * ii
        slot = lax.rem(ii, 2)
        gh_wait(i - 6, h0_v.at[slot], 2 * slot)
        gh_wait(i - 5, h1_v.at[slot], 2 * slot + 1)
        stage(i, z0_v, z1_v, lse0_v, lse1_v, top0_v, sum0_v, g1_v, g0_v, h0_v.at[slot])
        stage(i + 1, z1_v, z0_v, lse1_v, lse0_v, top1_v, sum1_v, g0_v, g1_v, h1_v.at[slot])
        gh_start(i - 2, h0_v.at[slot], 2 * slot)
        gh_start(i - 1, h1_v.at[slot], 2 * slot + 1)

    for back in (2, 1):
        slot = lax.rem(trips - back + 2, 2)
        gh_wait(2 * (trips - back) - 2, h0_v.at[slot], 2 * slot)
        gh_wait(2 * (trips - back) - 1, h1_v.at[slot], 2 * slot + 1)
    gw_ref[...] = gwt_v[...].T
    loss_ref[...] = lacc_v[...].T[0:1, :] - blank_sum - log_z

    @pl.loop(n_iter * NCH, n_seq * n_per)
    def _(k):
        zero_copy(k).wait()


def solution(mesh):
    n_dev = mesh.shape["tp"]

    def device_fn(enc_out, w_loc, labels, in_len, lab_len):
        n_seq, n_frames, hidden = enc_out.shape
        n_lab = labels.shape[1]
        n_cols = w_loc.shape[1]
        n_vocab = n_cols * n_dev
        vmem = pl.BlockSpec(memory_space=pltpu.VMEM)
        smem = pl.BlockSpec(memory_space=pltpu.SMEM)
        anyspace = pl.BlockSpec(memory_space=pl.ANY)
        w_all = pl.pallas_call(
            gather_kernel,
            out_shape=jax.ShapeDtypeStruct((n_dev, hidden, n_cols), BF16),
            in_specs=[vmem],
            out_specs=vmem,
            scratch_shapes=[pltpu.SemaphoreType.DMA((9,)), pltpu.SemaphoreType.DMA((9,))],
            compiler_params=pltpu.CompilerParams(collective_id=0, has_side_effects=True),
            name="gather_w",
        )(w_loc)
        n_per = n_frames // CH
        n_grp = n_seq // 4
        loss, grad_w, grad_hs = pl.pallas_call(
            functools.partial(ctc_kernel, n_seq, n_frames, n_lab),
            out_shape=(
                jax.ShapeDtypeStruct((1, n_seq), F32),
                jax.ShapeDtypeStruct((hidden, n_cols), F32),
                jax.ShapeDtypeStruct((n_seq * n_frames, hidden), F32),
            ),
            in_specs=[smem, vmem, vmem, vmem, anyspace, anyspace],
            out_specs=(vmem, vmem, anyspace),
            scratch_shapes=[
                pltpu.VMEM((n_seq * n_frames, hidden), BF16),
                pltpu.VMEM((hidden, n_vocab), BF16),
                pltpu.VMEM((n_vocab, hidden), BF16),
                pltpu.VMEM((192, n_vocab), BF16),
                pltpu.VMEM((192, n_vocab), BF16),
                pltpu.VMEM((512, hidden), BF16),
                pltpu.VMEM((512, hidden), BF16),
                pltpu.VMEM((n_frames // 2 * PITCH, 128), F32),
                pltpu.VMEM((n_frames * 48, 128), F32),
                pltpu.VMEM((n_frames * 104, 128), F32),
                pltpu.VMEM((n_seq * n_dev, 128), jnp.int32),
                pltpu.VMEM((n_seq, 128), jnp.int32),
                pltpu.VMEM((NCH * CH, n_vocab), F32),
                pltpu.VMEM((NCH * CH, n_vocab), F32),
                pltpu.VMEM((NCH * CH, n_vocab), BF16),
                pltpu.VMEM((NCH * CH, n_vocab), BF16),
                pltpu.VMEM((2, NCH * CH, hidden), F32),
                pltpu.VMEM((2, NCH * CH, hidden), F32),
                pltpu.VMEM((NCH * CH, 128), F32),
                pltpu.VMEM((NCH * CH, 128), F32),
                pltpu.VMEM((NCH * CH, 128), F32),
                pltpu.VMEM((NCH * CH, 128), F32),
                pltpu.VMEM((NCH * CH, 128), F32),
                pltpu.VMEM((NCH * CH, 128), F32),
                pltpu.VMEM((n_cols, hidden), F32),
                pltpu.VMEM((n_seq, 128), F32),
                pltpu.VMEM((CH, hidden), F32),
                pltpu.VMEM((8, 128), jnp.int32),
                pltpu.SMEM((n_seq * n_per + 3 * PAD,), jnp.int32),
                pltpu.SMEM((n_seq * n_per + 3 * PAD,), jnp.int32),
                pltpu.SMEM((8, 128), jnp.int32),
                pltpu.SemaphoreType.DMA((n_grp,)),
                pltpu.SemaphoreType.DMA((n_dev,)),
                pltpu.SemaphoreType.DMA((4,)),
                pltpu.SemaphoreType.DMA,
                pltpu.SemaphoreType.DMA,
            ],
            compiler_params=pltpu.CompilerParams(vmem_limit_bytes=63 * 1024 * 1024),
            name="ctc",
        )(in_len, labels.T, in_len.reshape(1, n_seq), lab_len.reshape(1, n_seq), enc_out.reshape(n_seq * n_frames, hidden), w_all)
        return loss.reshape(n_seq), grad_w, grad_hs.reshape(n_seq, n_frames, hidden)

    return jax.shard_map(device_fn, mesh=mesh, in_specs=(P("dp"), P(None, "tp"), P("dp"), P("dp"), P("dp")), out_specs=(P("dp"), P("dp", "tp"), P("dp")), check_vma=False)
```

```python
import functools

import jax
import jax.numpy as jnp
from jax import lax
from jax.experimental import pallas as pl
from jax.experimental.pallas import tpu as pltpu
from jax.sharding import PartitionSpec as P

NEG_FILL = -1.0e30
CH = 32
NCH = 16
PAD = 6 * NCH
PITCH = 136
DUMMY = 55
AHEAD = 6
MESH = pl.DeviceIdType.MESH
F32 = jnp.float32
BF16 = jnp.bfloat16


def gather_kernel(w_ref, out_ref, send_sem, recv_sem):
    me = lax.axis_index("tp")
    core, col, row = lax.rem(me, 2), lax.rem(me // 2, 2), me // 4
    mate = me + 1 - 2 * core
    across = me + 2 * (1 - 2 * col)
    along = me + 4 * (1 - 2 * row)
    far = across + along - me
    barrier = pltpu.get_barrier_semaphore()
    for peer in (mate, across, along):
        pl.semaphore_signal(barrier, inc=1, device_id={"tp": peer}, device_id_type=MESH)
    pl.semaphore_wait(barrier, 3)
    rows = w_ref.shape[0]
    upper, lower = pl.ds(0, rows // 2), pl.ds(rows // 2, rows // 2)

    def push(k, src, dst, peer):
        copy = pltpu.make_async_remote_copy(
            src_ref=src, dst_ref=dst, send_sem=send_sem.at[k], recv_sem=recv_sem.at[k],
            device_id={"tp": peer}, device_id_type=MESH,
        )
        copy.start()
        return copy

    own = out_ref.at[me]
    copies = [push(1, w_ref, own, across), push(2, w_ref, own, along), push(0, w_ref, own, mate)]
    out_ref[me] = w_ref[...]
    copies[0].wait_recv()
    copies.append(push(4, out_ref.at[across, upper], out_ref.at[across, upper], along))
    copies.append(push(3, out_ref.at[across], out_ref.at[across], mate))
    copies[1].wait_recv()
    copies.append(push(6, out_ref.at[along, lower], out_ref.at[along, lower], across))
    copies.append(push(5, out_ref.at[along], out_ref.at[along], mate))
    copies[3].wait_recv()
    copies.append(push(7, out_ref.at[far, upper], out_ref.at[far, upper], mate))
    copies[5].wait_recv()
    copies.append(push(8, out_ref.at[far, lower], out_ref.at[far, lower], mate))
    for k in (2, 4, 6, 7, 8):
        copies[k].wait_recv()
    for copy in copies:
        copy.wait_send()


def take_lanes(x, idx):
    return jnp.take_along_axis(x, idx, axis=1, mode="promise_in_bounds")


def lse2(a, b):
    top = jnp.maximum(a, b)
    return top + jnp.log(1.0 + jnp.exp(jnp.minimum(a, b) - top))


def ctc_kernel(
    n_seq, n_frames, n_lab,
    in_len, labt_ref, inrow_ref, lenrow_ref, enc_hbm, wg_hbm,
    loss_ref, gw_ref, ghs_hbm,
    enc_v, w_v, wt_v, oh0_v, oh1_v, gl0_v, gl1_v, eo_v, et_v, ab_v, inv_v, nxt_v, z0_v, z1_v, g0_v, g1_v, h0_v, h1_v, top0_v, top1_v, sum0_v, sum1_v, lse0_v, lse1_v, gwt_v, lacc_v, zero_v, flag_v,
    tabb, tabt, rep_s, flag_s, enc_sem, w_sem, gh_sem, zero_sem, flag_sem,
):
    me = lax.axis_index("tp")
    n_vocab = w_v.shape[1]
    n_blk = n_vocab // 128
    n_grp = n_seq // 4
    mid = n_frames // 2
    n_per = n_frames // CH
    per_mid = mid // CH

    def enc_copy(g):
        rows = pl.ds(pl.multiple_of(4 * g * n_frames, 4 * n_frames), 4 * n_frames)
        return pltpu.make_async_copy(enc_hbm.at[rows], enc_v.at[rows], enc_sem.at[g])

    w_copies = [pltpu.make_async_copy(wg_hbm.at[k], w_v.at[:, pl.ds(k * 128, 128)], w_sem.at[k]) for k in range(n_blk)]
    for copy in w_copies:
        copy.start()

    for g in range(AHEAD):
        enc_copy(g).start()

    for ref in (zero_v, lacc_v, gwt_v, z1_v, lse1_v, g0_v, g1_v):
        ref[...] = jnp.zeros_like(ref)
    sub48 = lax.broadcasted_iota(jnp.int32, (48, 128), 0)
    in_row = inrow_ref[...]
    len_row = lenrow_ref[...]
    lab48 = jnp.where(sub48 < len_row, labt_ref[...], -1 - sub48)
    skip = lab48 != pltpu.roll(lab48, 1, 0)

    nxt = jnp.full((48, 128), DUMMY, jnp.int32)
    later = jnp.zeros((48, 128), jnp.int32)
    for d in range(n_lab - 1, 0, -1):
        same = (pltpu.roll(lab48, 48 - d, 0) == lab48) & (sub48 < 48 - d)
        nxt = jnp.where(same, sub48 + d, nxt)
        later = later + jnp.where(same, 1, 0)
    nxt_f = jnp.concatenate([nxt.astype(F32), jnp.full((16, 128), float(DUMMY), F32)], axis=0)
    nxt_v[0:n_seq] = jnp.concatenate([nxt_f, nxt_f + 64.0], axis=0).T.astype(jnp.int32)
    nxt_v[n_seq:n_seq + 8] = jnp.full((8, 128), DUMMY, jnp.int32)
    flag_v[...] = jnp.broadcast_to(jnp.max(later.astype(F32), axis=0, keepdims=True), (8, 128)).astype(jnp.int32)
    flag_copy = pltpu.make_async_copy(flag_v, flag_s, flag_sem)
    flag_copy.start()

    for copy in w_copies:
        copy.wait()
    wt_v[...] = w_v[...].T
    row16 = lax.broadcasted_iota(jnp.int32, (16, wt_v.shape[1]), 0)
    tail = jnp.where(row16 == 0, wt_v[0:16, :].astype(F32), 0.0).astype(BF16)
    for k in range(8):
        gl0_v[k * 64 + 48:(k + 1) * 64, :] = tail
        gl1_v[k * 64 + 48:(k + 1) * 64, :] = tail

    lane48 = lax.broadcasted_iota(jnp.int32, (48, 128), 1)
    sub48f = sub48.astype(F32)
    lane1 = lax.broadcasted_iota(jnp.int32, (1, 128), 1)
    lane_mid = lax.broadcasted_iota(jnp.int32, (mid, 128), 1)

    def list_group(g, n):
        for k in range(4):
            b = 4 * g + k
            cnt = (in_len[jnp.minimum(b, n_seq - 1)] + CH - 1) // CH
            dead = n_seq * n_per - 1 - (b * n_per - n)
            for j in range(n_per):
                slot = jnp.where(g < n_grp, PAD + jnp.where(j < cnt, n + j, dead - (j - cnt)), j)
                tabb[slot] = b
                tabt[slot] = j * CH
            n = n + jnp.where(g < n_grp, cnt, 0)
        return n

    def build_hot(g, oh_v):
        for k in range(4):
            b = 4 * g + k
            col = take_lanes(lab48, jnp.full((48, 128), b, jnp.int32))
            firsts = []
            for j in range(n_blk):
                hit = col == lane48 + 128 * j
                oh_v[k * 48:(k + 1) * 48, j * 128:(j + 1) * 128] = jnp.where(hit, 1.0, 0.0).astype(BF16)
                start = jnp.where(lane1 == 0, 48.0, float(DUMMY)) if j == 0 else float(DUMMY)
                firsts.append(jnp.minimum(jnp.min(jnp.where(hit, sub48f, float(DUMMY)), axis=0, keepdims=True), start))
            inv_v[pl.ds(pl.multiple_of(b * 8, 8), 8), :] = jnp.concatenate(firsts, axis=0).astype(jnp.int32)

    def pick_cols(oh_v, gl_v):
        picked = jnp.dot(oh_v[...], wt_v[...], preferred_element_type=F32).astype(BF16)
        for k in range(4):
            for h in range(2):
                gl_v[k * 128 + h * 64:k * 128 + h * 64 + 48, :] = picked[k * 48:(k + 1) * 48]

    def emit_group(g, gl_v):
        for k in range(4):
            b = 4 * g + k
            x = enc_v[pl.ds(pl.multiple_of(b * n_frames, n_frames), n_frames), :]
            e = lax.dot_general(x, gl_v[k * 128:(k + 1) * 128, :], (((1,), (1,)), ((), ())), preferred_element_type=F32)
            eo_v[pl.ds(b, mid, stride=PITCH), :] = jnp.where(lane_mid < 64, e[0:mid], e[mid:n_frames])

    build_hot(0, oh0_v)

    def emit_pair(ii, n):
        for s in range(2):
            g = 2 * ii + s

            @pl.when((g >= 1) & (g <= n_grp))
            def _():
                enc_copy(g - 1).wait()

            @pl.when(g + AHEAD < n_grp)
            def _():
                enc_copy(g + AHEAD).start()
        n = list_group(2 * ii + 1, list_group(2 * ii, n))
        for s in range(2):
            g = 2 * ii + s
            build_hot(jnp.minimum(g + 1, n_grp - 1), (oh1_v, oh0_v)[s])
            pick_cols((oh0_v, oh1_v)[s], (gl0_v, gl1_v)[s])
            emit_group(jnp.clip(g - 1, 0, n_grp - 1), (gl1_v, gl0_v)[s])
        return n

    n_live = lax.fori_loop(0, n_grp // 2 + 1, emit_pair, 0)
    for j in range(PAD):
        for base in (0, PAD + n_seq * n_per):
            tabb[base + j] = 0
            tabt[base + j] = 0
    n_iter = (n_live + NCH - 1) // NCH

    def zero_copy(k):
        row = pl.multiple_of(tabb[PAD + k] * n_frames + tabt[PAD + k], CH)
        return pltpu.make_async_copy(zero_v, ghs_hbm.at[pl.ds(row, CH)], zero_sem)

    @pl.loop(n_iter * NCH, n_seq * n_per)
    def _(k):
        zero_copy(k).start()

    def turn_in(j, acc):
        turned = eo_v[pl.ds(pl.multiple_of(j * PITCH, 8), n_seq), :].T
        low = turned[48:49]
        high = turned[112:113]
        et_v[pl.ds(pl.multiple_of(j * 48, 8), 48), :] = turned[0:48] - low
        et_v[pl.ds(pl.multiple_of((j + mid) * 48, 8), 48), :] = turned[64:112] - high
        return acc + jnp.where(j < in_row, low, 0.0) + jnp.where(j + mid < in_row, high, 0.0)

    blank_sum = jnp.zeros((1, 128), F32)
    for j in (0, 1, mid - 1):
        blank_sum = turn_in(j, blank_sum)

    neg8 = jnp.full((8, 128), NEG_FILL, F32)
    sub56 = lax.broadcasted_iota(jnp.int32, (56, 128), 0)

    def emit_at(t):
        return et_v[pl.ds(pl.multiple_of(t * 48, 8), 48), :]

    def alpha_step(t, blk, lab):
        shifted = pltpu.roll(jnp.concatenate([lab, neg8], axis=0), 1, 0)
        blk_new = lse2(blk, shifted)
        via = jnp.where(skip, blk_new[0:48], blk[0:48])
        lab_new = lse2(lab, via) + emit_at(t)
        live = t < in_row
        return jnp.where(live, blk_new, blk), jnp.where(live, lab_new, lab)

    def beta_step(t, blk, lab):
        emitted = lab + emit_at(t + 1)
        blk_new = lse2(blk, jnp.concatenate([emitted, neg8], axis=0))
        via = jnp.concatenate([jnp.where(skip, blk_new[0:48], blk[0:48]), blk_new[48:56]], axis=0)
        lab_new = lse2(emitted, pltpu.roll(via, 55, 0)[0:48])
        live = t + 1 < in_row
        return jnp.where(live, blk_new, blk), jnp.where(live, lab_new, lab)

    def keep(t, blk, lab):
        row = pl.multiple_of(t * 104, 8)
        ab_v[pl.ds(row, 56), :] = blk
        ab_v[pl.ds(row + 56, 48), :] = lab

    a_blk = jnp.where(sub56 == 0, 0.0, NEG_FILL).astype(F32) + jnp.zeros((56, 128), F32)
    a_lab = jnp.full((48, 128), NEG_FILL, F32)
    b_blk = jnp.where(sub56 == len_row, 0.0, NEG_FILL).astype(F32)
    b_lab = jnp.where(sub48 == len_row - 1, 0.0, NEG_FILL).astype(F32)

    a_blk, a_lab = alpha_step(0, a_blk, a_lab)
    keep(0, a_blk, a_lab)
    keep(n_frames - 1, b_blk, b_lab)

    def first_half(k, state):
        a_blk, a_lab, b_blk, b_lab = state
        a_blk, a_lab = alpha_step(k, a_blk, a_lab)
        keep(k, a_blk, a_lab)
        t = n_frames - 1 - k
        b_blk, b_lab = beta_step(t, b_blk, b_lab)
        keep(t, b_blk, b_lab)
        return a_blk, a_lab, b_blk, b_lab

    def first_quarter(k, state):
        new = first_half(k, state[:4])
        return (*new, turn_in(mid - 1 - k, turn_in(k + 1, state[4])))

    quarter = mid // 2
    a_blk, a_lab, b_blk, b_lab, blank_sum = lax.fori_loop(1, quarter - 1, first_quarter, (a_blk, a_lab, b_blk, b_lab, blank_sum))
    blank_sum = turn_in(quarter, blank_sum)

    flag_copy.wait()

    def second_quarter(k, state):
        n = state[4]
        for u in range(3):
            b = jnp.minimum(3 * (k - quarter + 1) + u, n_seq)
            rep_s[n] = b
            n = n + jnp.where((b < n_seq) & (flag_s[0, jnp.minimum(b, n_seq - 1)] > 0), 1, 0)
        return (*first_half(k, state[:4]), n)

    a_blk, a_lab, b_blk, b_lab, n_rep = lax.fori_loop(quarter - 1, mid, second_quarter, (a_blk, a_lab, b_blk, b_lab, 0))
    for u in range(4):
        rep_s[n_rep + u] = n_seq

    m_blk, m_lab = beta_step(mid - 1, b_blk, b_lab)
    s_blk = a_blk + m_blk
    s_lab = a_lab + m_lab
    top = jnp.maximum(jnp.max(s_blk, axis=0, keepdims=True), jnp.max(s_lab, axis=0, keepdims=True))
    total = jnp.sum(jnp.exp(s_blk - top), axis=0, keepdims=True) + jnp.sum(jnp.exp(s_lab - top), axis=0, keepdims=True)
    log_z = top + jnp.log(total)
    sub8 = lax.broadcasted_iota(jnp.int32, (8, 128), 0)

    def put_occ(t, blk, lab):
        row = pl.multiple_of(t * 104, 8)
        occ_blk = jnp.sum(jnp.exp(ab_v[pl.ds(row, 56), :] + (blk - log_z)), axis=0, keepdims=True)
        occ_lab = jnp.exp(ab_v[pl.ds(row + 56, 48), :] + (lab - log_z))
        ab_v[pl.ds(row, 48), :] = occ_lab
        ab_v[pl.ds(row + 48, 8), :] = jnp.where(sub8 == 0, occ_blk, 0.0)

    zero8 = jnp.zeros((8, 128), F32)

    def turn_out(j):
        low = ab_v[pl.ds(pl.multiple_of(j * 104, 8), 56), :]
        high = ab_v[pl.ds(pl.multiple_of((j + mid) * 104, 8), 56), :]
        turned = jnp.concatenate([low, zero8, high, zero8], axis=0).T
        eo_v[pl.ds(pl.multiple_of(j * PITCH, 8), n_seq), :] = turned

    def second_half(k, state):
        a_blk, a_lab, b_blk, b_lab = state
        t = n_frames - 1 - k
        put_occ(k - 1, a_blk, a_lab)
        put_occ(t + 1, b_blk, b_lab)
        a_blk, a_lab = alpha_step(k, a_blk, a_lab)
        b_blk, b_lab = beta_step(t, b_blk, b_lab)
        return a_blk, a_lab, b_blk, b_lab

    def last_quarter(k, state):
        turn_out(k - 2 - mid)
        turn_out(n_frames + 1 - k)
        return second_half(k, state)

    a_blk, a_lab = alpha_step(mid, a_blk, a_lab)
    state = lax.fori_loop(mid + 1, mid + quarter + 2, second_half, (a_blk, a_lab, m_blk, m_lab))
    a_blk, a_lab, b_blk, b_lab = lax.fori_loop(mid + quarter + 2, n_frames, last_quarter, state)
    put_occ(n_frames - 1, a_blk, a_lab)
    put_occ(0, b_blk, b_lab)
    for j in (mid - 2, 1, mid - 1, 0):
        turn_out(j)

    @pl.loop(0, (n_rep + 3) // 4)
    def _(q):
        seqs = [rep_s[4 * q + u] for u in range(4)]
        occs = [eo_v[pl.ds(b, mid, stride=PITCH), :] for b in seqs]
        links = [nxt_v[pl.ds(b, 1), :] for b in seqs]
        for b, occ, link in zip(seqs, occs, links):
            eo_v[pl.ds(b, mid, stride=PITCH), :] = occ + take_lanes(occ, jnp.broadcast_to(link, (mid, 128)))

    @pl.loop(0, n_rep)
    def _(r):
        b = rep_s[r]
        count = flag_s[0, b]

        @pl.when(count > 1)
        def _():
            rows = pl.ds(b, mid, stride=PITCH)
            rounds = sum((count >= 2 ** r).astype(jnp.int32) for r in range(1, 6))

            def more(_, link):
                link = take_lanes(link, link)
                occ = eo_v[rows, :]
                eo_v[rows, :] = occ + take_lanes(occ, jnp.broadcast_to(link[0:1], (mid, 128)))
                return link

            lax.fori_loop(0, rounds, more, jnp.broadcast_to(nxt_v[pl.ds(b, 1), :], (8, 128)))

    row_ids = lax.broadcasted_iota(jnp.int32, (CH, 128), 0)
    own = pl.ds(pl.multiple_of(me * 128, 128), 128)

    def chunk(i, c):
        idx = i * NCH + c
        return tabb[idx + PAD], tabt[idx + PAD], (i >= 0) & (i < n_iter)

    def enc_rows(i):
        parts = []
        for c in range(NCH):
            b, t0, _ = chunk(i, c)
            parts.append(enc_v[pl.ds(pl.multiple_of(b * n_frames + t0, CH), CH), :])
        return jnp.concatenate(parts, axis=0)

    def gh_wait(i, h_v, par):
        @pl.when((i >= 0) & (i < n_iter))
        def _():
            pltpu.make_async_copy(h_v, ghs_hbm.at[pl.ds(0, NCH * CH)], gh_sem.at[par]).wait()

    def gh_start(i, h_v, par):
        @pl.when((i >= 0) & (i < n_iter))
        def _():
            for c in range(NCH):
                b, t0, _ = chunk(i, c)
                row = pl.multiple_of(b * n_frames + t0, CH)
                pltpu.make_async_copy(h_v.at[pl.ds(c * CH, CH)], ghs_hbm.at[pl.ds(row, CH)], gh_sem.at[par]).start()

    def stage(i, zw, zr, lse_w, lse_r, top_v, sum_v, gwr, gr, h_v):
        zw[...] = jnp.dot(enc_rows(i), w_v[...], preferred_element_type=F32)
        h_v[...] = jnp.dot(gr[...], wt_v[...], preferred_element_type=F32)
        gwt_v[...] += lax.dot_general(gr[:, own], enc_rows(i - 2), (((0,), (0,)), ((), ())), preferred_element_type=F32)
        for c in range(NCH):
            b, t0, ok = chunk(i - 1, c)
            rows = slice(c * CH, (c + 1) * CH)
            live = row_ids < jnp.where(ok, in_len[b], 0) - t0
            lse = lse_r[rows, :]
            lacc_v[pl.ds(b, 1), :] += jnp.sum(jnp.where(live, lse, 0.0), axis=0, keepdims=True)
            lse = jnp.where(live, lse, 3.0e38)
            upper = (t0 >= mid).astype(jnp.int32)
            occ = jnp.where(live, eo_v[pl.ds(b + (t0 - upper * mid) * PITCH, CH, stride=PITCH), :], 0.0)
            inv = inv_v[pl.ds(pl.multiple_of(b * 8, 8), 8), :] + upper * 64
            for j in range(n_blk):
                cols = slice(j * 128, (j + 1) * 128)
                col_occ = take_lanes(occ, jnp.broadcast_to(inv[j:j + 1], (CH, 128)))
                gwr[rows, cols] = (jnp.exp(zr[rows, cols] - lse) - col_occ).astype(BF16)
        for r in range(NCH * CH // 8):
            rows = slice(r * 8, (r + 1) * 8)
            z = zw[rows, :]
            parts = [z[:, j * 128:(j + 1) * 128] for j in range(n_blk)]
            top = functools.reduce(jnp.maximum, parts)
            top_v[rows, :] = top
            sum_v[rows, :] = functools.reduce(jnp.add, [jnp.exp(part - top) for part in parts])
        tops = top_v[...]
        top = jnp.max(tops, axis=1, keepdims=True)
        lse_w[...] = jnp.broadcast_to(top + jnp.log(jnp.sum(sum_v[...] * jnp.exp(tops - top), axis=1, keepdims=True)), (NCH * CH, 128))

    trips = (n_iter + 3) // 2

    @pl.loop(0, trips)
    def _(ii):
        i = 2 * ii
        slot = lax.rem(ii, 2)
        gh_wait(i - 6, h0_v.at[slot], 2 * slot)
        gh_wait(i - 5, h1_v.at[slot], 2 * slot + 1)
        stage(i, z0_v, z1_v, lse0_v, lse1_v, top0_v, sum0_v, g1_v, g0_v, h0_v.at[slot])
        stage(i + 1, z1_v, z0_v, lse1_v, lse0_v, top1_v, sum1_v, g0_v, g1_v, h1_v.at[slot])
        gh_start(i - 2, h0_v.at[slot], 2 * slot)
        gh_start(i - 1, h1_v.at[slot], 2 * slot + 1)

    for back in (2, 1):
        slot = lax.rem(trips - back + 2, 2)
        gh_wait(2 * (trips - back) - 2, h0_v.at[slot], 2 * slot)
        gh_wait(2 * (trips - back) - 1, h1_v.at[slot], 2 * slot + 1)
    gw_ref[...] = gwt_v[...].T
    loss_ref[...] = lacc_v[...].T[0:1, :] - blank_sum - log_z

    @pl.loop(n_iter * NCH, n_seq * n_per)
    def _(k):
        zero_copy(k).wait()


def solution(mesh):
    n_dev = mesh.shape["tp"]

    def device_fn(enc_out, w_loc, labels, in_len, lab_len):
        n_seq, n_frames, hidden = enc_out.shape
        n_lab = labels.shape[1]
        n_cols = w_loc.shape[1]
        n_vocab = n_cols * n_dev
        vmem = pl.BlockSpec(memory_space=pltpu.VMEM)
        smem = pl.BlockSpec(memory_space=pltpu.SMEM)
        anyspace = pl.BlockSpec(memory_space=pl.ANY)
        w_all = pl.pallas_call(
            gather_kernel,
            out_shape=jax.ShapeDtypeStruct((n_dev, hidden, n_cols), BF16),
            in_specs=[vmem],
            out_specs=vmem,
            scratch_shapes=[pltpu.SemaphoreType.DMA((9,)), pltpu.SemaphoreType.DMA((9,))],
            compiler_params=pltpu.CompilerParams(collective_id=0, has_side_effects=True),
            name="gather_w",
        )(w_loc)
        n_per = n_frames // CH
        n_grp = n_seq // 4
        loss, grad_w, grad_hs = pl.pallas_call(
            functools.partial(ctc_kernel, n_seq, n_frames, n_lab),
            out_shape=(
                jax.ShapeDtypeStruct((1, n_seq), F32),
                jax.ShapeDtypeStruct((hidden, n_cols), F32),
                jax.ShapeDtypeStruct((n_seq * n_frames, hidden), F32),
            ),
            in_specs=[smem, vmem, vmem, vmem, anyspace, anyspace],
            out_specs=(vmem, vmem, anyspace),
            scratch_shapes=[
                pltpu.VMEM((n_seq * n_frames, hidden), BF16),
                pltpu.VMEM((hidden, n_vocab), BF16),
                pltpu.VMEM((n_vocab, hidden), BF16),
                pltpu.VMEM((192, n_vocab), BF16),
                pltpu.VMEM((192, n_vocab), BF16),
                pltpu.VMEM((512, hidden), BF16),
                pltpu.VMEM((512, hidden), BF16),
                pltpu.VMEM((n_frames // 2 * PITCH, 128), F32),
                pltpu.VMEM((n_frames * 48, 128), F32),
                pltpu.VMEM((n_frames * 104, 128), F32),
                pltpu.VMEM((n_seq * n_dev, 128), jnp.int32),
                pltpu.VMEM((n_seq + 8, 128), jnp.int32),
                pltpu.VMEM((NCH * CH, n_vocab), F32),
                pltpu.VMEM((NCH * CH, n_vocab), F32),
                pltpu.VMEM((NCH * CH, n_vocab), BF16),
                pltpu.VMEM((NCH * CH, n_vocab), BF16),
                pltpu.VMEM((2, NCH * CH, hidden), F32),
                pltpu.VMEM((2, NCH * CH, hidden), F32),
                pltpu.VMEM((NCH * CH, 128), F32),
                pltpu.VMEM((NCH * CH, 128), F32),
                pltpu.VMEM((NCH * CH, 128), F32),
                pltpu.VMEM((NCH * CH, 128), F32),
                pltpu.VMEM((NCH * CH, 128), F32),
                pltpu.VMEM((NCH * CH, 128), F32),
                pltpu.VMEM((n_cols, hidden), F32),
                pltpu.VMEM((n_seq, 128), F32),
                pltpu.VMEM((CH, hidden), F32),
                pltpu.VMEM((8, 128), jnp.int32),
                pltpu.SMEM((n_seq * n_per + 3 * PAD,), jnp.int32),
                pltpu.SMEM((n_seq * n_per + 3 * PAD,), jnp.int32),
                pltpu.SMEM((n_seq + 8,), jnp.int32),
                pltpu.SMEM((8, 128), jnp.int32),
                pltpu.SemaphoreType.DMA((n_grp,)),
                pltpu.SemaphoreType.DMA((n_dev,)),
                pltpu.SemaphoreType.DMA((4,)),
                pltpu.SemaphoreType.DMA,
                pltpu.SemaphoreType.DMA,
            ],
            compiler_params=pltpu.CompilerParams(vmem_limit_bytes=63 * 1024 * 1024),
            name="ctc",
        )(in_len, labels.T, in_len.reshape(1, n_seq), lab_len.reshape(1, n_seq), enc_out.reshape(n_seq * n_frames, hidden), w_all)
        return loss.reshape(n_seq), grad_w, grad_hs.reshape(n_seq, n_frames, hidden)

    return jax.shard_map(device_fn, mesh=mesh, in_specs=(P("dp"), P(None, "tp"), P("dp"), P("dp"), P("dp")), out_specs=(P("dp"), P("dp", "tp"), P("dp")), check_vma=False)
```

```python
import functools

import jax
import jax.numpy as jnp
from jax import lax
from jax.experimental import pallas as pl
from jax.experimental.pallas import tpu as pltpu
from jax.sharding import PartitionSpec as P

NEG_FILL = -1.0e30
CH = 32
NCH = 16
PAD = 6 * NCH
PITCH = 136
DUMMY = 55
AHEAD = 6
MESH = pl.DeviceIdType.MESH
F32 = jnp.float32
BF16 = jnp.bfloat16


def gather_kernel(w_hbm, out_hbm, buf, send_sem, recv_sem, in_sem, out_sem):
    me = lax.axis_index("tp")
    core, col, row = lax.rem(me, 2), lax.rem(me // 2, 2), me // 4
    mate = me + 1 - 2 * core
    across = me + 2 * (1 - 2 * col)
    along = me + 4 * (1 - 2 * row)
    far = across + along - me
    load = pltpu.make_async_copy(w_hbm, buf.at[me], in_sem)
    load.start()
    barrier = pltpu.get_barrier_semaphore()
    for peer in (mate, across, along):
        pl.semaphore_signal(barrier, inc=1, device_id={"tp": peer}, device_id_type=MESH)
    load.wait()
    pl.semaphore_wait(barrier, 3)
    rows = w_hbm.shape[0]
    upper, lower, whole = pl.ds(0, rows // 2), pl.ds(rows // 2, rows // 2), pl.ds(0, rows)

    def push(k, block, part, peer):
        copy = pltpu.make_async_remote_copy(
            src_ref=buf.at[block, part], dst_ref=buf.at[block, part], send_sem=send_sem.at[k], recv_sem=recv_sem.at[k],
            device_id={"tp": peer}, device_id_type=MESH,
        )
        copy.start()
        return copy

    stores = []

    def put(block):
        copy = pltpu.make_async_copy(buf.at[block], out_hbm.at[block], out_sem.at[len(stores)])
        copy.start()
        stores.append(copy)

    pushes = [
        push(0, me, upper, across), push(1, me, lower, along), push(2, me, lower, across), push(3, me, upper, along),
        push(4, me, whole, mate),
    ]
    put(me)
    pushes[0].wait_recv()
    pushes.append(push(5, across, upper, along))
    pushes[1].wait_recv()
    pushes.append(push(6, along, lower, across))
    pushes[4].wait_recv()
    put(mate)
    pushes[2].wait_recv()
    pushes.append(push(7, across, whole, mate))
    put(across)
    pushes[3].wait_recv()
    pushes.append(push(8, along, whole, mate))
    put(along)
    pushes[5].wait_recv()
    pushes.append(push(9, far, upper, mate))
    pushes[6].wait_recv()
    pushes.append(push(10, far, lower, mate))
    put(far)
    pushes[7].wait_recv()
    put(mate + across - me)
    pushes[8].wait_recv()
    put(mate + along - me)
    pushes[9].wait_recv()
    pushes[10].wait_recv()
    put(mate + far - me)
    for copy in pushes:
        copy.wait_send()
    for copy in stores:
        copy.wait()


def take_lanes(x, idx):
    return jnp.take_along_axis(x, idx, axis=1, mode="promise_in_bounds")


def steps_of_four(low, high, step, state):
    def body(q, st):
        for u in range(4):
            st = step(low + 4 * q + u, st)
        return st

    state = lax.fori_loop(0, (high - low) // 4, body, state)
    for k in range(high - (high - low) % 4, high):
        state = step(k, state)
    return state


def lse2(a, b):
    top = jnp.maximum(a, b)
    return top + jnp.log(1.0 + jnp.exp(jnp.minimum(a, b) - top))


def ctc_kernel(
    n_seq, n_frames, n_lab,
    in_len, labt_ref, inrow_ref, lenrow_ref, enc_hbm, wg_hbm,
    loss_ref, gw_ref, ghs_hbm,
    enc_v, w_v, wt_v, oh0_v, oh1_v, gl0_v, gl1_v, eo_v, et_v, ab_v, inv_v, nxt_v, z0_v, z1_v, g0_v, g1_v, h0_v, h1_v, top0_v, top1_v, sum0_v, sum1_v, lse0_v, lse1_v, gwt_v, lacc_v, zero_v, flag_v,
    tabb, tabt, rep_s, flag_s, enc_sem, w_sem, gh_sem, zero_sem, flag_sem,
):
    me = lax.axis_index("tp")
    n_vocab = w_v.shape[1]
    n_blk = n_vocab // 128
    n_grp = n_seq // 4
    mid = n_frames // 2
    n_per = n_frames // CH
    per_mid = mid // CH

    def enc_copy(g):
        rows = pl.ds(pl.multiple_of(4 * g * n_frames, 4 * n_frames), 4 * n_frames)
        return pltpu.make_async_copy(enc_hbm.at[rows], enc_v.at[rows], enc_sem.at[g])

    w_copies = [pltpu.make_async_copy(wg_hbm.at[k], w_v.at[:, pl.ds(k * 128, 128)], w_sem.at[k]) for k in range(n_blk)]
    for copy in w_copies:
        copy.start()

    for g in range(AHEAD):
        enc_copy(g).start()

    for ref in (zero_v, lacc_v, gwt_v, z1_v, lse1_v, g0_v, g1_v):
        ref[...] = jnp.zeros_like(ref)
    sub48 = lax.broadcasted_iota(jnp.int32, (48, 128), 0)
    in_row = inrow_ref[...]
    len_row = lenrow_ref[...]
    lab48 = jnp.where(sub48 < len_row, labt_ref[...], -1 - sub48)
    skip = lab48 != pltpu.roll(lab48, 1, 0)

    nxt = jnp.full((48, 128), DUMMY, jnp.int32)
    later = jnp.zeros((48, 128), jnp.int32)
    for d in range(n_lab - 1, 0, -1):
        same = (pltpu.roll(lab48, 48 - d, 0) == lab48) & (sub48 < 48 - d)
        nxt = jnp.where(same, sub48 + d, nxt)
        later = later + jnp.where(same, 1, 0)
    nxt_f = jnp.concatenate([nxt.astype(F32), jnp.full((16, 128), float(DUMMY), F32)], axis=0)
    nxt_v[0:n_seq] = jnp.concatenate([nxt_f, nxt_f + 64.0], axis=0).T.astype(jnp.int32)
    nxt_v[n_seq:n_seq + 8] = jnp.full((8, 128), DUMMY, jnp.int32)
    flag_v[...] = jnp.broadcast_to(jnp.max(later.astype(F32), axis=0, keepdims=True), (8, 128)).astype(jnp.int32)
    flag_copy = pltpu.make_async_copy(flag_v, flag_s, flag_sem)
    flag_copy.start()

    for copy in w_copies:
        copy.wait()
    wt_v[...] = w_v[...].T
    row16 = lax.broadcasted_iota(jnp.int32, (16, wt_v.shape[1]), 0)
    tail = jnp.where(row16 == 0, wt_v[0:16, :].astype(F32), 0.0).astype(BF16)
    for k in range(8):
        gl0_v[k * 64 + 48:(k + 1) * 64, :] = tail
        gl1_v[k * 64 + 48:(k + 1) * 64, :] = tail

    lane48 = lax.broadcasted_iota(jnp.int32, (48, 128), 1)
    sub48f = sub48.astype(F32)
    lane1 = lax.broadcasted_iota(jnp.int32, (1, 128), 1)
    lane_mid = lax.broadcasted_iota(jnp.int32, (mid, 128), 1)

    def list_group(g, n):
        for k in range(4):
            b = 4 * g + k
            cnt = (in_len[jnp.minimum(b, n_seq - 1)] + CH - 1) // CH
            dead = n_seq * n_per - 1 - (b * n_per - n)
            for j in range(n_per):
                slot = jnp.where(g < n_grp, PAD + jnp.where(j < cnt, n + j, dead - (j - cnt)), j)
                tabb[slot] = b
                tabt[slot] = j * CH
            n = n + jnp.where(g < n_grp, cnt, 0)
        return n

    def build_hot(g, oh_v):
        for k in range(4):
            b = 4 * g + k
            col = take_lanes(lab48, jnp.full((48, 128), b, jnp.int32))
            firsts = []
            for j in range(n_blk):
                hit = col == lane48 + 128 * j
                oh_v[k * 48:(k + 1) * 48, j * 128:(j + 1) * 128] = jnp.where(hit, 1.0, 0.0).astype(BF16)
                start = jnp.where(lane1 == 0, 48.0, float(DUMMY)) if j == 0 else float(DUMMY)
                firsts.append(jnp.minimum(jnp.min(jnp.where(hit, sub48f, float(DUMMY)), axis=0, keepdims=True), start))
            inv_v[pl.ds(pl.multiple_of(b * 8, 8), 8), :] = jnp.concatenate(firsts, axis=0).astype(jnp.int32)

    def pick_cols(oh_v, gl_v):
        picked = jnp.dot(oh_v[...], wt_v[...], preferred_element_type=F32).astype(BF16)
        for k in range(4):
            for h in range(2):
                gl_v[k * 128 + h * 64:k * 128 + h * 64 + 48, :] = picked[k * 48:(k + 1) * 48]

    def emit_group(g, gl_v):
        for k in range(4):
            b = 4 * g + k
            x = enc_v[pl.ds(pl.multiple_of(b * n_frames, n_frames), n_frames), :]
            e = lax.dot_general(x, gl_v[k * 128:(k + 1) * 128, :], (((1,), (1,)), ((), ())), preferred_element_type=F32)
            eo_v[pl.ds(b, mid, stride=PITCH), :] = jnp.where(lane_mid < 64, e[0:mid], e[mid:n_frames])

    build_hot(0, oh0_v)

    def emit_pair(ii, n):
        for s in range(2):
            g = 2 * ii + s

            @pl.when((g >= 1) & (g <= n_grp))
            def _():
                enc_copy(g - 1).wait()

            @pl.when(g + AHEAD < n_grp)
            def _():
                enc_copy(g + AHEAD).start()
        n = list_group(2 * ii + 1, list_group(2 * ii, n))
        for s in range(2):
            g = 2 * ii + s
            build_hot(jnp.minimum(g + 1, n_grp - 1), (oh1_v, oh0_v)[s])
            pick_cols((oh0_v, oh1_v)[s], (gl0_v, gl1_v)[s])
            emit_group(jnp.clip(g - 1, 0, n_grp - 1), (gl1_v, gl0_v)[s])
        return n

    n_live = lax.fori_loop(0, n_grp // 2 + 1, emit_pair, 0)
    for j in range(PAD):
        for base in (0, PAD + n_seq * n_per):
            tabb[base + j] = 0
            tabt[base + j] = 0
    n_iter = (n_live + NCH - 1) // NCH

    def zero_copy(k):
        row = pl.multiple_of(tabb[PAD + k] * n_frames + tabt[PAD + k], CH)
        return pltpu.make_async_copy(zero_v, ghs_hbm.at[pl.ds(row, CH)], zero_sem)

    @pl.loop(n_iter * NCH, n_seq * n_per)
    def _(k):
        zero_copy(k).start()

    def turn_in(j, acc):
        turned = eo_v[pl.ds(pl.multiple_of(j * PITCH, 8), n_seq), :].T
        low = turned[48:49]
        high = turned[112:113]
        et_v[pl.ds(pl.multiple_of(j * 48, 8), 48), :] = turned[0:48] - low
        et_v[pl.ds(pl.multiple_of((j + mid) * 48, 8), 48), :] = turned[64:112] - high
        return acc + jnp.where(j < in_row, low, 0.0) + jnp.where(j + mid < in_row, high, 0.0)

    blank_sum = jnp.zeros((1, 128), F32)
    for j in (0, 1, mid - 1):
        blank_sum = turn_in(j, blank_sum)

    neg8 = jnp.full((8, 128), NEG_FILL, F32)
    sub56 = lax.broadcasted_iota(jnp.int32, (56, 128), 0)

    def emit_at(t):
        return et_v[pl.ds(pl.multiple_of(t * 48, 8), 48), :]

    def alpha_step(t, blk, lab):
        shifted = pltpu.roll(jnp.concatenate([lab, neg8], axis=0), 1, 0)
        blk_new = lse2(blk, shifted)
        via = jnp.where(skip, blk_new[0:48], blk[0:48])
        lab_new = lse2(lab, via) + emit_at(t)
        live = t < in_row
        return jnp.where(live, blk_new, blk), jnp.where(live, lab_new, lab)

    def beta_step(t, blk, lab):
        emitted = lab + emit_at(t + 1)
        blk_new = lse2(blk, jnp.concatenate([emitted, neg8], axis=0))
        via = jnp.concatenate([jnp.where(skip, blk_new[0:48], blk[0:48]), blk_new[48:56]], axis=0)
        lab_new = lse2(emitted, pltpu.roll(via, 55, 0)[0:48])
        live = t + 1 < in_row
        return jnp.where(live, blk_new, blk), jnp.where(live, lab_new, lab)

    def keep(t, blk, lab):
        row = pl.multiple_of(t * 104, 8)
        ab_v[pl.ds(row, 56), :] = blk
        ab_v[pl.ds(row + 56, 48), :] = lab

    a_blk = jnp.where(sub56 == 0, 0.0, NEG_FILL).astype(F32) + jnp.zeros((56, 128), F32)
    a_lab = jnp.full((48, 128), NEG_FILL, F32)
    b_blk = jnp.where(sub56 == len_row, 0.0, NEG_FILL).astype(F32)
    b_lab = jnp.where(sub48 == len_row - 1, 0.0, NEG_FILL).astype(F32)

    a_blk, a_lab = alpha_step(0, a_blk, a_lab)
    keep(0, a_blk, a_lab)
    keep(n_frames - 1, b_blk, b_lab)

    def first_half(k, state):
        a_blk, a_lab, b_blk, b_lab = state
        a_blk, a_lab = alpha_step(k, a_blk, a_lab)
        keep(k, a_blk, a_lab)
        t = n_frames - 1 - k
        b_blk, b_lab = beta_step(t, b_blk, b_lab)
        keep(t, b_blk, b_lab)
        return a_blk, a_lab, b_blk, b_lab

    def first_quarter(k, state):
        new = first_half(k, state[:4])
        return (*new, turn_in(mid - 1 - k, turn_in(k + 1, state[4])))

    quarter = mid // 2
    a_blk, a_lab, b_blk, b_lab, blank_sum = steps_of_four(1, quarter - 1, first_quarter, (a_blk, a_lab, b_blk, b_lab, blank_sum))
    blank_sum = turn_in(quarter, blank_sum)

    flag_copy.wait()

    def second_quarter(k, state):
        n = state[4]
        for u in range(3):
            b = jnp.minimum(3 * (k - quarter + 1) + u, n_seq)
            rep_s[n] = b
            n = n + jnp.where((b < n_seq) & (flag_s[0, jnp.minimum(b, n_seq - 1)] > 0), 1, 0)
        return (*first_half(k, state[:4]), n)

    a_blk, a_lab, b_blk, b_lab, n_rep = steps_of_four(quarter - 1, mid, second_quarter, (a_blk, a_lab, b_blk, b_lab, 0))
    for u in range(4):
        rep_s[n_rep + u] = n_seq

    m_blk, m_lab = beta_step(mid - 1, b_blk, b_lab)
    s_blk = a_blk + m_blk
    s_lab = a_lab + m_lab
    top = jnp.maximum(jnp.max(s_blk, axis=0, keepdims=True), jnp.max(s_lab, axis=0, keepdims=True))
    total = jnp.sum(jnp.exp(s_blk - top), axis=0, keepdims=True) + jnp.sum(jnp.exp(s_lab - top), axis=0, keepdims=True)
    log_z = top + jnp.log(total)
    sub8 = lax.broadcasted_iota(jnp.int32, (8, 128), 0)

    def put_occ(t, blk, lab):
        row = pl.multiple_of(t * 104, 8)
        occ_blk = jnp.sum(jnp.exp(ab_v[pl.ds(row, 56), :] + (blk - log_z)), axis=0, keepdims=True)
        occ_lab = jnp.exp(ab_v[pl.ds(row + 56, 48), :] + (lab - log_z))
        ab_v[pl.ds(row, 48), :] = occ_lab
        ab_v[pl.ds(row + 48, 8), :] = jnp.where(sub8 == 0, occ_blk, 0.0)

    zero8 = jnp.zeros((8, 128), F32)

    def turn_out(j):
        low = ab_v[pl.ds(pl.multiple_of(j * 104, 8), 56), :]
        high = ab_v[pl.ds(pl.multiple_of((j + mid) * 104, 8), 56), :]
        turned = jnp.concatenate([low, zero8, high, zero8], axis=0).T
        eo_v[pl.ds(pl.multiple_of(j * PITCH, 8), n_seq), :] = turned

    def second_half(k, state):
        a_blk, a_lab, b_blk, b_lab = state
        t = n_frames - 1 - k
        put_occ(k - 1, a_blk, a_lab)
        put_occ(t + 1, b_blk, b_lab)
        a_blk, a_lab = alpha_step(k, a_blk, a_lab)
        b_blk, b_lab = beta_step(t, b_blk, b_lab)
        return a_blk, a_lab, b_blk, b_lab

    def last_quarter(k, state):
        turn_out(k - 2 - mid)
        turn_out(n_frames + 1 - k)
        return second_half(k, state)

    a_blk, a_lab = alpha_step(mid, a_blk, a_lab)
    state = steps_of_four(mid + 1, mid + quarter + 2, second_half, (a_blk, a_lab, m_blk, m_lab))
    a_blk, a_lab, b_blk, b_lab = steps_of_four(mid + quarter + 2, n_frames, last_quarter, state)
    put_occ(n_frames - 1, a_blk, a_lab)
    put_occ(0, b_blk, b_lab)
    for j in (mid - 2, 1, mid - 1, 0):
        turn_out(j)

    @pl.loop(0, (n_rep + 3) // 4)
    def _(q):
        seqs = [rep_s[4 * q + u] for u in range(4)]
        occs = [eo_v[pl.ds(b, mid, stride=PITCH), :] for b in seqs]
        links = [nxt_v[pl.ds(b, 1), :] for b in seqs]
        for b, occ, link in zip(seqs, occs, links):
            eo_v[pl.ds(b, mid, stride=PITCH), :] = occ + take_lanes(occ, jnp.broadcast_to(link, (mid, 128)))

    @pl.loop(0, n_rep)
    def _(r):
        b = rep_s[r]
        count = flag_s[0, b]

        @pl.when(count > 1)
        def _():
            rows = pl.ds(b, mid, stride=PITCH)
            rounds = sum((count >= 2 ** r).astype(jnp.int32) for r in range(1, 6))

            def more(_, link):
                link = take_lanes(link, link)
                occ = eo_v[rows, :]
                eo_v[rows, :] = occ + take_lanes(occ, jnp.broadcast_to(link[0:1], (mid, 128)))
                return link

            lax.fori_loop(0, rounds, more, jnp.broadcast_to(nxt_v[pl.ds(b, 1), :], (8, 128)))

    row_ids = lax.broadcasted_iota(jnp.int32, (CH, 128), 0)
    own = pl.ds(pl.multiple_of(me * 128, 128), 128)

    def chunk(i, c):
        idx = i * NCH + c
        return tabb[idx + PAD], tabt[idx + PAD], (i >= 0) & (i < n_iter)

    def enc_rows(i):
        parts = []
        for c in range(NCH):
            b, t0, _ = chunk(i, c)
            parts.append(enc_v[pl.ds(pl.multiple_of(b * n_frames + t0, CH), CH), :])
        return jnp.concatenate(parts, axis=0)

    def gh_wait(i, h_v, par):
        @pl.when((i >= 0) & (i < n_iter))
        def _():
            pltpu.make_async_copy(h_v, ghs_hbm.at[pl.ds(0, NCH * CH)], gh_sem.at[par]).wait()

    def gh_start(i, h_v, par):
        @pl.when((i >= 0) & (i < n_iter))
        def _():
            for c in range(NCH):
                b, t0, _ = chunk(i, c)
                row = pl.multiple_of(b * n_frames + t0, CH)
                pltpu.make_async_copy(h_v.at[pl.ds(c * CH, CH)], ghs_hbm.at[pl.ds(row, CH)], gh_sem.at[par]).start()

    def stage(i, zw, zr, lse_w, lse_r, top_v, sum_v, gwr, gr, h_v):
        zw[...] = jnp.dot(enc_rows(i), w_v[...], preferred_element_type=F32)
        h_v[...] = jnp.dot(gr[...], wt_v[...], preferred_element_type=F32)
        gwt_v[...] += lax.dot_general(gr[:, own], enc_rows(i - 2), (((0,), (0,)), ((), ())), preferred_element_type=F32)
        for c in range(NCH):
            b, t0, ok = chunk(i - 1, c)
            rows = slice(c * CH, (c + 1) * CH)
            live = row_ids < jnp.where(ok, in_len[b], 0) - t0
            lse = lse_r[rows, :]
            lacc_v[pl.ds(b, 1), :] += jnp.sum(jnp.where(live, lse, 0.0), axis=0, keepdims=True)
            lse = jnp.where(live, lse, 3.0e38)
            upper = (t0 >= mid).astype(jnp.int32)
            occ = jnp.where(live, eo_v[pl.ds(b + (t0 - upper * mid) * PITCH, CH, stride=PITCH), :], 0.0)
            inv = inv_v[pl.ds(pl.multiple_of(b * 8, 8), 8), :] + upper * 64
            for j in range(n_blk):
                cols = slice(j * 128, (j + 1) * 128)
                col_occ = take_lanes(occ, jnp.broadcast_to(inv[j:j + 1], (CH, 128)))
                gwr[rows, cols] = (jnp.exp(zr[rows, cols] - lse) - col_occ).astype(BF16)
        for r in range(NCH * CH // 8):
            rows = slice(r * 8, (r + 1) * 8)
            z = zw[rows, :]
            parts = [z[:, j * 128:(j + 1) * 128] for j in range(n_blk)]
            top = functools.reduce(jnp.maximum, parts)
            top_v[rows, :] = top
            sum_v[rows, :] = functools.reduce(jnp.add, [jnp.exp(part - top) for part in parts])
        tops = top_v[...]
        top = jnp.max(tops, axis=1, keepdims=True)
        lse_w[...] = jnp.broadcast_to(top + jnp.log(jnp.sum(sum_v[...] * jnp.exp(tops - top), axis=1, keepdims=True)), (NCH * CH, 128))

    trips = (n_iter + 3) // 2

    @pl.loop(0, trips)
    def _(ii):
        i = 2 * ii
        slot = lax.rem(ii, 2)
        gh_wait(i - 6, h0_v.at[slot], 2 * slot)
        gh_wait(i - 5, h1_v.at[slot], 2 * slot + 1)
        stage(i, z0_v, z1_v, lse0_v, lse1_v, top0_v, sum0_v, g1_v, g0_v, h0_v.at[slot])
        stage(i + 1, z1_v, z0_v, lse1_v, lse0_v, top1_v, sum1_v, g0_v, g1_v, h1_v.at[slot])
        gh_start(i - 2, h0_v.at[slot], 2 * slot)
        gh_start(i - 1, h1_v.at[slot], 2 * slot + 1)

    for back in (2, 1):
        slot = lax.rem(trips - back + 2, 2)
        gh_wait(2 * (trips - back) - 2, h0_v.at[slot], 2 * slot)
        gh_wait(2 * (trips - back) - 1, h1_v.at[slot], 2 * slot + 1)
    gw_ref[...] = gwt_v[...].T
    loss_ref[...] = lacc_v[...].T[0:1, :] - blank_sum - log_z

    @pl.loop(n_iter * NCH, n_seq * n_per)
    def _(k):
        zero_copy(k).wait()


def solution(mesh):
    n_dev = mesh.shape["tp"]

    def device_fn(enc_out, w_loc, labels, in_len, lab_len):
        n_seq, n_frames, hidden = enc_out.shape
        n_lab = labels.shape[1]
        n_cols = w_loc.shape[1]
        n_vocab = n_cols * n_dev
        vmem = pl.BlockSpec(memory_space=pltpu.VMEM)
        smem = pl.BlockSpec(memory_space=pltpu.SMEM)
        anyspace = pl.BlockSpec(memory_space=pl.ANY)
        w_all = pl.pallas_call(
            gather_kernel,
            out_shape=jax.ShapeDtypeStruct((n_dev, hidden, n_cols), BF16),
            in_specs=[anyspace],
            out_specs=anyspace,
            scratch_shapes=[
                pltpu.VMEM((n_dev, hidden, n_cols), BF16),
                pltpu.SemaphoreType.DMA((11,)),
                pltpu.SemaphoreType.DMA((11,)),
                pltpu.SemaphoreType.DMA,
                pltpu.SemaphoreType.DMA((n_dev,)),
            ],
            compiler_params=pltpu.CompilerParams(collective_id=0, has_side_effects=True),
            name="gather_w",
        )(w_loc)
        n_per = n_frames // CH
        n_grp = n_seq // 4
        loss, grad_w, grad_hs = pl.pallas_call(
            functools.partial(ctc_kernel, n_seq, n_frames, n_lab),
            out_shape=(
                jax.ShapeDtypeStruct((1, n_seq), F32),
                jax.ShapeDtypeStruct((hidden, n_cols), F32),
                jax.ShapeDtypeStruct((n_seq * n_frames, hidden), F32),
            ),
            in_specs=[smem, vmem, vmem, vmem, anyspace, anyspace],
            out_specs=(vmem, vmem, anyspace),
            scratch_shapes=[
                pltpu.VMEM((n_seq * n_frames, hidden), BF16),
                pltpu.VMEM((hidden, n_vocab), BF16),
                pltpu.VMEM((n_vocab, hidden), BF16),
                pltpu.VMEM((192, n_vocab), BF16),
                pltpu.VMEM((192, n_vocab), BF16),
                pltpu.VMEM((512, hidden), BF16),
                pltpu.VMEM((512, hidden), BF16),
                pltpu.VMEM((n_frames // 2 * PITCH, 128), F32),
                pltpu.VMEM((n_frames * 48, 128), F32),
                pltpu.VMEM((n_frames * 104, 128), F32),
                pltpu.VMEM((n_seq * n_dev, 128), jnp.int32),
                pltpu.VMEM((n_seq + 8, 128), jnp.int32),
                pltpu.VMEM((NCH * CH, n_vocab), F32),
                pltpu.VMEM((NCH * CH, n_vocab), F32),
                pltpu.VMEM((NCH * CH, n_vocab), BF16),
                pltpu.VMEM((NCH * CH, n_vocab), BF16),
                pltpu.VMEM((2, NCH * CH, hidden), F32),
                pltpu.VMEM((2, NCH * CH, hidden), F32),
                pltpu.VMEM((NCH * CH, 128), F32),
                pltpu.VMEM((NCH * CH, 128), F32),
                pltpu.VMEM((NCH * CH, 128), F32),
                pltpu.VMEM((NCH * CH, 128), F32),
                pltpu.VMEM((NCH * CH, 128), F32),
                pltpu.VMEM((NCH * CH, 128), F32),
                pltpu.VMEM((n_cols, hidden), F32),
                pltpu.VMEM((n_seq, 128), F32),
                pltpu.VMEM((CH, hidden), F32),
                pltpu.VMEM((8, 128), jnp.int32),
                pltpu.SMEM((n_seq * n_per + 3 * PAD,), jnp.int32),
                pltpu.SMEM((n_seq * n_per + 3 * PAD,), jnp.int32),
                pltpu.SMEM((n_seq + 8,), jnp.int32),
                pltpu.SMEM((8, 128), jnp.int32),
                pltpu.SemaphoreType.DMA((n_grp,)),
                pltpu.SemaphoreType.DMA((n_dev,)),
                pltpu.SemaphoreType.DMA((4,)),
                pltpu.SemaphoreType.DMA,
                pltpu.SemaphoreType.DMA,
            ],
            compiler_params=pltpu.CompilerParams(vmem_limit_bytes=63 * 1024 * 1024),
            name="ctc",
        )(in_len, labels.T, in_len.reshape(1, n_seq), lab_len.reshape(1, n_seq), enc_out.reshape(n_seq * n_frames, hidden), w_all)
        return loss.reshape(n_seq), grad_w, grad_hs.reshape(n_seq, n_frames, hidden)

    return jax.shard_map(device_fn, mesh=mesh, in_specs=(P("dp"), P(None, "tp"), P("dp"), P("dp"), P("dp")), out_specs=(P("dp"), P("dp", "tp"), P("dp")), check_vma=False)
```

```python
import functools

import jax
import jax.numpy as jnp
from jax import lax
from jax.experimental import pallas as pl
from jax.experimental.pallas import tpu as pltpu
from jax.sharding import PartitionSpec as P

NEG_FILL = -1.0e30
CH = 32
NCH = 16
PAD = 6 * NCH
PITCH = 136
DUMMY = 55
AHEAD = 6
MESH = pl.DeviceIdType.MESH
F32 = jnp.float32
BF16 = jnp.bfloat16


def gather_kernel(w_hbm, out_hbm, buf, send_sem, recv_sem, in_sem, out_sem):
    me = lax.axis_index("tp")
    core, col, row = lax.rem(me, 2), lax.rem(me // 2, 2), me // 4
    mate = me + 1 - 2 * core
    across = me + 2 * (1 - 2 * col)
    along = me + 4 * (1 - 2 * row)
    far = across + along - me
    load = pltpu.make_async_copy(w_hbm, buf.at[me], in_sem)
    load.start()
    barrier = pltpu.get_barrier_semaphore()
    for peer in (mate, across, along):
        pl.semaphore_signal(barrier, inc=1, device_id={"tp": peer}, device_id_type=MESH)
    load.wait()
    pl.semaphore_wait(barrier, 3)
    rows = w_hbm.shape[0]
    upper, lower, whole = pl.ds(0, rows // 2), pl.ds(rows // 2, rows // 2), pl.ds(0, rows)

    def push(k, block, part, peer):
        copy = pltpu.make_async_remote_copy(
            src_ref=buf.at[block, part], dst_ref=buf.at[block, part], send_sem=send_sem.at[k], recv_sem=recv_sem.at[k],
            device_id={"tp": peer}, device_id_type=MESH,
        )
        copy.start()
        return copy

    stores = []

    def put(block):
        copy = pltpu.make_async_copy(buf.at[block], out_hbm.at[block], out_sem.at[len(stores)])
        copy.start()
        stores.append(copy)

    pushes = [
        push(0, me, upper, across), push(1, me, lower, along), push(2, me, lower, across), push(3, me, upper, along),
        push(4, me, whole, mate),
    ]
    put(me)
    pushes[0].wait_recv()
    pushes.append(push(5, across, upper, along))
    pushes[1].wait_recv()
    pushes.append(push(6, along, lower, across))
    pushes[4].wait_recv()
    put(mate)
    pushes[2].wait_recv()
    pushes.append(push(7, across, whole, mate))
    put(across)
    pushes[3].wait_recv()
    pushes.append(push(8, along, whole, mate))
    put(along)
    pushes[5].wait_recv()
    pushes.append(push(9, far, upper, mate))
    pushes[6].wait_recv()
    pushes.append(push(10, far, lower, mate))
    put(far)
    pushes[7].wait_recv()
    put(mate + across - me)
    pushes[8].wait_recv()
    put(mate + along - me)
    pushes[9].wait_recv()
    pushes[10].wait_recv()
    put(mate + far - me)
    for copy in pushes:
        copy.wait_send()
    for copy in stores:
        copy.wait()


def take_lanes(x, idx):
    return jnp.take_along_axis(x, idx, axis=1, mode="promise_in_bounds")


def steps_of_four(low, high, step, state):
    def body(q, st):
        for u in range(4):
            st = step(low + 4 * q + u, st)
        return st

    state = lax.fori_loop(0, (high - low) // 4, body, state)
    for k in range(high - (high - low) % 4, high):
        state = step(k, state)
    return state


def lse2(a, b):
    top = jnp.maximum(a, b)
    return top + jnp.log(1.0 + jnp.exp(jnp.minimum(a, b) - top))


def ctc_kernel(
    n_seq, n_frames, n_lab,
    in_len, labt_ref, inrow_ref, lenrow_ref, enc_hbm, wg_hbm,
    loss_ref, gw_ref, ghs_hbm,
    enc_v, w_v, wt_v, oh0_v, oh1_v, gl0_v, gl1_v, eo_v, et_v, ab_v, inv_v, nxt_v, z0_v, z1_v, g0_v, g1_v, h0_v, h1_v, top0_v, top1_v, sum0_v, sum1_v, lse0_v, lse1_v, gwt_v, lacc_v, zero_v, flag_v,
    tabb, tabt, rep_s, flag_s, enc_sem, w_sem, gh_sem, zero_sem, flag_sem,
):
    me = lax.axis_index("tp")
    n_vocab = w_v.shape[1]
    n_blk = n_vocab // 128
    n_grp = n_seq // 4
    mid = n_frames // 2
    n_per = n_frames // CH
    per_mid = mid // CH

    def enc_copy(g):
        rows = pl.ds(pl.multiple_of(4 * g * n_frames, 4 * n_frames), 4 * n_frames)
        return pltpu.make_async_copy(enc_hbm.at[rows], enc_v.at[rows], enc_sem.at[g])

    w_copies = [pltpu.make_async_copy(wg_hbm.at[k], w_v.at[:, pl.ds(k * 128, 128)], w_sem.at[k]) for k in range(n_blk)]
    for copy in w_copies:
        copy.start()

    for g in range(AHEAD):
        enc_copy(g).start()

    for ref in (zero_v, lacc_v, gwt_v, z1_v, lse1_v, g0_v, g1_v):
        ref[...] = jnp.zeros_like(ref)
    sub48 = lax.broadcasted_iota(jnp.int32, (48, 128), 0)
    in_row = inrow_ref[...]
    len_row = lenrow_ref[...]
    lab48 = jnp.where(sub48 < len_row, labt_ref[...], -1 - sub48)
    skip = lab48 != pltpu.roll(lab48, 1, 0)

    nxt = jnp.full((48, 128), DUMMY, jnp.int32)
    later = jnp.zeros((48, 128), jnp.int32)
    for d in range(n_lab - 1, 0, -1):
        same = (pltpu.roll(lab48, 48 - d, 0) == lab48) & (sub48 < 48 - d)
        nxt = jnp.where(same, sub48 + d, nxt)
        later = later + jnp.where(same, 1, 0)
    nxt_f = jnp.concatenate([nxt.astype(F32), jnp.full((16, 128), float(DUMMY), F32)], axis=0)
    nxt_v[0:n_seq] = jnp.concatenate([nxt_f, nxt_f + 64.0], axis=0).T.astype(jnp.int32)
    nxt_v[n_seq:n_seq + 8] = jnp.full((8, 128), DUMMY, jnp.int32)
    flag_v[...] = jnp.broadcast_to(jnp.max(later.astype(F32), axis=0, keepdims=True), (8, 128)).astype(jnp.int32)
    flag_copy = pltpu.make_async_copy(flag_v, flag_s, flag_sem)
    flag_copy.start()

    for copy in w_copies:
        copy.wait()
    wt_v[...] = w_v[...].T
    row16 = lax.broadcasted_iota(jnp.int32, (16, wt_v.shape[1]), 0)
    tail = jnp.where(row16 == 0, wt_v[0:16, :].astype(F32), 0.0).astype(BF16)
    for k in range(8):
        gl0_v[k * 64 + 48:(k + 1) * 64, :] = tail
        gl1_v[k * 64 + 48:(k + 1) * 64, :] = tail

    lane48 = lax.broadcasted_iota(jnp.int32, (48, 128), 1)
    sub48f = sub48.astype(F32)
    lane1 = lax.broadcasted_iota(jnp.int32, (1, 128), 1)
    lane_mid = lax.broadcasted_iota(jnp.int32, (mid, 128), 1)

    def list_group(g, n):
        for k in range(4):
            b = 4 * g + k
            cnt = (in_len[jnp.minimum(b, n_seq - 1)] + CH - 1) // CH
            dead = n_seq * n_per - 1 - (b * n_per - n)
            for j in range(n_per):
                slot = jnp.where(g < n_grp, PAD + jnp.where(j < cnt, n + j, dead - (j - cnt)), j)
                tabb[slot] = b
                tabt[slot] = j * CH
            n = n + jnp.where(g < n_grp, cnt, 0)
        return n

    def build_hot(g, oh_v):
        for k in range(4):
            b = 4 * g + k
            col = take_lanes(lab48, jnp.full((48, 128), b, jnp.int32))
            firsts = []
            for j in range(n_blk):
                hit = col == lane48 + 128 * j
                oh_v[k * 48:(k + 1) * 48, j * 128:(j + 1) * 128] = jnp.where(hit, 1.0, 0.0).astype(BF16)
                start = jnp.where(lane1 == 0, 48.0, float(DUMMY)) if j == 0 else float(DUMMY)
                firsts.append(jnp.minimum(jnp.min(jnp.where(hit, sub48f, float(DUMMY)), axis=0, keepdims=True), start))
            inv_v[pl.ds(pl.multiple_of(b * 8, 8), 8), :] = jnp.concatenate(firsts, axis=0).astype(jnp.int32)

    def pick_cols(oh_v, gl_v):
        picked = jnp.dot(oh_v[...], wt_v[...], preferred_element_type=F32).astype(BF16)
        for k in range(4):
            for h in range(2):
                gl_v[k * 128 + h * 64:k * 128 + h * 64 + 48, :] = picked[k * 48:(k + 1) * 48]

    def emit_group(g, gl_v):
        for k in range(4):
            b = 4 * g + k
            x = enc_v[pl.ds(pl.multiple_of(b * n_frames, n_frames), n_frames), :]
            e = lax.dot_general(x, gl_v[k * 128:(k + 1) * 128, :], (((1,), (1,)), ((), ())), preferred_element_type=F32)
            eo_v[pl.ds(b, mid, stride=PITCH), :] = jnp.where(lane_mid < 64, e[0:mid], e[mid:n_frames])

    build_hot(0, oh0_v)

    def emit_pair(ii, n):
        for s in range(2):
            g = 2 * ii + s

            @pl.when((g >= 1) & (g <= n_grp))
            def _():
                enc_copy(g - 1).wait()

            @pl.when(g + AHEAD < n_grp)
            def _():
                enc_copy(g + AHEAD).start()
        n = list_group(2 * ii + 1, list_group(2 * ii, n))
        for s in range(2):
            g = 2 * ii + s
            build_hot(jnp.minimum(g + 1, n_grp - 1), (oh1_v, oh0_v)[s])
            pick_cols((oh0_v, oh1_v)[s], (gl0_v, gl1_v)[s])
            emit_group(jnp.clip(g - 1, 0, n_grp - 1), (gl1_v, gl0_v)[s])
        return n

    n_live = lax.fori_loop(0, n_grp // 2 + 1, emit_pair, 0)
    for j in range(PAD):
        for base in (0, PAD + n_seq * n_per):
            tabb[base + j] = 0
            tabt[base + j] = 0
    n_iter = (n_live + NCH - 1) // NCH

    def turn_in(j, acc):
        turned = eo_v[pl.ds(pl.multiple_of(j * PITCH, 8), n_seq), :].T
        low = turned[48:49]
        high = turned[112:113]
        et_v[pl.ds(pl.multiple_of(j * 48, 8), 48), :] = turned[0:48] - low
        et_v[pl.ds(pl.multiple_of((j + mid) * 48, 8), 48), :] = turned[64:112] - high
        return acc + jnp.where(j < in_row, low, 0.0) + jnp.where(j + mid < in_row, high, 0.0)

    blank_sum = jnp.zeros((1, 128), F32)
    for j in (0, 1, mid - 1):
        blank_sum = turn_in(j, blank_sum)

    neg8 = jnp.full((8, 128), NEG_FILL, F32)
    sub56 = lax.broadcasted_iota(jnp.int32, (56, 128), 0)

    def emit_at(t):
        return et_v[pl.ds(pl.multiple_of(t * 48, 8), 48), :]

    def alpha_step(t, blk, lab):
        shifted = pltpu.roll(jnp.concatenate([lab, neg8], axis=0), 1, 0)
        blk_new = lse2(blk, shifted)
        via = jnp.where(skip, blk_new[0:48], blk[0:48])
        lab_new = lse2(lab, via) + emit_at(t)
        live = t < in_row
        return jnp.where(live, blk_new, blk), jnp.where(live, lab_new, lab)

    def beta_step(t, blk, lab):
        emitted = lab + emit_at(t + 1)
        blk_new = lse2(blk, jnp.concatenate([emitted, neg8], axis=0))
        via = jnp.concatenate([jnp.where(skip, blk_new[0:48], blk[0:48]), blk_new[48:56]], axis=0)
        lab_new = lse2(emitted, pltpu.roll(via, 55, 0)[0:48])
        live = t + 1 < in_row
        return jnp.where(live, blk_new, blk), jnp.where(live, lab_new, lab)

    def keep(t, blk, lab):
        row = pl.multiple_of(t * 104, 8)
        ab_v[pl.ds(row, 56), :] = blk
        ab_v[pl.ds(row + 56, 48), :] = lab

    a_blk = jnp.where(sub56 == 0, 0.0, NEG_FILL).astype(F32) + jnp.zeros((56, 128), F32)
    a_lab = jnp.full((48, 128), NEG_FILL, F32)
    b_blk = jnp.where(sub56 == len_row, 0.0, NEG_FILL).astype(F32)
    b_lab = jnp.where(sub48 == len_row - 1, 0.0, NEG_FILL).astype(F32)

    a_blk, a_lab = alpha_step(0, a_blk, a_lab)
    keep(0, a_blk, a_lab)
    keep(n_frames - 1, b_blk, b_lab)

    def first_half(k, state):
        a_blk, a_lab, b_blk, b_lab = state
        a_blk, a_lab = alpha_step(k, a_blk, a_lab)
        keep(k, a_blk, a_lab)
        t = n_frames - 1 - k
        b_blk, b_lab = beta_step(t, b_blk, b_lab)
        keep(t, b_blk, b_lab)
        return a_blk, a_lab, b_blk, b_lab

    def first_quarter(k, state):
        new = first_half(k, state[:4])
        return (*new, turn_in(mid - 1 - k, turn_in(k + 1, state[4])))

    quarter = mid // 2
    a_blk, a_lab, b_blk, b_lab, blank_sum = steps_of_four(1, quarter - 1, first_quarter, (a_blk, a_lab, b_blk, b_lab, blank_sum))
    blank_sum = turn_in(quarter, blank_sum)

    flag_copy.wait()

    def second_quarter(k, state):
        n = state[4]
        for u in range(3):
            b = jnp.minimum(3 * (k - quarter + 1) + u, n_seq)
            rep_s[n] = b
            n = n + jnp.where((b < n_seq) & (flag_s[0, jnp.minimum(b, n_seq - 1)] > 0), 1, 0)
        return (*first_half(k, state[:4]), n)

    a_blk, a_lab, b_blk, b_lab, n_rep = steps_of_four(quarter - 1, mid, second_quarter, (a_blk, a_lab, b_blk, b_lab, 0))
    for u in range(4):
        rep_s[n_rep + u] = n_seq

    m_blk, m_lab = beta_step(mid - 1, b_blk, b_lab)
    s_blk = a_blk + m_blk
    s_lab = a_lab + m_lab
    top = jnp.maximum(jnp.max(s_blk, axis=0, keepdims=True), jnp.max(s_lab, axis=0, keepdims=True))
    total = jnp.sum(jnp.exp(s_blk - top), axis=0, keepdims=True) + jnp.sum(jnp.exp(s_lab - top), axis=0, keepdims=True)
    log_z = top + jnp.log(total)
    sub8 = lax.broadcasted_iota(jnp.int32, (8, 128), 0)

    def put_occ(t, blk, lab):
        row = pl.multiple_of(t * 104, 8)
        occ_blk = jnp.sum(jnp.exp(ab_v[pl.ds(row, 56), :] + (blk - log_z)), axis=0, keepdims=True)
        occ_lab = jnp.exp(ab_v[pl.ds(row + 56, 48), :] + (lab - log_z))
        ab_v[pl.ds(row, 48), :] = occ_lab
        ab_v[pl.ds(row + 48, 8), :] = jnp.where(sub8 == 0, occ_blk, 0.0)

    zero8 = jnp.zeros((8, 128), F32)

    def turn_out(j):
        low = ab_v[pl.ds(pl.multiple_of(j * 104, 8), 56), :]
        high = ab_v[pl.ds(pl.multiple_of((j + mid) * 104, 8), 56), :]
        turned = jnp.concatenate([low, zero8, high, zero8], axis=0).T
        eo_v[pl.ds(pl.multiple_of(j * PITCH, 8), n_seq), :] = turned

    per_step = -(-(n_seq * (n_per - 1)) // (n_frames - mid - 1))

    def second_half(k, state):
        for u in range(per_step):
            idx = n_live + per_step * (k - mid - 1) + u

            @pl.when(idx < n_seq * n_per)
            def _():
                row = pl.multiple_of(tabb[PAD + idx] * n_frames + tabt[PAD + idx], CH)
                pltpu.make_async_copy(zero_v, ghs_hbm.at[pl.ds(row, CH)], zero_sem).start()

        a_blk, a_lab, b_blk, b_lab = state
        t = n_frames - 1 - k
        put_occ(k - 1, a_blk, a_lab)
        put_occ(t + 1, b_blk, b_lab)
        a_blk, a_lab = alpha_step(k, a_blk, a_lab)
        b_blk, b_lab = beta_step(t, b_blk, b_lab)
        return a_blk, a_lab, b_blk, b_lab

    def last_quarter(k, state):
        turn_out(k - 2 - mid)
        turn_out(n_frames + 1 - k)
        return second_half(k, state)

    a_blk, a_lab = alpha_step(mid, a_blk, a_lab)
    state = steps_of_four(mid + 1, mid + quarter + 2, second_half, (a_blk, a_lab, m_blk, m_lab))
    a_blk, a_lab, b_blk, b_lab = steps_of_four(mid + quarter + 2, n_frames, last_quarter, state)
    put_occ(n_frames - 1, a_blk, a_lab)
    put_occ(0, b_blk, b_lab)
    for j in (mid - 2, 1, mid - 1, 0):
        turn_out(j)

    @pl.loop(0, (n_rep + 3) // 4)
    def _(q):
        seqs = [rep_s[4 * q + u] for u in range(4)]
        occs = [eo_v[pl.ds(b, mid, stride=PITCH), :] for b in seqs]
        links = [nxt_v[pl.ds(b, 1), :] for b in seqs]
        for b, occ, link in zip(seqs, occs, links):
            eo_v[pl.ds(b, mid, stride=PITCH), :] = occ + take_lanes(occ, jnp.broadcast_to(link, (mid, 128)))

    @pl.loop(0, n_rep)
    def _(r):
        b = rep_s[r]
        count = flag_s[0, b]

        @pl.when(count > 1)
        def _():
            rows = pl.ds(b, mid, stride=PITCH)
            rounds = sum((count >= 2 ** r).astype(jnp.int32) for r in range(1, 6))

            def more(_, link):
                link = take_lanes(link, link)
                occ = eo_v[rows, :]
                eo_v[rows, :] = occ + take_lanes(occ, jnp.broadcast_to(link[0:1], (mid, 128)))
                return link

            lax.fori_loop(0, rounds, more, jnp.broadcast_to(nxt_v[pl.ds(b, 1), :], (8, 128)))

    n_dead = n_seq * n_per - n_live
    for r in range((n_seq * n_per).bit_length()):
        @pl.when(lax.rem(n_dead // 2 ** r, 2) == 1)
        def _():
            part = ghs_hbm.at[pl.ds(0, CH * 2 ** r)]
            pltpu.make_async_copy(part, part, zero_sem).wait()

    row_ids = lax.broadcasted_iota(jnp.int32, (CH, 128), 0)
    own = pl.ds(pl.multiple_of(me * 128, 128), 128)

    def chunk(i, c):
        idx = i * NCH + c
        return tabb[idx + PAD], tabt[idx + PAD], (i >= 0) & (i < n_iter)

    def enc_rows(i):
        parts = []
        for c in range(NCH):
            b, t0, _ = chunk(i, c)
            parts.append(enc_v[pl.ds(pl.multiple_of(b * n_frames + t0, CH), CH), :])
        return jnp.concatenate(parts, axis=0)

    def gh_wait(i, h_v, par):
        @pl.when((i >= 0) & (i < n_iter))
        def _():
            pltpu.make_async_copy(h_v, ghs_hbm.at[pl.ds(0, NCH * CH)], gh_sem.at[par]).wait()

    def gh_start(i, h_v, par):
        @pl.when((i >= 0) & (i < n_iter))
        def _():
            for c in range(NCH):
                b, t0, _ = chunk(i, c)
                row = pl.multiple_of(b * n_frames + t0, CH)
                pltpu.make_async_copy(h_v.at[pl.ds(c * CH, CH)], ghs_hbm.at[pl.ds(row, CH)], gh_sem.at[par]).start()

    def stage(i, zw, zr, lse_w, lse_r, top_v, sum_v, gwr, gr, h_v):
        zw[...] = jnp.dot(enc_rows(i), w_v[...], preferred_element_type=F32)
        h_v[...] = jnp.dot(gr[...], wt_v[...], preferred_element_type=F32)
        gwt_v[...] += lax.dot_general(gr[:, own], enc_rows(i - 2), (((0,), (0,)), ((), ())), preferred_element_type=F32)
        for c in range(NCH):
            b, t0, ok = chunk(i - 1, c)
            rows = slice(c * CH, (c + 1) * CH)
            live = row_ids < jnp.where(ok, in_len[b], 0) - t0
            lse = lse_r[rows, :]
            lacc_v[pl.ds(b, 1), :] += jnp.sum(jnp.where(live, lse, 0.0), axis=0, keepdims=True)
            lse = jnp.where(live, lse, 3.0e38)
            upper = (t0 >= mid).astype(jnp.int32)
            occ = jnp.where(live, eo_v[pl.ds(b + (t0 - upper * mid) * PITCH, CH, stride=PITCH), :], 0.0)
            inv = inv_v[pl.ds(pl.multiple_of(b * 8, 8), 8), :] + upper * 64
            for j in range(n_blk):
                cols = slice(j * 128, (j + 1) * 128)
                col_occ = take_lanes(occ, jnp.broadcast_to(inv[j:j + 1], (CH, 128)))
                gwr[rows, cols] = (jnp.exp(zr[rows, cols] - lse) - col_occ).astype(BF16)
        for r in range(NCH * CH // 8):
            rows = slice(r * 8, (r + 1) * 8)
            z = zw[rows, :]
            parts = [z[:, j * 128:(j + 1) * 128] for j in range(n_blk)]
            top = functools.reduce(jnp.maximum, parts)
            top_v[rows, :] = top
            sum_v[rows, :] = functools.reduce(jnp.add, [jnp.exp(part - top) for part in parts])
        tops = top_v[...]
        top = jnp.max(tops, axis=1, keepdims=True)
        lse_w[...] = jnp.broadcast_to(top + jnp.log(jnp.sum(sum_v[...] * jnp.exp(tops - top), axis=1, keepdims=True)), (NCH * CH, 128))

    trips = (n_iter + 3) // 2

    @pl.loop(0, trips)
    def _(ii):
        i = 2 * ii
        slot = lax.rem(ii, 2)
        gh_wait(i - 6, h0_v.at[slot], 2 * slot)
        gh_wait(i - 5, h1_v.at[slot], 2 * slot + 1)
        stage(i, z0_v, z1_v, lse0_v, lse1_v, top0_v, sum0_v, g1_v, g0_v, h0_v.at[slot])
        stage(i + 1, z1_v, z0_v, lse1_v, lse0_v, top1_v, sum1_v, g0_v, g1_v, h1_v.at[slot])
        gh_start(i - 2, h0_v.at[slot], 2 * slot)
        gh_start(i - 1, h1_v.at[slot], 2 * slot + 1)

    for back in (2, 1):
        slot = lax.rem(trips - back + 2, 2)
        gh_wait(2 * (trips - back) - 2, h0_v.at[slot], 2 * slot)
        gh_wait(2 * (trips - back) - 1, h1_v.at[slot], 2 * slot + 1)
    gw_ref[...] = gwt_v[...].T
    loss_ref[...] = lacc_v[...].T[0:1, :] - blank_sum - log_z


def solution(mesh):
    n_dev = mesh.shape["tp"]

    def device_fn(enc_out, w_loc, labels, in_len, lab_len):
        n_seq, n_frames, hidden = enc_out.shape
        n_lab = labels.shape[1]
        n_cols = w_loc.shape[1]
        n_vocab = n_cols * n_dev
        vmem = pl.BlockSpec(memory_space=pltpu.VMEM)
        smem = pl.BlockSpec(memory_space=pltpu.SMEM)
        anyspace = pl.BlockSpec(memory_space=pl.ANY)
        w_all = pl.pallas_call(
            gather_kernel,
            out_shape=jax.ShapeDtypeStruct((n_dev, hidden, n_cols), BF16),
            in_specs=[anyspace],
            out_specs=anyspace,
            scratch_shapes=[
                pltpu.VMEM((n_dev, hidden, n_cols), BF16),
                pltpu.SemaphoreType.DMA((11,)),
                pltpu.SemaphoreType.DMA((11,)),
                pltpu.SemaphoreType.DMA,
                pltpu.SemaphoreType.DMA((n_dev,)),
            ],
            compiler_params=pltpu.CompilerParams(collective_id=0, has_side_effects=True),
            name="gather_w",
        )(w_loc)
        n_per = n_frames // CH
        n_grp = n_seq // 4
        loss, grad_w, grad_hs = pl.pallas_call(
            functools.partial(ctc_kernel, n_seq, n_frames, n_lab),
            out_shape=(
                jax.ShapeDtypeStruct((1, n_seq), F32),
                jax.ShapeDtypeStruct((hidden, n_cols), F32),
                jax.ShapeDtypeStruct((n_seq * n_frames, hidden), F32),
            ),
            in_specs=[smem, vmem, vmem, vmem, anyspace, anyspace],
            out_specs=(vmem, vmem, anyspace),
            scratch_shapes=[
                pltpu.VMEM((n_seq * n_frames, hidden), BF16),
                pltpu.VMEM((hidden, n_vocab), BF16),
                pltpu.VMEM((n_vocab, hidden), BF16),
                pltpu.VMEM((192, n_vocab), BF16),
                pltpu.VMEM((192, n_vocab), BF16),
                pltpu.VMEM((512, hidden), BF16),
                pltpu.VMEM((512, hidden), BF16),
                pltpu.VMEM((n_frames // 2 * PITCH, 128), F32),
                pltpu.VMEM((n_frames * 48, 128), F32),
                pltpu.VMEM((n_frames * 104, 128), F32),
                pltpu.VMEM((n_seq * n_dev, 128), jnp.int32),
                pltpu.VMEM((n_seq + 8, 128), jnp.int32),
                pltpu.VMEM((NCH * CH, n_vocab), F32),
                pltpu.VMEM((NCH * CH, n_vocab), F32),
                pltpu.VMEM((NCH * CH, n_vocab), BF16),
                pltpu.VMEM((NCH * CH, n_vocab), BF16),
                pltpu.VMEM((2, NCH * CH, hidden), F32),
                pltpu.VMEM((2, NCH * CH, hidden), F32),
                pltpu.VMEM((NCH * CH, 128), F32),
                pltpu.VMEM((NCH * CH, 128), F32),
                pltpu.VMEM((NCH * CH, 128), F32),
                pltpu.VMEM((NCH * CH, 128), F32),
                pltpu.VMEM((NCH * CH, 128), F32),
                pltpu.VMEM((NCH * CH, 128), F32),
                pltpu.VMEM((n_cols, hidden), F32),
                pltpu.VMEM((n_seq, 128), F32),
                pltpu.VMEM((CH, hidden), F32),
                pltpu.VMEM((8, 128), jnp.int32),
                pltpu.SMEM((n_seq * n_per + 3 * PAD,), jnp.int32),
                pltpu.SMEM((n_seq * n_per + 3 * PAD,), jnp.int32),
                pltpu.SMEM((n_seq + 8,), jnp.int32),
                pltpu.SMEM((8, 128), jnp.int32),
                pltpu.SemaphoreType.DMA((n_grp,)),
                pltpu.SemaphoreType.DMA((n_dev,)),
                pltpu.SemaphoreType.DMA((4,)),
                pltpu.SemaphoreType.DMA,
                pltpu.SemaphoreType.DMA,
            ],
            compiler_params=pltpu.CompilerParams(vmem_limit_bytes=63 * 1024 * 1024),
            name="ctc",
        )(in_len, labels.T, in_len.reshape(1, n_seq), lab_len.reshape(1, n_seq), enc_out.reshape(n_seq * n_frames, hidden), w_all)
        return loss.reshape(n_seq), grad_w, grad_hs.reshape(n_seq, n_frames, hidden)

    return jax.shard_map(device_fn, mesh=mesh, in_specs=(P("dp"), P(None, "tp"), P("dp"), P("dp"), P("dp")), out_specs=(P("dp"), P("dp", "tp"), P("dp")), check_vma=False)
```

```python
import functools

import jax
import jax.numpy as jnp
from jax import lax
from jax.experimental import pallas as pl
from jax.experimental.pallas import tpu as pltpu
from jax.sharding import PartitionSpec as P

NEG_FILL = -1.0e30
CH = 32
NCH = 16
PAD = 6 * NCH
PITCH = 136
DUMMY = 55
AHEAD = 6
MESH = pl.DeviceIdType.MESH
F32 = jnp.float32
BF16 = jnp.bfloat16


def gather_kernel(w_hbm, out_hbm, buf, send_sem, recv_sem, in_sem, out_sem):
    me = lax.axis_index("tp")
    core, col, row = lax.rem(me, 2), lax.rem(me // 2, 2), me // 4
    mate = me + 1 - 2 * core
    across = me + 2 * (1 - 2 * col)
    along = me + 4 * (1 - 2 * row)
    far = across + along - me
    load = pltpu.make_async_copy(w_hbm, buf.at[me], in_sem)
    load.start()
    barrier = pltpu.get_barrier_semaphore()
    for peer in (mate, across, along):
        pl.semaphore_signal(barrier, inc=1, device_id={"tp": peer}, device_id_type=MESH)
    load.wait()
    pl.semaphore_wait(barrier, 3)
    rows = w_hbm.shape[0]
    upper, lower, whole = pl.ds(0, rows // 2), pl.ds(rows // 2, rows // 2), pl.ds(0, rows)

    def push(k, block, part, peer):
        copy = pltpu.make_async_remote_copy(
            src_ref=buf.at[block, part], dst_ref=buf.at[block, part], send_sem=send_sem.at[k], recv_sem=recv_sem.at[k],
            device_id={"tp": peer}, device_id_type=MESH,
        )
        copy.start()
        return copy

    stores = []

    def put(block):
        copy = pltpu.make_async_copy(buf.at[block], out_hbm.at[block], out_sem.at[len(stores)])
        copy.start()
        stores.append(copy)

    pushes = [
        push(0, me, upper, across), push(1, me, lower, along), push(2, me, lower, across), push(3, me, upper, along),
        push(4, me, whole, mate),
    ]
    put(me)
    pushes[0].wait_recv()
    pushes.append(push(5, across, upper, along))
    pushes[1].wait_recv()
    pushes.append(push(6, along, lower, across))
    pushes[4].wait_recv()
    put(mate)
    pushes[2].wait_recv()
    pushes.append(push(7, across, whole, mate))
    put(across)
    pushes[3].wait_recv()
    pushes.append(push(8, along, whole, mate))
    put(along)
    pushes[5].wait_recv()
    pushes.append(push(9, far, upper, mate))
    pushes[6].wait_recv()
    pushes.append(push(10, far, lower, mate))
    put(far)
    pushes[7].wait_recv()
    put(mate + across - me)
    pushes[8].wait_recv()
    put(mate + along - me)
    pushes[9].wait_recv()
    pushes[10].wait_recv()
    put(mate + far - me)
    for copy in pushes:
        copy.wait_send()
    for copy in stores:
        copy.wait()


def take_lanes(x, idx):
    return jnp.take_along_axis(x, idx, axis=1, mode="promise_in_bounds")


def steps_of_four(low, high, step, state):
    def body(q, st):
        for u in range(4):
            st = step(low + 4 * q + u, st)
        return st

    state = lax.fori_loop(0, (high - low) // 4, body, state)
    for k in range(high - (high - low) % 4, high):
        state = step(k, state)
    return state


def lse2(a, b):
    top = jnp.maximum(a, b)
    return top + jnp.log(1.0 + jnp.exp(jnp.minimum(a, b) - top))


def ctc_kernel(
    n_seq, n_frames, n_lab,
    in_len, labt_ref, inrow_ref, lenrow_ref, enc_hbm, wg_hbm,
    loss_ref, gw_ref, ghs_hbm,
    enc_v, w_v, wt_v, oh0_v, oh1_v, gl0_v, gl1_v, eo_v, et_v, ab_v, inv_v, nxt_v, z0_v, z1_v, g0_v, g1_v, h0_v, h1_v, top0_v, top1_v, sum0_v, sum1_v, lse0_v, lse1_v, gwt_v, lacc_v, zero_v, flag_v,
    tabb, tabt, rep_s, flag_s, enc_sem, w_sem, gh_sem, zero_sem, flag_sem,
):
    me = lax.axis_index("tp")
    n_vocab = w_v.shape[1]
    n_blk = n_vocab // 128
    n_grp = n_seq // 4
    mid = n_frames // 2
    n_per = n_frames // CH
    per_mid = mid // CH

    def enc_copy(g):
        rows = pl.ds(pl.multiple_of(4 * g * n_frames, 4 * n_frames), 4 * n_frames)
        return pltpu.make_async_copy(enc_hbm.at[rows], enc_v.at[rows], enc_sem.at[g])

    w_copies = [pltpu.make_async_copy(wg_hbm.at[k], w_v.at[:, pl.ds(k * 128, 128)], w_sem.at[k]) for k in range(n_blk)]
    for copy in w_copies:
        copy.start()

    for g in range(AHEAD):
        enc_copy(g).start()

    for ref in (zero_v, lacc_v, gwt_v, z1_v, lse1_v, g0_v, g1_v):
        ref[...] = jnp.zeros_like(ref)
    sub48 = lax.broadcasted_iota(jnp.int32, (48, 128), 0)
    in_row = inrow_ref[...]
    len_row = lenrow_ref[...]
    lab48 = jnp.where(sub48 < len_row, labt_ref[...], -1 - sub48)
    skip = lab48 != pltpu.roll(lab48, 1, 0)

    nxt = jnp.full((48, 128), DUMMY, jnp.int32)
    later = jnp.zeros((48, 128), jnp.int32)
    for d in range(n_lab - 1, 0, -1):
        same = (pltpu.roll(lab48, 48 - d, 0) == lab48) & (sub48 < 48 - d)
        nxt = jnp.where(same, sub48 + d, nxt)
        later = later + jnp.where(same, 1, 0)
    nxt_f = jnp.concatenate([nxt.astype(F32), jnp.full((16, 128), float(DUMMY), F32)], axis=0)
    nxt_v[0:n_seq] = jnp.concatenate([nxt_f, nxt_f + 64.0], axis=0).T.astype(jnp.int32)
    nxt_v[n_seq:n_seq + 8] = jnp.full((8, 128), DUMMY, jnp.int32)
    flag_v[...] = jnp.broadcast_to(jnp.max(later.astype(F32), axis=0, keepdims=True), (8, 128)).astype(jnp.int32)
    flag_copy = pltpu.make_async_copy(flag_v, flag_s, flag_sem)
    flag_copy.start()

    for copy in w_copies:
        copy.wait()
    wt_v[...] = w_v[...].T
    row16 = lax.broadcasted_iota(jnp.int32, (16, wt_v.shape[1]), 0)
    tail = jnp.where(row16 == 0, wt_v[0:16, :].astype(F32), 0.0).astype(BF16)
    for k in range(8):
        gl0_v[k * 64 + 48:(k + 1) * 64, :] = tail
        gl1_v[k * 64 + 48:(k + 1) * 64, :] = tail

    lane48 = lax.broadcasted_iota(jnp.int32, (48, 128), 1)
    sub48f = sub48.astype(F32)
    lane1 = lax.broadcasted_iota(jnp.int32, (1, 128), 1)
    lane_mid = lax.broadcasted_iota(jnp.int32, (mid, 128), 1)

    def list_group(g, n):
        for k in range(4):
            b = 4 * g + k
            cnt = (in_len[jnp.minimum(b, n_seq - 1)] + CH - 1) // CH
            dead = n_seq * n_per - 1 - (b * n_per - n)
            for j in range(n_per):
                slot = jnp.where(g < n_grp, PAD + jnp.where(j < cnt, n + j, dead - (j - cnt)), j)
                tabb[slot] = b
                tabt[slot] = j * CH
            n = n + jnp.where(g < n_grp, cnt, 0)
        return n

    def build_hot(g, oh_v):
        for k in range(4):
            b = 4 * g + k
            col = take_lanes(lab48, jnp.full((48, 128), b, jnp.int32))
            firsts = []
            for j in range(n_blk):
                hit = col == lane48 + 128 * j
                oh_v[k * 48:(k + 1) * 48, j * 128:(j + 1) * 128] = jnp.where(hit, 1.0, 0.0).astype(BF16)
                start = jnp.where(lane1 == 0, 48.0, float(DUMMY)) if j == 0 else float(DUMMY)
                firsts.append(jnp.minimum(jnp.min(jnp.where(hit, sub48f, float(DUMMY)), axis=0, keepdims=True), start))
            inv_v[pl.ds(pl.multiple_of(b * 8, 8), 8), :] = jnp.concatenate(firsts, axis=0).astype(jnp.int32)

    def pick_cols(oh_v, gl_v):
        picked = jnp.dot(oh_v[...], wt_v[...], preferred_element_type=F32).astype(BF16)
        for k in range(4):
            for h in range(2):
                gl_v[k * 128 + h * 64:k * 128 + h * 64 + 48, :] = picked[k * 48:(k + 1) * 48]

    def emit_group(g, gl_v):
        for k in range(4):
            b = 4 * g + k
            x = enc_v[pl.ds(pl.multiple_of(b * n_frames, n_frames), n_frames), :]
            e = lax.dot_general(x, gl_v[k * 128:(k + 1) * 128, :], (((1,), (1,)), ((), ())), preferred_element_type=F32)
            eo_v[pl.ds(b, mid, stride=PITCH), :] = jnp.where(lane_mid < 64, e[0:mid], e[mid:n_frames])

    build_hot(0, oh0_v)

    def emit_pair(ii, n):
        for s in range(2):
            g = 2 * ii + s

            @pl.when((g >= 1) & (g <= n_grp))
            def _():
                enc_copy(g - 1).wait()

            @pl.when(g + AHEAD < n_grp)
            def _():
                enc_copy(g + AHEAD).start()
        n = list_group(2 * ii + 1, list_group(2 * ii, n))
        for s in range(2):
            g = 2 * ii + s
            build_hot(jnp.minimum(g + 1, n_grp - 1), (oh1_v, oh0_v)[s])
            pick_cols((oh0_v, oh1_v)[s], (gl0_v, gl1_v)[s])
            emit_group(jnp.clip(g - 1, 0, n_grp - 1), (gl1_v, gl0_v)[s])
        return n

    n_live = lax.fori_loop(0, n_grp // 2 + 1, emit_pair, 0)
    for j in range(PAD):
        for base in (0, PAD + n_seq * n_per):
            tabb[base + j] = 0
            tabt[base + j] = 0
    n_iter = (n_live + NCH - 1) // NCH

    def turn_in(j, acc):
        turned = eo_v[pl.ds(pl.multiple_of(j * PITCH, 8), n_seq), :].T
        low = turned[48:49]
        high = turned[112:113]
        et_v[pl.ds(pl.multiple_of(j * 48, 8), 48), :] = turned[0:48] - low
        et_v[pl.ds(pl.multiple_of((j + mid) * 48, 8), 48), :] = turned[64:112] - high
        return acc + jnp.where(j < in_row, low, 0.0) + jnp.where(j + mid < in_row, high, 0.0)

    blank_sum = jnp.zeros((1, 128), F32)
    for j in (0, 1, mid - 1):
        blank_sum = turn_in(j, blank_sum)

    neg8 = jnp.full((8, 128), NEG_FILL, F32)
    sub56 = lax.broadcasted_iota(jnp.int32, (56, 128), 0)

    def emit_at(t):
        return et_v[pl.ds(pl.multiple_of(t * 48, 8), 48), :]

    def alpha_step(t, blk, lab):
        shifted = pltpu.roll(jnp.concatenate([lab, neg8], axis=0), 1, 0)
        blk_new = lse2(blk, shifted)
        via = jnp.where(skip, blk_new[0:48], blk[0:48])
        lab_new = lse2(lab, via) + emit_at(t)
        live = t < in_row
        return jnp.where(live, blk_new, blk), jnp.where(live, lab_new, lab)

    def beta_step(t, blk, lab):
        emitted = lab + emit_at(t + 1)
        blk_new = lse2(blk, jnp.concatenate([emitted, neg8], axis=0))
        via = jnp.concatenate([jnp.where(skip, blk_new[0:48], blk[0:48]), blk_new[48:56]], axis=0)
        lab_new = lse2(emitted, pltpu.roll(via, 55, 0)[0:48])
        live = t + 1 < in_row
        return jnp.where(live, blk_new, blk), jnp.where(live, lab_new, lab)

    def keep(t, blk, lab):
        row = pl.multiple_of(t * 104, 8)
        ab_v[pl.ds(row, 56), :] = blk
        ab_v[pl.ds(row + 56, 48), :] = lab

    a_blk = jnp.where(sub56 == 0, 0.0, NEG_FILL).astype(F32) + jnp.zeros((56, 128), F32)
    a_lab = jnp.full((48, 128), NEG_FILL, F32)
    b_blk = jnp.where(sub56 == len_row, 0.0, NEG_FILL).astype(F32)
    b_lab = jnp.where(sub48 == len_row - 1, 0.0, NEG_FILL).astype(F32)

    a_blk, a_lab = alpha_step(0, a_blk, a_lab)
    keep(0, a_blk, a_lab)
    keep(n_frames - 1, b_blk, b_lab)

    def first_half(k, state):
        a_blk, a_lab, b_blk, b_lab = state
        a_blk, a_lab = alpha_step(k, a_blk, a_lab)
        keep(k, a_blk, a_lab)
        t = n_frames - 1 - k
        b_blk, b_lab = beta_step(t, b_blk, b_lab)
        keep(t, b_blk, b_lab)
        return a_blk, a_lab, b_blk, b_lab

    def first_quarter(k, state):
        new = first_half(k, state[:4])
        return (*new, turn_in(mid - 1 - k, turn_in(k + 1, state[4])))

    quarter = mid // 2
    a_blk, a_lab, b_blk, b_lab, blank_sum = steps_of_four(1, quarter - 1, first_quarter, (a_blk, a_lab, b_blk, b_lab, blank_sum))
    blank_sum = turn_in(quarter, blank_sum)

    flag_copy.wait()

    def second_quarter(k, state):
        n = state[4]
        for u in range(3):
            b = jnp.minimum(3 * (k - quarter + 1) + u, n_seq)
            rep_s[n] = b
            n = n + jnp.where((b < n_seq) & (flag_s[0, jnp.minimum(b, n_seq - 1)] > 0), 1, 0)
        return (*first_half(k, state[:4]), n)

    a_blk, a_lab, b_blk, b_lab, n_rep = steps_of_four(quarter - 1, mid, second_quarter, (a_blk, a_lab, b_blk, b_lab, 0))
    for u in range(4):
        rep_s[n_rep + u] = n_seq

    m_blk, m_lab = beta_step(mid - 1, b_blk, b_lab)
    s_blk = a_blk + m_blk
    s_lab = a_lab + m_lab
    top = jnp.maximum(jnp.max(s_blk, axis=0, keepdims=True), jnp.max(s_lab, axis=0, keepdims=True))
    total = jnp.sum(jnp.exp(s_blk - top), axis=0, keepdims=True) + jnp.sum(jnp.exp(s_lab - top), axis=0, keepdims=True)
    log_z = top + jnp.log(total)
    sub8 = lax.broadcasted_iota(jnp.int32, (8, 128), 0)

    def put_occ(t, blk, lab):
        row = pl.multiple_of(t * 104, 8)
        occ_blk = jnp.sum(jnp.exp(ab_v[pl.ds(row, 56), :] + (blk - log_z)), axis=0, keepdims=True)
        occ_lab = jnp.exp(ab_v[pl.ds(row + 56, 48), :] + (lab - log_z))
        ab_v[pl.ds(row, 48), :] = occ_lab
        ab_v[pl.ds(row + 48, 8), :] = jnp.where(sub8 == 0, occ_blk, 0.0)

    zero8 = jnp.zeros((8, 128), F32)

    def turn_out(j):
        low = ab_v[pl.ds(pl.multiple_of(j * 104, 8), 56), :]
        high = ab_v[pl.ds(pl.multiple_of((j + mid) * 104, 8), 56), :]
        turned = jnp.concatenate([low, zero8, high, zero8], axis=0).T
        eo_v[pl.ds(pl.multiple_of(j * PITCH, 8), n_seq), :] = turned

    per_step = -(-(n_seq * (n_per - 1)) // (n_frames - mid - 1))

    def second_half(k, state):
        for u in range(per_step):
            idx = n_live + per_step * (k - mid - 1) + u

            @pl.when(idx < n_seq * n_per)
            def _():
                row = pl.multiple_of(tabb[PAD + idx] * n_frames + tabt[PAD + idx], CH)
                pltpu.make_async_copy(zero_v, ghs_hbm.at[pl.ds(row, CH)], zero_sem).start()

        a_blk, a_lab, b_blk, b_lab = state
        t = n_frames - 1 - k
        put_occ(k - 1, a_blk, a_lab)
        put_occ(t + 1, b_blk, b_lab)
        a_blk, a_lab = alpha_step(k, a_blk, a_lab)
        b_blk, b_lab = beta_step(t, b_blk, b_lab)
        return a_blk, a_lab, b_blk, b_lab

    def last_quarter(k, state):
        turn_out(k - 2 - mid)
        turn_out(n_frames + 1 - k)
        return second_half(k, state)

    a_blk, a_lab = alpha_step(mid, a_blk, a_lab)
    state = steps_of_four(mid + 1, mid + quarter + 2, second_half, (a_blk, a_lab, m_blk, m_lab))
    a_blk, a_lab, b_blk, b_lab = steps_of_four(mid + quarter + 2, n_frames, last_quarter, state)
    put_occ(n_frames - 1, a_blk, a_lab)
    put_occ(0, b_blk, b_lab)
    for j in (mid - 2, 1, mid - 1, 0):
        turn_out(j)

    @pl.loop(0, (n_rep + 3) // 4)
    def _(q):
        seqs = [rep_s[4 * q + u] for u in range(4)]
        occs = [eo_v[pl.ds(b, mid, stride=PITCH), :] for b in seqs]
        links = [nxt_v[pl.ds(b, 1), :] for b in seqs]
        for b, occ, link in zip(seqs, occs, links):
            eo_v[pl.ds(b, mid, stride=PITCH), :] = occ + take_lanes(occ, jnp.broadcast_to(link, (mid, 128)))

    @pl.loop(0, n_rep)
    def _(r):
        b = rep_s[r]
        count = flag_s[0, b]

        @pl.when(count > 1)
        def _():
            rows = pl.ds(b, mid, stride=PITCH)
            rounds = sum((count >= 2 ** r).astype(jnp.int32) for r in range(1, 6))

            def more(_, link):
                link = take_lanes(link, link)
                occ = eo_v[rows, :]
                eo_v[rows, :] = occ + take_lanes(occ, jnp.broadcast_to(link[0:1], (mid, 128)))
                return link

            lax.fori_loop(0, rounds, more, jnp.broadcast_to(nxt_v[pl.ds(b, 1), :], (8, 128)))

    n_dead = n_seq * n_per - n_live
    for r in range((n_seq * n_per).bit_length()):
        @pl.when(lax.rem(n_dead // 2 ** r, 2) == 1)
        def _():
            part = ghs_hbm.at[pl.ds(0, CH * 2 ** r)]
            pltpu.make_async_copy(part, part, zero_sem).wait()

    row_ids = lax.broadcasted_iota(jnp.int32, (CH, 128), 0)
    own = pl.ds(pl.multiple_of(me * 128, 128), 128)

    def chunk(i, c):
        idx = i * NCH + c
        return tabb[idx + PAD], tabt[idx + PAD], (i >= 0) & (i < n_iter)

    def enc_rows(i):
        parts = []
        for c in range(NCH):
            b, t0, _ = chunk(i, c)
            parts.append(enc_v[pl.ds(pl.multiple_of(b * n_frames + t0, CH), CH), :])
        return jnp.concatenate(parts, axis=0)

    def gh_wait(i, h_v, par):
        @pl.when((i >= 0) & (i < n_iter))
        def _():
            pltpu.make_async_copy(h_v, ghs_hbm.at[pl.ds(0, NCH * CH)], gh_sem.at[par]).wait()

    def gh_start(i, h_v, par):
        @pl.when((i >= 0) & (i < n_iter))
        def _():
            for c in range(NCH):
                b, t0, _ = chunk(i, c)
                row = pl.multiple_of(b * n_frames + t0, CH)
                pltpu.make_async_copy(h_v.at[pl.ds(c * CH, CH)], ghs_hbm.at[pl.ds(row, CH)], gh_sem.at[par]).start()

    def stage(i, zw, zr, lse_w, lse_r, top_v, sum_v, gwr, gr, h_v):
        zw[...] = jnp.dot(enc_rows(i), w_v[...], preferred_element_type=F32)
        h_v[...] = jnp.dot(gr[...], wt_v[...], preferred_element_type=F32)
        gwt_v[...] += lax.dot_general(gr[:, own], enc_rows(i - 2), (((0,), (0,)), ((), ())), preferred_element_type=F32)
        for c in range(NCH):
            b, t0, ok = chunk(i - 1, c)
            rows = slice(c * CH, (c + 1) * CH)
            live = row_ids < jnp.where(ok, in_len[b], 0) - t0
            lse = lse_r[rows, :]
            lacc_v[pl.ds(b, 1), :] += jnp.sum(jnp.where(live, lse, 0.0), axis=0, keepdims=True)
            lse = jnp.where(live, lse, 3.0e38)
            upper = (t0 >= mid).astype(jnp.int32)
            occ = jnp.where(live, eo_v[pl.ds(b + (t0 - upper * mid) * PITCH, CH, stride=PITCH), :], 0.0)
            inv = inv_v[pl.ds(pl.multiple_of(b * 8, 8), 8), :] + upper * 64
            for j in range(n_blk):
                cols = slice(j * 128, (j + 1) * 128)
                col_occ = take_lanes(occ, jnp.broadcast_to(inv[j:j + 1], (CH, 128)))
                gwr[rows, cols] = (jnp.exp(zr[rows, cols] - lse) - col_occ).astype(BF16)
        for r in range(NCH * CH // 8):
            rows = slice(r * 8, (r + 1) * 8)
            z = zw[rows, :]
            parts = [z[:, j * 128:(j + 1) * 128] for j in range(n_blk)]
            top = functools.reduce(jnp.maximum, parts)
            top_v[rows, :] = top
            sum_v[rows, :] = functools.reduce(jnp.add, [jnp.exp(part - top) for part in parts])
        tops = top_v[...]
        top = jnp.max(tops, axis=1, keepdims=True)
        lse_w[...] = jnp.broadcast_to(top + jnp.log(jnp.sum(sum_v[...] * jnp.exp(tops - top), axis=1, keepdims=True)), (NCH * CH, 128))

    trips = (n_iter + 2) // 2
    odd = lax.rem(n_iter, 2) == 1

    def even_stage(i, slot):
        stage(i, z0_v, z1_v, lse0_v, lse1_v, top0_v, sum0_v, g1_v, g0_v, h0_v.at[slot])

    @pl.loop(0, trips)
    def _(ii):
        i = 2 * ii
        slot = lax.rem(ii, 2)
        gh_wait(i - 6, h0_v.at[slot], 2 * slot)
        gh_wait(i - 5, h1_v.at[slot], 2 * slot + 1)
        even_stage(i, slot)
        stage(i + 1, z1_v, z0_v, lse1_v, lse0_v, top1_v, sum1_v, g0_v, g1_v, h1_v.at[slot])
        gh_start(i - 2, h0_v.at[slot], 2 * slot)
        gh_start(i - 1, h1_v.at[slot], 2 * slot + 1)

    last = lax.rem(trips, 2)

    @pl.when(odd)
    def _():
        gh_wait(2 * trips - 6, h0_v.at[last], 2 * last)
        even_stage(2 * trips, last)
        gh_start(2 * trips - 2, h0_v.at[last], 2 * last)

    gh_wait(jnp.where(odd, 2 * trips - 2, 2 * trips - 6), h0_v.at[last], 2 * last)
    gh_wait(2 * trips - 5, h1_v.at[last], 2 * last + 1)
    gh_wait(2 * trips - 4, h0_v.at[1 - last], 2 * (1 - last))
    gh_wait(2 * trips - 3, h1_v.at[1 - last], 2 * (1 - last) + 1)
    gw_ref[...] = gwt_v[...].T
    loss_ref[...] = lacc_v[...].T[0:1, :] - blank_sum - log_z


def solution(mesh):
    n_dev = mesh.shape["tp"]

    def device_fn(enc_out, w_loc, labels, in_len, lab_len):
        n_seq, n_frames, hidden = enc_out.shape
        n_lab = labels.shape[1]
        n_cols = w_loc.shape[1]
        n_vocab = n_cols * n_dev
        vmem = pl.BlockSpec(memory_space=pltpu.VMEM)
        smem = pl.BlockSpec(memory_space=pltpu.SMEM)
        anyspace = pl.BlockSpec(memory_space=pl.ANY)
        w_all = pl.pallas_call(
            gather_kernel,
            out_shape=jax.ShapeDtypeStruct((n_dev, hidden, n_cols), BF16),
            in_specs=[anyspace],
            out_specs=anyspace,
            scratch_shapes=[
                pltpu.VMEM((n_dev, hidden, n_cols), BF16),
                pltpu.SemaphoreType.DMA((11,)),
                pltpu.SemaphoreType.DMA((11,)),
                pltpu.SemaphoreType.DMA,
                pltpu.SemaphoreType.DMA((n_dev,)),
            ],
            compiler_params=pltpu.CompilerParams(collective_id=0, has_side_effects=True),
            name="gather_w",
        )(w_loc)
        n_per = n_frames // CH
        n_grp = n_seq // 4
        loss, grad_w, grad_hs = pl.pallas_call(
            functools.partial(ctc_kernel, n_seq, n_frames, n_lab),
            out_shape=(
                jax.ShapeDtypeStruct((1, n_seq), F32),
                jax.ShapeDtypeStruct((hidden, n_cols), F32),
                jax.ShapeDtypeStruct((n_seq * n_frames, hidden), F32),
            ),
            in_specs=[smem, vmem, vmem, vmem, anyspace, anyspace],
            out_specs=(vmem, vmem, anyspace),
            scratch_shapes=[
                pltpu.VMEM((n_seq * n_frames, hidden), BF16),
                pltpu.VMEM((hidden, n_vocab), BF16),
                pltpu.VMEM((n_vocab, hidden), BF16),
                pltpu.VMEM((192, n_vocab), BF16),
                pltpu.VMEM((192, n_vocab), BF16),
                pltpu.VMEM((512, hidden), BF16),
                pltpu.VMEM((512, hidden), BF16),
                pltpu.VMEM((n_frames // 2 * PITCH, 128), F32),
                pltpu.VMEM((n_frames * 48, 128), F32),
                pltpu.VMEM((n_frames * 104, 128), F32),
                pltpu.VMEM((n_seq * n_dev, 128), jnp.int32),
                pltpu.VMEM((n_seq + 8, 128), jnp.int32),
                pltpu.VMEM((NCH * CH, n_vocab), F32),
                pltpu.VMEM((NCH * CH, n_vocab), F32),
                pltpu.VMEM((NCH * CH, n_vocab), BF16),
                pltpu.VMEM((NCH * CH, n_vocab), BF16),
                pltpu.VMEM((2, NCH * CH, hidden), F32),
                pltpu.VMEM((2, NCH * CH, hidden), F32),
                pltpu.VMEM((NCH * CH, 128), F32),
                pltpu.VMEM((NCH * CH, 128), F32),
                pltpu.VMEM((NCH * CH, 128), F32),
                pltpu.VMEM((NCH * CH, 128), F32),
                pltpu.VMEM((NCH * CH, 128), F32),
                pltpu.VMEM((NCH * CH, 128), F32),
                pltpu.VMEM((n_cols, hidden), F32),
                pltpu.VMEM((n_seq, 128), F32),
                pltpu.VMEM((CH, hidden), F32),
                pltpu.VMEM((8, 128), jnp.int32),
                pltpu.SMEM((n_seq * n_per + 3 * PAD,), jnp.int32),
                pltpu.SMEM((n_seq * n_per + 3 * PAD,), jnp.int32),
                pltpu.SMEM((n_seq + 8,), jnp.int32),
                pltpu.SMEM((8, 128), jnp.int32),
                pltpu.SemaphoreType.DMA((n_grp,)),
                pltpu.SemaphoreType.DMA((n_dev,)),
                pltpu.SemaphoreType.DMA((4,)),
                pltpu.SemaphoreType.DMA,
                pltpu.SemaphoreType.DMA,
            ],
            compiler_params=pltpu.CompilerParams(vmem_limit_bytes=63 * 1024 * 1024),
            name="ctc",
        )(in_len, labels.T, in_len.reshape(1, n_seq), lab_len.reshape(1, n_seq), enc_out.reshape(n_seq * n_frames, hidden), w_all)
        return loss.reshape(n_seq), grad_w, grad_hs.reshape(n_seq, n_frames, hidden)

    return jax.shard_map(device_fn, mesh=mesh, in_specs=(P("dp"), P(None, "tp"), P("dp"), P("dp"), P("dp")), out_specs=(P("dp"), P("dp", "tp"), P("dp")), check_vma=False)
```

```python
import functools

import jax
import jax.numpy as jnp
from jax import lax
from jax.experimental import pallas as pl
from jax.experimental.pallas import tpu as pltpu
from jax.sharding import PartitionSpec as P

NEG_FILL = -1.0e30
CH = 32
NCH = 16
PAD = 6 * NCH
PITCH = 136
DUMMY = 55
AHEAD = 6
MESH = pl.DeviceIdType.MESH
F32 = jnp.float32
BF16 = jnp.bfloat16


def gather_kernel(w_hbm, out_hbm, buf, send_sem, recv_sem, in_sem, out_sem):
    me = lax.axis_index("tp")
    core, col, row = lax.rem(me, 2), lax.rem(me // 2, 2), me // 4
    mate = me + 1 - 2 * core
    across = me + 2 * (1 - 2 * col)
    along = me + 4 * (1 - 2 * row)
    far = across + along - me
    load = pltpu.make_async_copy(w_hbm, buf.at[me], in_sem)
    load.start()
    barrier = pltpu.get_barrier_semaphore()
    for peer in (mate, across, along):
        pl.semaphore_signal(barrier, inc=1, device_id={"tp": peer}, device_id_type=MESH)
    load.wait()
    pl.semaphore_wait(barrier, 3)
    rows = w_hbm.shape[0]
    upper, lower, whole = pl.ds(0, rows // 2), pl.ds(rows // 2, rows // 2), pl.ds(0, rows)

    def push(k, block, part, peer):
        copy = pltpu.make_async_remote_copy(
            src_ref=buf.at[block, part], dst_ref=buf.at[block, part], send_sem=send_sem.at[k], recv_sem=recv_sem.at[k],
            device_id={"tp": peer}, device_id_type=MESH,
        )
        copy.start()
        return copy

    stores = []

    def put(block):
        copy = pltpu.make_async_copy(buf.at[block], out_hbm.at[block], out_sem.at[len(stores)])
        copy.start()
        stores.append(copy)

    pushes = [
        push(0, me, upper, across), push(1, me, lower, along), push(2, me, lower, across), push(3, me, upper, along),
        push(4, me, whole, mate),
    ]
    put(me)
    pushes[0].wait_recv()
    pushes.append(push(5, across, upper, along))
    pushes[1].wait_recv()
    pushes.append(push(6, along, lower, across))
    pushes[4].wait_recv()
    put(mate)
    pushes[2].wait_recv()
    pushes.append(push(7, across, whole, mate))
    put(across)
    pushes[3].wait_recv()
    pushes.append(push(8, along, whole, mate))
    put(along)
    pushes[5].wait_recv()
    pushes.append(push(9, far, upper, mate))
    pushes[6].wait_recv()
    pushes.append(push(10, far, lower, mate))
    put(far)
    pushes[7].wait_recv()
    put(mate + across - me)
    pushes[8].wait_recv()
    put(mate + along - me)
    pushes[9].wait_recv()
    pushes[10].wait_recv()
    put(mate + far - me)
    for copy in pushes:
        copy.wait_send()
    for copy in stores:
        copy.wait()


def take_lanes(x, idx):
    return jnp.take_along_axis(x, idx, axis=1, mode="promise_in_bounds")


def steps_of_four(low, high, step, state):
    def body(q, st):
        for u in range(4):
            st = step(low + 4 * q + u, st)
        return st

    state = lax.fori_loop(0, (high - low) // 4, body, state)
    for k in range(high - (high - low) % 4, high):
        state = step(k, state)
    return state


def lse2(a, b):
    top = jnp.maximum(a, b)
    return top + jnp.log(1.0 + jnp.exp(jnp.minimum(a, b) - top))


def ctc_kernel(
    n_seq, n_frames, n_lab,
    in_len, labt_ref, inrow_ref, lenrow_ref, enc_hbm, wg_hbm,
    loss_ref, gw_ref, ghs_hbm,
    enc_v, w_v, wt_v, oh0_v, oh1_v, gl0_v, gl1_v, eo_v, et_v, ab_v, inv_v, nxt_v, z0_v, z1_v, g0_v, g1_v, h0_v, h1_v, top0_v, top1_v, sum0_v, sum1_v, lse0_v, lse1_v, gwt_v, lacc_v, zero_v, flag_v,
    tabb, tabt, rep_s, flag_s, enc_sem, w_sem, gh_sem, zero_sem, flag_sem,
):
    me = lax.axis_index("tp")
    n_vocab = w_v.shape[1]
    n_blk = n_vocab // 128
    n_grp = n_seq // 4
    mid = n_frames // 2
    n_per = n_frames // CH
    per_mid = mid // CH

    def enc_copy(g):
        rows = pl.ds(pl.multiple_of(4 * g * n_frames, 4 * n_frames), 4 * n_frames)
        return pltpu.make_async_copy(enc_hbm.at[rows], enc_v.at[rows], enc_sem.at[g])

    w_copies = [pltpu.make_async_copy(wg_hbm.at[k], w_v.at[:, pl.ds(k * 128, 128)], w_sem.at[k]) for k in range(n_blk)]
    for copy in w_copies:
        copy.start()

    for g in range(AHEAD):
        enc_copy(g).start()

    for ref in (zero_v, lacc_v, gwt_v, z1_v, lse1_v, g0_v, g1_v):
        ref[...] = jnp.zeros_like(ref)
    sub48 = lax.broadcasted_iota(jnp.int32, (48, 128), 0)
    in_row = inrow_ref[...]
    len_row = lenrow_ref[...]
    lab48 = jnp.where(sub48 < len_row, labt_ref[...], -1 - sub48)
    skip = lab48 != pltpu.roll(lab48, 1, 0)

    nxt = jnp.full((48, 128), DUMMY, jnp.int32)
    later = jnp.zeros((48, 128), jnp.int32)
    for d in range(n_lab - 1, 0, -1):
        same = (pltpu.roll(lab48, 48 - d, 0) == lab48) & (sub48 < 48 - d)
        nxt = jnp.where(same, sub48 + d, nxt)
        later = later + jnp.where(same, 1, 0)
    nxt_f = jnp.concatenate([nxt.astype(F32), jnp.full((16, 128), float(DUMMY), F32)], axis=0)
    nxt_v[0:n_seq] = jnp.concatenate([nxt_f, nxt_f + 64.0], axis=0).T.astype(jnp.int32)
    nxt_v[n_seq:n_seq + 8] = jnp.full((8, 128), DUMMY, jnp.int32)
    flag_v[...] = jnp.broadcast_to(jnp.max(later.astype(F32), axis=0, keepdims=True), (8, 128)).astype(jnp.int32)
    flag_copy = pltpu.make_async_copy(flag_v, flag_s, flag_sem)
    flag_copy.start()

    for copy in w_copies:
        copy.wait()
    wt_v[...] = w_v[...].T
    row16 = lax.broadcasted_iota(jnp.int32, (16, wt_v.shape[1]), 0)
    tail = jnp.where(row16 == 0, wt_v[0:16, :].astype(F32), 0.0).astype(BF16)
    for k in range(8):
        gl0_v[k * 64 + 48:(k + 1) * 64, :] = tail
        gl1_v[k * 64 + 48:(k + 1) * 64, :] = tail

    lane48 = lax.broadcasted_iota(jnp.int32, (48, 128), 1)
    sub48f = sub48.astype(F32)
    lane1 = lax.broadcasted_iota(jnp.int32, (1, 128), 1)
    lane_mid = lax.broadcasted_iota(jnp.int32, (mid, 128), 1)

    def list_group(g, n):
        for k in range(4):
            b = 4 * g + k
            cnt = (in_len[jnp.minimum(b, n_seq - 1)] + CH - 1) // CH
            dead = n_seq * n_per - 1 - (b * n_per - n)
            for j in range(n_per):
                slot = jnp.where(g < n_grp, PAD + jnp.where(j < cnt, n + j, dead - (j - cnt)), j)
                tabb[slot] = b
                tabt[slot] = j * CH
            n = n + jnp.where(g < n_grp, cnt, 0)
        return n

    def build_hot(g, oh_v):
        for k in range(4):
            b = 4 * g + k
            col = take_lanes(lab48, jnp.full((48, 128), b, jnp.int32))
            firsts = []
            for j in range(n_blk):
                hit = col == lane48 + 128 * j
                oh_v[k * 48:(k + 1) * 48, j * 128:(j + 1) * 128] = jnp.where(hit, 1.0, 0.0).astype(BF16)
                start = jnp.where(lane1 == 0, 48.0, float(DUMMY)) if j == 0 else float(DUMMY)
                firsts.append(jnp.minimum(jnp.min(jnp.where(hit, sub48f, float(DUMMY)), axis=0, keepdims=True), start))
            inv_v[pl.ds(pl.multiple_of(b * 8, 8), 8), :] = jnp.concatenate(firsts, axis=0).astype(jnp.int32)

    def pick_cols(oh_v, gl_v):
        picked = jnp.dot(oh_v[...], wt_v[...], preferred_element_type=F32).astype(BF16)
        for k in range(4):
            for h in range(2):
                gl_v[k * 128 + h * 64:k * 128 + h * 64 + 48, :] = picked[k * 48:(k + 1) * 48]

    def emit_group(g, gl_v):
        for k in range(4):
            b = 4 * g + k
            x = enc_v[pl.ds(pl.multiple_of(b * n_frames, n_frames), n_frames), :]
            e = lax.dot_general(x, gl_v[k * 128:(k + 1) * 128, :], (((1,), (1,)), ((), ())), preferred_element_type=F32)
            eo_v[pl.ds(b, mid, stride=PITCH), :] = jnp.where(lane_mid < 64, e[0:mid], e[mid:n_frames])

    build_hot(0, oh0_v)

    def emit_pair(ii, n):
        for s in range(2):
            g = 2 * ii + s

            @pl.when((g >= 1) & (g <= n_grp))
            def _():
                enc_copy(g - 1).wait()

            @pl.when(g + AHEAD < n_grp)
            def _():
                enc_copy(g + AHEAD).start()
        n = list_group(2 * ii + 1, list_group(2 * ii, n))
        for s in range(2):
            g = 2 * ii + s
            build_hot(jnp.minimum(g + 1, n_grp - 1), (oh1_v, oh0_v)[s])
            pick_cols((oh0_v, oh1_v)[s], (gl0_v, gl1_v)[s])
            emit_group(jnp.clip(g - 1, 0, n_grp - 1), (gl1_v, gl0_v)[s])
        return n

    n_live = lax.fori_loop(0, n_grp // 2 + 1, emit_pair, 0)
    for j in range(PAD):
        for base in (0, PAD + n_seq * n_per):
            tabb[base + j] = 0
            tabt[base + j] = 0
    n_iter = (n_live + NCH - 1) // NCH

    def turn_in(j, acc):
        turned = eo_v[pl.ds(pl.multiple_of(j * PITCH, 8), n_seq), :].T
        low = turned[48:49]
        high = turned[112:113]
        et_v[pl.ds(pl.multiple_of(j * 48, 8), 48), :] = turned[0:48] - low
        et_v[pl.ds(pl.multiple_of((j + mid) * 48, 8), 48), :] = turned[64:112] - high
        return acc + jnp.where(j < in_row, low, 0.0) + jnp.where(j + mid < in_row, high, 0.0)

    blank_sum = jnp.zeros((1, 128), F32)
    for j in (0, 1, mid - 1):
        blank_sum = turn_in(j, blank_sum)

    neg8 = jnp.full((8, 128), NEG_FILL, F32)
    sub56 = lax.broadcasted_iota(jnp.int32, (56, 128), 0)

    def emit_at(t):
        return et_v[pl.ds(pl.multiple_of(t * 48, 8), 48), :]

    def alpha_step(t, blk, lab):
        shifted = pltpu.roll(jnp.concatenate([lab, neg8], axis=0), 1, 0)
        blk_new = lse2(blk, shifted)
        via = jnp.where(skip, blk_new[0:48], blk[0:48])
        lab_new = lse2(lab, via) + emit_at(t)
        live = t < in_row
        return jnp.where(live, blk_new, blk), jnp.where(live, lab_new, lab)

    def beta_step(t, blk, lab):
        emitted = lab + emit_at(t + 1)
        blk_new = lse2(blk, jnp.concatenate([emitted, neg8], axis=0))
        via = jnp.concatenate([jnp.where(skip, blk_new[0:48], blk[0:48]), blk_new[48:56]], axis=0)
        lab_new = lse2(emitted, pltpu.roll(via, 55, 0)[0:48])
        live = t + 1 < in_row
        return jnp.where(live, blk_new, blk), jnp.where(live, lab_new, lab)

    def keep(t, blk, lab):
        row = pl.multiple_of(t * 104, 8)
        ab_v[pl.ds(row, 56), :] = blk
        ab_v[pl.ds(row + 56, 48), :] = lab

    a_blk = jnp.where(sub56 == 0, 0.0, NEG_FILL).astype(F32) + jnp.zeros((56, 128), F32)
    a_lab = jnp.full((48, 128), NEG_FILL, F32)
    b_blk = jnp.where(sub56 == len_row, 0.0, NEG_FILL).astype(F32)
    b_lab = jnp.where(sub48 == len_row - 1, 0.0, NEG_FILL).astype(F32)

    a_blk, a_lab = alpha_step(0, a_blk, a_lab)
    keep(0, a_blk, a_lab)
    keep(n_frames - 1, b_blk, b_lab)

    def first_half(k, state):
        a_blk, a_lab, b_blk, b_lab = state
        a_blk, a_lab = alpha_step(k, a_blk, a_lab)
        keep(k, a_blk, a_lab)
        t = n_frames - 1 - k
        b_blk, b_lab = beta_step(t, b_blk, b_lab)
        keep(t, b_blk, b_lab)
        return a_blk, a_lab, b_blk, b_lab

    def first_quarter(k, state):
        new = first_half(k, state[:4])
        return (*new, turn_in(mid - 1 - k, turn_in(k + 1, state[4])))

    quarter = mid // 2
    a_blk, a_lab, b_blk, b_lab, blank_sum = steps_of_four(1, quarter - 1, first_quarter, (a_blk, a_lab, b_blk, b_lab, blank_sum))
    blank_sum = turn_in(quarter, blank_sum)

    flag_copy.wait()

    def second_quarter(k, state):
        n = state[4]
        for u in range(3):
            b = jnp.minimum(3 * (k - quarter + 1) + u, n_seq)
            rep_s[n] = b
            n = n + jnp.where((b < n_seq) & (flag_s[0, jnp.minimum(b, n_seq - 1)] > 0), 1, 0)
        return (*first_half(k, state[:4]), n)

    a_blk, a_lab, b_blk, b_lab, n_rep = steps_of_four(quarter - 1, mid, second_quarter, (a_blk, a_lab, b_blk, b_lab, 0))
    for u in range(4):
        rep_s[n_rep + u] = n_seq

    m_blk, m_lab = beta_step(mid - 1, b_blk, b_lab)
    s_blk = a_blk + m_blk
    s_lab = a_lab + m_lab
    top = jnp.maximum(jnp.max(s_blk, axis=0, keepdims=True), jnp.max(s_lab, axis=0, keepdims=True))
    total = jnp.sum(jnp.exp(s_blk - top), axis=0, keepdims=True) + jnp.sum(jnp.exp(s_lab - top), axis=0, keepdims=True)
    log_z = top + jnp.log(total)
    sub8 = lax.broadcasted_iota(jnp.int32, (8, 128), 0)

    def put_occ(t, blk, lab):
        row = pl.multiple_of(t * 104, 8)
        occ_blk = jnp.sum(jnp.exp(ab_v[pl.ds(row, 56), :] + (blk - log_z)), axis=0, keepdims=True)
        occ_lab = jnp.exp(ab_v[pl.ds(row + 56, 48), :] + (lab - log_z))
        ab_v[pl.ds(row, 48), :] = occ_lab
        ab_v[pl.ds(row + 48, 8), :] = jnp.where(sub8 == 0, occ_blk, 0.0)

    zero8 = jnp.zeros((8, 128), F32)

    def turn_out(j):
        low = ab_v[pl.ds(pl.multiple_of(j * 104, 8), 56), :]
        high = ab_v[pl.ds(pl.multiple_of((j + mid) * 104, 8), 56), :]
        turned = jnp.concatenate([low, zero8, high, zero8], axis=0).T
        eo_v[pl.ds(pl.multiple_of(j * PITCH, 8), n_seq), :] = turned

    per_step = -(-(n_seq * (n_per - 1)) // (mid // 2 + 1))

    def late_step(k, state):
        a_blk, a_lab, b_blk, b_lab = state
        t = n_frames - 1 - k
        put_occ(k - 1, a_blk, a_lab)
        put_occ(t + 1, b_blk, b_lab)
        a_blk, a_lab = alpha_step(k, a_blk, a_lab)
        b_blk, b_lab = beta_step(t, b_blk, b_lab)
        return a_blk, a_lab, b_blk, b_lab

    def third_quarter(k, state):
        for u in range(per_step):
            idx = n_live + per_step * (k - mid - 1) + u

            @pl.when(idx < n_seq * n_per)
            def _():
                row = pl.multiple_of(tabb[PAD + idx] * n_frames + tabt[PAD + idx], CH)
                pltpu.make_async_copy(zero_v, ghs_hbm.at[pl.ds(row, CH)], zero_sem).start()

        return late_step(k, state)

    def last_quarter(k, state):
        turn_out(k - 2 - mid)
        turn_out(n_frames + 1 - k)
        return late_step(k, state)

    a_blk, a_lab = alpha_step(mid, a_blk, a_lab)
    state = steps_of_four(mid + 1, mid + quarter + 2, third_quarter, (a_blk, a_lab, m_blk, m_lab))
    a_blk, a_lab, b_blk, b_lab = steps_of_four(mid + quarter + 2, n_frames, last_quarter, state)
    put_occ(n_frames - 1, a_blk, a_lab)
    put_occ(0, b_blk, b_lab)
    for j in (mid - 2, 1, mid - 1, 0):
        turn_out(j)

    @pl.loop(0, (n_rep + 3) // 4)
    def _(q):
        seqs = [rep_s[4 * q + u] for u in range(4)]
        occs = [eo_v[pl.ds(b, mid, stride=PITCH), :] for b in seqs]
        links = [nxt_v[pl.ds(b, 1), :] for b in seqs]
        for b, occ, link in zip(seqs, occs, links):
            eo_v[pl.ds(b, mid, stride=PITCH), :] = occ + take_lanes(occ, jnp.broadcast_to(link, (mid, 128)))

    @pl.loop(0, n_rep)
    def _(r):
        b = rep_s[r]
        count = flag_s[0, b]

        @pl.when(count > 1)
        def _():
            rows = pl.ds(b, mid, stride=PITCH)
            rounds = sum((count >= 2 ** r).astype(jnp.int32) for r in range(1, 6))

            def more(_, link):
                link = take_lanes(link, link)
                occ = eo_v[rows, :]
                eo_v[rows, :] = occ + take_lanes(occ, jnp.broadcast_to(link[0:1], (mid, 128)))
                return link

            lax.fori_loop(0, rounds, more, jnp.broadcast_to(nxt_v[pl.ds(b, 1), :], (8, 128)))

    n_dead = n_seq * n_per - n_live
    for r in range((n_seq * n_per).bit_length()):
        @pl.when(lax.rem(n_dead // 2 ** r, 2) == 1)
        def _():
            part = ghs_hbm.at[pl.ds(0, CH * 2 ** r)]
            pltpu.make_async_copy(part, part, zero_sem).wait()

    row_ids = lax.broadcasted_iota(jnp.int32, (CH, 128), 0)
    own = pl.ds(pl.multiple_of(me * 128, 128), 128)

    def chunk(i, c):
        idx = i * NCH + c
        return tabb[idx + PAD], tabt[idx + PAD], (i >= 0) & (i < n_iter)

    def enc_rows(i):
        parts = []
        for c in range(NCH):
            b, t0, _ = chunk(i, c)
            parts.append(enc_v[pl.ds(pl.multiple_of(b * n_frames + t0, CH), CH), :])
        return jnp.concatenate(parts, axis=0)

    def gh_wait(i, h_v, par):
        @pl.when((i >= 0) & (i < n_iter))
        def _():
            pltpu.make_async_copy(h_v, ghs_hbm.at[pl.ds(0, NCH * CH)], gh_sem.at[par]).wait()

    def gh_start(i, h_v, par):
        @pl.when((i >= 0) & (i < n_iter))
        def _():
            for c in range(NCH):
                b, t0, _ = chunk(i, c)
                row = pl.multiple_of(b * n_frames + t0, CH)
                pltpu.make_async_copy(h_v.at[pl.ds(c * CH, CH)], ghs_hbm.at[pl.ds(row, CH)], gh_sem.at[par]).start()

    def stage(i, zw, zr, lse_w, lse_r, top_v, sum_v, gwr, gr, h_v):
        zw[...] = jnp.dot(enc_rows(i), w_v[...], preferred_element_type=F32)
        h_v[...] = jnp.dot(gr[...], wt_v[...], preferred_element_type=F32)
        gwt_v[...] += lax.dot_general(gr[:, own], enc_rows(i - 2), (((0,), (0,)), ((), ())), preferred_element_type=F32)
        for c in range(NCH):
            b, t0, ok = chunk(i - 1, c)
            rows = slice(c * CH, (c + 1) * CH)
            live = row_ids < jnp.where(ok, in_len[b], 0) - t0
            lse = lse_r[rows, :]
            lacc_v[pl.ds(b, 1), :] += jnp.sum(jnp.where(live, lse, 0.0), axis=0, keepdims=True)
            lse = jnp.where(live, lse, 3.0e38)
            upper = (t0 >= mid).astype(jnp.int32)
            occ = jnp.where(live, eo_v[pl.ds(b + (t0 - upper * mid) * PITCH, CH, stride=PITCH), :], 0.0)
            inv = inv_v[pl.ds(pl.multiple_of(b * 8, 8), 8), :] + upper * 64
            for j in range(n_blk):
                cols = slice(j * 128, (j + 1) * 128)
                col_occ = take_lanes(occ, jnp.broadcast_to(inv[j:j + 1], (CH, 128)))
                gwr[rows, cols] = (jnp.exp(zr[rows, cols] - lse) - col_occ).astype(BF16)
        for r in range(NCH * CH // 8):
            rows = slice(r * 8, (r + 1) * 8)
            z = zw[rows, :]
            parts = [z[:, j * 128:(j + 1) * 128] for j in range(n_blk)]
            top = functools.reduce(jnp.maximum, parts)
            top_v[rows, :] = top
            sum_v[rows, :] = functools.reduce(jnp.add, [jnp.exp(part - top) for part in parts])
        tops = top_v[...]
        top = jnp.max(tops, axis=1, keepdims=True)
        lse_w[...] = jnp.broadcast_to(top + jnp.log(jnp.sum(sum_v[...] * jnp.exp(tops - top), axis=1, keepdims=True)), (NCH * CH, 128))

    trips = (n_iter + 2) // 2
    odd = lax.rem(n_iter, 2) == 1

    def even_stage(i, slot):
        stage(i, z0_v, z1_v, lse0_v, lse1_v, top0_v, sum0_v, g1_v, g0_v, h0_v.at[slot])

    @pl.loop(0, trips)
    def _(ii):
        i = 2 * ii
        slot = lax.rem(ii, 2)
        gh_wait(i - 6, h0_v.at[slot], 2 * slot)
        gh_wait(i - 5, h1_v.at[slot], 2 * slot + 1)
        even_stage(i, slot)
        stage(i + 1, z1_v, z0_v, lse1_v, lse0_v, top1_v, sum1_v, g0_v, g1_v, h1_v.at[slot])
        gh_start(i - 2, h0_v.at[slot], 2 * slot)
        gh_start(i - 1, h1_v.at[slot], 2 * slot + 1)

    last = lax.rem(trips, 2)

    @pl.when(odd)
    def _():
        gh_wait(2 * trips - 6, h0_v.at[last], 2 * last)
        even_stage(2 * trips, last)
        gh_start(2 * trips - 2, h0_v.at[last], 2 * last)

    gh_wait(jnp.where(odd, 2 * trips - 2, 2 * trips - 6), h0_v.at[last], 2 * last)
    gh_wait(2 * trips - 5, h1_v.at[last], 2 * last + 1)
    gh_wait(2 * trips - 4, h0_v.at[1 - last], 2 * (1 - last))
    gh_wait(2 * trips - 3, h1_v.at[1 - last], 2 * (1 - last) + 1)
    gw_ref[...] = gwt_v[...].T
    loss_ref[...] = lacc_v[...].T[0:1, :] - blank_sum - log_z


def solution(mesh):
    n_dev = mesh.shape["tp"]

    def device_fn(enc_out, w_loc, labels, in_len, lab_len):
        n_seq, n_frames, hidden = enc_out.shape
        n_lab = labels.shape[1]
        n_cols = w_loc.shape[1]
        n_vocab = n_cols * n_dev
        vmem = pl.BlockSpec(memory_space=pltpu.VMEM)
        smem = pl.BlockSpec(memory_space=pltpu.SMEM)
        anyspace = pl.BlockSpec(memory_space=pl.ANY)
        w_all = pl.pallas_call(
            gather_kernel,
            out_shape=jax.ShapeDtypeStruct((n_dev, hidden, n_cols), BF16),
            in_specs=[anyspace],
            out_specs=anyspace,
            scratch_shapes=[
                pltpu.VMEM((n_dev, hidden, n_cols), BF16),
                pltpu.SemaphoreType.DMA((11,)),
                pltpu.SemaphoreType.DMA((11,)),
                pltpu.SemaphoreType.DMA,
                pltpu.SemaphoreType.DMA((n_dev,)),
            ],
            compiler_params=pltpu.CompilerParams(collective_id=0, has_side_effects=True),
            name="gather_w",
        )(w_loc)
        n_per = n_frames // CH
        n_grp = n_seq // 4
        loss, grad_w, grad_hs = pl.pallas_call(
            functools.partial(ctc_kernel, n_seq, n_frames, n_lab),
            out_shape=(
                jax.ShapeDtypeStruct((1, n_seq), F32),
                jax.ShapeDtypeStruct((hidden, n_cols), F32),
                jax.ShapeDtypeStruct((n_seq * n_frames, hidden), F32),
            ),
            in_specs=[smem, vmem, vmem, vmem, anyspace, anyspace],
            out_specs=(vmem, vmem, anyspace),
            scratch_shapes=[
                pltpu.VMEM((n_seq * n_frames, hidden), BF16),
                pltpu.VMEM((hidden, n_vocab), BF16),
                pltpu.VMEM((n_vocab, hidden), BF16),
                pltpu.VMEM((192, n_vocab), BF16),
                pltpu.VMEM((192, n_vocab), BF16),
                pltpu.VMEM((512, hidden), BF16),
                pltpu.VMEM((512, hidden), BF16),
                pltpu.VMEM((n_frames // 2 * PITCH, 128), F32),
                pltpu.VMEM((n_frames * 48, 128), F32),
                pltpu.VMEM((n_frames * 104, 128), F32),
                pltpu.VMEM((n_seq * n_dev, 128), jnp.int32),
                pltpu.VMEM((n_seq + 8, 128), jnp.int32),
                pltpu.VMEM((NCH * CH, n_vocab), F32),
                pltpu.VMEM((NCH * CH, n_vocab), F32),
                pltpu.VMEM((NCH * CH, n_vocab), BF16),
                pltpu.VMEM((NCH * CH, n_vocab), BF16),
                pltpu.VMEM((2, NCH * CH, hidden), F32),
                pltpu.VMEM((2, NCH * CH, hidden), F32),
                pltpu.VMEM((NCH * CH, 128), F32),
                pltpu.VMEM((NCH * CH, 128), F32),
                pltpu.VMEM((NCH * CH, 128), F32),
                pltpu.VMEM((NCH * CH, 128), F32),
                pltpu.VMEM((NCH * CH, 128), F32),
                pltpu.VMEM((NCH * CH, 128), F32),
                pltpu.VMEM((n_cols, hidden), F32),
                pltpu.VMEM((n_seq, 128), F32),
                pltpu.VMEM((CH, hidden), F32),
                pltpu.VMEM((8, 128), jnp.int32),
                pltpu.SMEM((n_seq * n_per + 3 * PAD,), jnp.int32),
                pltpu.SMEM((n_seq * n_per + 3 * PAD,), jnp.int32),
                pltpu.SMEM((n_seq + 8,), jnp.int32),
                pltpu.SMEM((8, 128), jnp.int32),
                pltpu.SemaphoreType.DMA((n_grp,)),
                pltpu.SemaphoreType.DMA((n_dev,)),
                pltpu.SemaphoreType.DMA((4,)),
                pltpu.SemaphoreType.DMA,
                pltpu.SemaphoreType.DMA,
            ],
            compiler_params=pltpu.CompilerParams(vmem_limit_bytes=63 * 1024 * 1024),
            name="ctc",
        )(in_len, labels.T, in_len.reshape(1, n_seq), lab_len.reshape(1, n_seq), enc_out.reshape(n_seq * n_frames, hidden), w_all)
        return loss.reshape(n_seq), grad_w, grad_hs.reshape(n_seq, n_frames, hidden)

    return jax.shard_map(device_fn, mesh=mesh, in_specs=(P("dp"), P(None, "tp"), P("dp"), P("dp"), P("dp")), out_specs=(P("dp"), P("dp", "tp"), P("dp")), check_vma=False)
```
